256 devices in a mesh: lon: 16 (over z, x_hi), lat: 4 (over x_lo, core), head: 4 (over y).
Axes of the slice: x: 4 (x_hi: 2, x_lo: 2; x = x_hi * 2 + x_lo), y: 4, z: 8, core: 2. Of those that a mesh axis runs over, the one named last changes fastest.
Arguments:
- features: bfloat16 [8, 24, 192, 384], P(None, 'lat', 'lon'), may hold values from -6 to 6
- attend_weight: bfloat16 [3, 384, 384], P(None, None, 'head'), may hold values from -0.3125 to 0.3125
- output_weight: bfloat16 [384, 384], P('head'), may hold values from -0.3125 to 0.3125
- bias_table: float32 [64, 12, 3312], P(None, 'head'), may hold values from -3 to 304
- bias_type: int32 [4, 4], P(None, 'lat'), may hold values from 0 to 63
- window_shift: int32 [1], replicated, may hold values from 1 to 11
- grad_out: bfloat16 [8, 24, 192, 384], P(None, 'lat', 'lon'), may hold values from -6 to 6
Outputs:
- feature_grad: bfloat16 [8, 24, 192, 384], P(None, 'lat', 'lon', 'head')
- attend_grad: float32 [3, 384, 384], P(None, None, 'head')
- output_grad: float32 [384, 384], P('head')
- bias_grad: float32 [64, 12, 3312], P(None, 'head')
The draws below stay inside these ranges and needn't reach their ends.
All inputs are finite; a program needn't handle non-finite values.
Results may differ from the reference program's by a relative error of at most 0.01.
Values may be sent and summed in bfloat16 or wider, within the bound.
A program may use at most 128 MiB of HBM per device.

```python
import jax
import jax.numpy as jnp
import numpy as np
from jax import lax

D = 384
HEADS = 12
TYPES = 64
WIN_LEVEL = 2
WIN_LAT = 6
WIN_LON = 12
REL_COUNT = 3312
LEVELS = 8
LAT = 24
LON = 192
LEVEL_WINS = 4
LAT_WINS = 4
N_HEAD = 4


def draw_bias_table(key, part):
    base_key = jax.random.fold_in(key, 11)
    first_key = jax.random.fold_in(base_key, 0)
    table = jnp.clip(jax.random.normal(first_key, (TYPES, HEADS, REL_COUNT), jnp.float32), -3.0, 3.0)
    return table


def with_ends(values, key, smallest, top_value):
    spot = [jax.random.randint(jax.random.fold_in(key, axis), (), 0, length) for axis, length in enumerate(values.shape)]
    main_axis = values.shape.index(max(values.shape))
    next_to = spot[:main_axis] + [(spot[main_axis] + 1) % values.shape[main_axis]] + spot[main_axis + 1:]
    return values.at[tuple(spot)].set(smallest).at[tuple(next_to)].set(top_value)


def levels(rng, extent, shards, least, high):
    gain, own = 1.0, jax.random.fold_in(rng, 6)
    for dim, shards_of in shards:
        heights = jnp.exp(jax.random.uniform(jax.random.fold_in(own, dim), (shards_of,), jnp.float32, least / len(shards), high / len(shards)))
        gain = gain * jnp.repeat(heights, extent[dim] // shards_of).reshape([-1 if axis == dim else 1 for axis in range(len(extent))])
    return gain


def centred(own_key, dims, width, most, cuts=(), held_as=jnp.bfloat16):
    gain = levels(own_key, dims, cuts, -0.22, 0.18) if cuts else 1.0
    entries = jax.random.normal(own_key, dims, jnp.float32) * width * gain
    return jnp.minimum(jnp.maximum(entries, -most), most).astype(held_as)


def setup_inputs(seed: int = 0) -> dict:
    seeds = jax.random.split(jax.random.key(seed), 8)
    return {
        "features": centred(seeds[0], (LEVELS, LAT, LON, D), 1.0, 6.0, ((1, 4), (2, 16))),
        "attend_weight": centred(seeds[1], (3, D, D), D ** -0.5, 0.3125, ((2, 4),)),
        "output_weight": centred(seeds[2], (D, D), D ** -0.5, 0.3125, ((0, 4),)),
        "bias_table": draw_bias_table(jax.random.fold_in(seeds[7], 71), 0),
        "bias_type": with_ends(jax.random.randint(seeds[4], (LEVEL_WINS, LAT_WINS), 0, TYPES), jax.random.fold_in(seeds[4], 1), 0, TYPES - 1).astype(jnp.int32),
        "window_shift": jax.random.randint(seeds[5], (1,), 1, WIN_LON).astype(jnp.int32),
        "grad_out": centred(seeds[6], (LEVELS, LAT, LON, D), 1.0, 6.0, ((1, 4), (2, 16))),
    }


def relative_index(win_level, win_lat, win_lon):
    level_pos, lat_pos, lon_pos = np.meshgrid(np.arange(win_level), np.arange(win_lat), np.arange(win_lon), indexing="ij")
    level_pos = level_pos.reshape(-1)
    lat_pos = lat_pos.reshape(-1)
    lon_pos = lon_pos.reshape(-1)
    pair_level = level_pos[:, None] * win_level + level_pos[None, :]
    pair_lat = lat_pos[:, None] * win_lat + lat_pos[None, :]
    offset_lon = lon_pos[:, None] - lon_pos[None, :] + win_lon - 1
    combined = (pair_level * win_lat * win_lat + pair_lat) * (2 * win_lon - 1) + offset_lon
    return jnp.asarray(combined.reshape(-1).astype(np.int32))


def halve(values):
    return lax.optimization_barrier(values.astype(jnp.bfloat16)).astype(jnp.float32)


def attend_backward(tokens, grad_rows, window_types, attend_weight, output_weight, bias_table, relation):
    outer_count, inner_count, win_tokens, model_width = tokens.shape
    head_count = bias_table.shape[1]
    head_size = attend_weight.shape[2] // head_count
    scaling = head_size ** -0.5
    tokens_full = tokens.astype(jnp.float32)
    grad_full = grad_rows.astype(jnp.float32)
    projected = halve(jnp.einsum("abnd,cdk->cabnk", tokens_full, attend_weight.astype(jnp.float32)))
    split = projected.reshape(3, outer_count, inner_count, win_tokens, head_count, head_size)
    queries, key_rows, values = split[0], split[1], split[2]
    table_rows = jnp.take(bias_table, window_types, axis=0)
    bias_full = jnp.take(table_rows, relation, axis=2).reshape(outer_count, head_count, win_tokens, win_tokens)
    scores = jnp.einsum("abihe,abjhe->abhij", queries, key_rows) * scaling + bias_full[:, None]
    softened = jax.nn.softmax(scores, axis=-1)
    softened_half = halve(softened)
    attended = halve(jnp.einsum("abhij,abjhe->abihe", softened_half, values))
    grad_attended = halve(jnp.einsum("abnd,kd->abnk", grad_full, output_weight.astype(jnp.float32)))
    grad_heads = grad_attended.reshape(outer_count, inner_count, win_tokens, head_count, head_size)
    grad_values = halve(jnp.einsum("abhij,abihe->abjhe", softened_half, grad_heads))
    grad_softened = jnp.einsum("abihe,abjhe->abhij", grad_heads, values)
    grad_scores = softened * (grad_softened - jnp.sum(softened * grad_softened, axis=-1, keepdims=True))
    grad_scores_half = halve(grad_scores)
    grad_queries = halve(jnp.einsum("abhij,abjhe->abihe", grad_scores_half, key_rows) * scaling)
    grad_keys = halve(jnp.einsum("abhij,abihe->abjhe", grad_scores_half, queries) * scaling)
    grad_projected = jnp.stack([grad_queries, grad_keys, grad_values]).reshape(3, outer_count, inner_count, win_tokens, head_count * head_size)
    attended = attended.reshape(outer_count, inner_count, win_tokens, head_count * head_size)
    return attended, grad_projected, grad_scores


def reference(features, attend_weight, output_weight, bias_table, bias_type, window_shift, grad_out):
    offset = window_shift[0]
    rolled = jnp.roll(features, -offset, axis=2)
    rolled_grad = jnp.roll(grad_out, -offset, axis=2)
    relation = relative_index(WIN_LEVEL, WIN_LAT, WIN_LON)
    lon_wins = LON // WIN_LON
    level_wins = LEVELS // WIN_LEVEL
    win_tokens = WIN_LEVEL * WIN_LAT * WIN_LON
    head_count = bias_table.shape[1]
    rel_total = bias_table.shape[2]
    group_cols = D // N_HEAD

    def to_windows(band):
        shaped = band.reshape(level_wins, WIN_LEVEL, WIN_LAT, lon_wins, WIN_LON, D)
        return shaped.transpose(0, 3, 1, 2, 4, 5).reshape(level_wins, lon_wins, win_tokens, D)

    def from_windows(windows):
        shaped = windows.reshape(level_wins, lon_wins, WIN_LEVEL, WIN_LAT, WIN_LON, D)
        return shaped.transpose(0, 2, 3, 1, 4, 5).reshape(LEVELS, WIN_LAT, LON, D)

    def band_step(totals, band_index):
        grad_attend, grad_output, grad_bias = totals
        band_start = band_index * WIN_LAT
        tokens = to_windows(lax.dynamic_slice_in_dim(rolled, band_start, WIN_LAT, 1))
        grad_rows = to_windows(lax.dynamic_slice_in_dim(rolled_grad, band_start, WIN_LAT, 1))
        window_types = lax.dynamic_slice_in_dim(bias_type, band_index, 1, 1)[:, 0].astype(jnp.int32)
        attended, grad_projected, grad_scores = attend_backward(tokens, grad_rows, window_types, attend_weight, output_weight, bias_table, relation)
        tokens_full = tokens.astype(jnp.float32)
        grad_attend = grad_attend + jnp.einsum("abnd,cabnk->cdk", tokens_full, grad_projected)
        grad_output = grad_output + jnp.einsum("abnk,abnd->kd", attended, grad_rows.astype(jnp.float32))
        summed_scores = jnp.sum(grad_scores, axis=1).reshape(-1)
        segment_ids = (window_types[:, None, None] * head_count * rel_total + jnp.arange(head_count, dtype=jnp.int32)[None, :, None] * rel_total + relation[None, None, :]).reshape(-1)
        grad_bias = grad_bias + jax.ops.segment_sum(summed_scores, segment_ids, num_segments=bias_table.shape[0] * head_count * rel_total).reshape(bias_table.shape)
        grouped = grad_projected.reshape(3, level_wins, lon_wins, win_tokens, N_HEAD, group_cols)
        weight_grouped = attend_weight.astype(jnp.float32).reshape(3, D, N_HEAD, group_cols)
        pieces = halve(jnp.einsum("cabngk,cdgk->gabnd", grouped, weight_grouped))
        band_grad = from_windows(jnp.sum(pieces, axis=0)).astype(jnp.bfloat16)
        return (grad_attend, grad_output, grad_bias), band_grad

    start_totals = (jnp.zeros((3, D, D), jnp.float32), jnp.zeros((D, D), jnp.float32), jnp.zeros(bias_table.shape, jnp.float32))
    totals, bands = lax.scan(band_step, start_totals, jnp.arange(LAT // WIN_LAT, dtype=jnp.int32))
    grid_grad = bands.transpose(1, 0, 2, 3, 4).reshape(LEVELS, LAT, LON, D)
    feature_grad = jnp.roll(grid_grad, offset, axis=2)
    return feature_grad, totals[0], totals[1], totals[2]
```

```python
import functools

import jax
import jax.numpy as jnp
from jax import lax
from jax.experimental import pallas as pl
from jax.experimental.pallas import tpu as pltpu
from jax.sharding import PartitionSpec as P

F32 = jnp.float32
BF16 = jnp.bfloat16
HEADS = 3
WINS = 4
WIDTH = 96
HEAD = 32
SLOTS = 12
GRID = 72
TOKENS = 144
MODEL = 384
SPAN = 23
TABLE = 3312
TABLE_PAD = 3328
GROUP = 138
SCALE = HEAD ** (-0.5)
VMEM = pl.BlockSpec(memory_space=pltpu.VMEM)
SMEM = pl.BlockSpec(memory_space=pltpu.SMEM)
ANY = pl.BlockSpec(memory_space=pl.ANY)


def dot(a, b, da, db):
    return lax.dot_general(a, b, (((da,), (db,)), ((), ())), preferred_element_type=F32)


def three(x):
    hi = x.astype(BF16)
    rest = x - hi.astype(F32)
    mid = rest.astype(BF16)
    return hi, mid, (rest - mid.astype(F32)).astype(BF16)


def fold_map(ci, shift):
    rows = lax.broadcasted_iota(jnp.int32, (288, 256), 0)
    lane = lax.broadcasted_iota(jnp.int32, (1, 256), 1)
    block = lane // SLOTS
    cj = lane - block * SLOTS
    wrap = jnp.where(ci < shift, 12, 0) - jnp.where(cj < shift, 12, 0)
    target = block * SPAN + (11 + ci) - cj + wrap
    target = jnp.where(lane < TOKENS, target, -1)
    return jnp.where(rows == target, 1.0, 0.0).astype(BF16)


def expand_bias(types, shift, table, tabw, spread, maps, bias):
    for h in range(HEADS):
        for w in range(WINS):
            n = h * WINS + w
            tabw[n : n + 1, 0:TABLE] = table[h, pl.ds(types[w], 1), :]
    spread[...] = jnp.zeros_like(spread)
    for zi in range(2):
        for ai in range(6):
            for zj in range(2):
                at = zi * 1656 + zj * 828 + ai * GROUP
                spread[zi * 6 + ai, 0:12, zj * GROUP : (zj + 1) * GROUP] = tabw[0:12, at : at + GROUP]
    parts = three(spread[...].reshape(192, 288))
    for ci in range(SLOTS):
        chosen = fold_map(ci, shift)
        maps[ci] = chosen
        full = dot(parts[0], chosen, 1, 0) + dot(parts[1], chosen, 1, 0) + dot(parts[2], chosen, 1, 0)
        for n in range(12):
            for k in range(2):
                bias[k, pl.ds(n * SLOTS + ci, 12, stride=TOKENS), :] = full[
                    n * 16 : n * 16 + 12, k * 128 : (k + 1) * 128
                ]


def bias_kernel(types_ref, shift_ref, table, maps, bias, tabw, spread):
    expand_bias([types_ref[w, 0] for w in range(WINS)], shift_ref[0], table, tabw, spread, maps, bias)


def gather_rows(own, east, shift, scratch):
    for c in range(SLOTS):
        mine = c >= shift
        for a in range(6):
            rows = jnp.where(mine, own[a, c].astype(F32), east[a, c].astype(F32))
            for k in range(3):
                scratch[k, (a * SLOTS + c) * 8 : (a * SLOTS + c + 1) * 8, :] = rows[:, k * 128 : (k + 1) * 128]


def window_rows(scratch, w):
    halves = []
    for z in range(2):
        lanes = [scratch[k, pl.ds(2 * w + z, GRID, stride=8), :] for k in range(3)]
        halves.append(jnp.concatenate(lanes, axis=1))
    return jnp.concatenate(halves, axis=0).astype(BF16)


def only(x, h):
    return jnp.concatenate([x[k * HEAD : (k + 1) * HEAD] if k == h else jnp.zeros((HEAD, x.shape[1]), x.dtype) for k in range(HEADS)], axis=0)


def attend(shift, x, xe, g, ge, wt, wo, maps, bias, sums, folded, piece, xs, gs, wflip, scores, fold):
    gather_rows(x, xe, shift, xs)
    gather_rows(g, ge, shift, gs)
    wts = wt[...].reshape(3 * WIDTH, MODEL)
    wos = wo[...]
    wflip[...] = wts.astype(F32).T.astype(BF16)
    grads = []
    for w in range(WINS):
        xw = window_rows(xs, w)
        gw = window_rows(gs, w)
        proj = dot(wts, xw, 1, 1).astype(BF16)
        qt, kt, vt = proj[0:96], proj[96:192], proj[192:288]
        q = dot(xw, wts[0:WIDTH], 1, 1).astype(BF16)
        dat = dot(wos, gw, 1, 1).astype(BF16)
        da = dot(gw, wos, 1, 1).astype(BF16)
        att, dq, dk, dv = [], [], [], []
        for h in range(HEADS):
            n = h * WINS + w
            rows = slice(n * TOKENS, (n + 1) * TOKENS)
            own = slice(h * HEAD, (h + 1) * HEAD)
            added = jnp.concatenate([bias[0, rows, :], bias[1, rows, 0:16]], axis=1)
            logits = dot(q, only(kt, h), 1, 0) * SCALE + added
            logits = jnp.exp(logits - jnp.max(logits, axis=1, keepdims=True))
            soft = logits / jnp.sum(logits, axis=1, keepdims=True)
            half = soft.astype(BF16)
            att.append(dot(vt[own], half, 1, 1))
            dv.append(dot(dat[own], half, 1, 0))
            gsoft = dot(da, only(vt, h), 1, 0)
            gsc = soft * (gsoft - jnp.sum(soft * gsoft, axis=1, keepdims=True))
            scores[0, rows, :] = gsc[:, 0:128]
            scores[1, rows, 0:16] = gsc[:, 128:144]
            gh = gsc.astype(BF16)
            dq.append(dot(kt[own], gh, 1, 1) * SCALE)
            dk.append(dot(qt[own], gh, 1, 0) * SCALE)
        dproj = jnp.concatenate(dq + dk + dv, axis=0).astype(BF16)
        attended = jnp.concatenate(att, axis=0).astype(BF16)
        top = dot(dproj, xw, 1, 0)
        low = dot(attended, gw, 1, 0)
        if w == 0:
            sums[0:288, :] = top
            sums[288:384, :] = low
        else:
            sums[0:288, :] += top
            sums[288:384, :] += low
        back = dot(wflip[...], dproj, 1, 0).astype(BF16)
        piece[:, w * TOKENS : (w + 1) * TOKENS] = back
    piece[:, 576:640] = jnp.zeros((MODEL, 64), BF16)
    total = None
    for ci in range(SLOTS):
        part = jnp.concatenate(
            [scores[0, pl.ds(ci, TOKENS, stride=SLOTS), :], scores[1, pl.ds(ci, TOKENS, stride=SLOTS), :][:, 0:16]], axis=1
        )
        hi = part.astype(BF16)
        lo = (part - hi.astype(F32)).astype(BF16)
        chosen = maps[ci][:, 0:TOKENS]
        term = dot(hi, chosen, 1, 1) + dot(lo, chosen, 1, 1)
        total = term if total is None else total + term
    for k in range(3):
        wide = min(128, 288 - k * 128)
        fold[k, :, 0:wide] = total[:, k * 128 : k * 128 + wide]
    folded[...] = jnp.zeros_like(folded)
    for zi in range(2):
        for ai in range(6):
            got = [fold[k, pl.ds(zi * 6 + ai, 12, stride=12), :] for k in range(3)]
            line = jnp.concatenate(got, axis=1)
            for zj in range(2):
                at = zi * 1656 + zj * 828 + ai * GROUP
                folded[0:12, at : at + GROUP] = line[:, zj * GROUP : (zj + 1) * GROUP]


def attend_kernel(shift_ref, x, xe, g, ge, wt, wo, maps, bias, sums, folded, piece, xs, gs, wflip, scores, fold):
    attend(shift_ref[0], x, xe, g, ge, wt, wo, maps, bias, sums, folded, piece, xs, gs, wflip, scores, fold)


def scatter_types(types, rows, out):
    lane = lax.broadcasted_iota(jnp.int32, (64, 16), 1)
    row = lax.broadcasted_iota(jnp.int32, (64, 16), 0)
    wanted = jnp.zeros((64, 16), jnp.int32)
    for n in range(16):
        wanted = jnp.where(lane == n, types[n], wanted)
    pick = jnp.where(row == wanted, 1.0, 0.0).astype(BF16)
    for h in range(HEADS):
        parts = three(rows(h))
        out[h] = (dot(pick, parts[0], 1, 0) + dot(pick, parts[1], 1, 0) + dot(pick, parts[2], 1, 0))[:, 0:TABLE]


def finish_kernel(types_ref, shift_ref, fsum, own, west, bias_out, feat_out, lines):
    def rows(h):
        return jnp.concatenate([fsum[q, h * WINS : (h + 1) * WINS, :] for q in range(4)], axis=0)

    scatter_types([types_ref[n % 4, n // 4] for n in range(16)], rows, bias_out)
    place_features(shift_ref[0], own, west, feat_out, lines)


def place_features(shift, own, west, feat_out, lines):
    lane = lax.broadcasted_iota(jnp.int32, (1, TOKENS), 1)
    mine = (lane - (lane // SLOTS) * SLOTS) >= shift
    for w in range(WINS):
        cols = slice(w * TOKENS, (w + 1) * TOKENS)
        both = jnp.where(mine, own[:, cols].astype(F32), west[:, cols].astype(F32))
        both = jnp.concatenate([both, jnp.zeros((32, TOKENS), F32)], axis=0).T
        for z in range(2):
            lines[pl.ds(2 * w + z, GRID, stride=8), :] = both[z * GRID : (z + 1) * GRID]
    for a in range(6):
        for c in range(SLOTS):
            at = (a * SLOTS + c) * 8
            feat_out[a, c] = lines[at : at + 8, 0:WIDTH].astype(BF16)


def per_device(features, attend_weight, output_weight, bias_table, bias_type, window_shift, grad_out):
    x = features.transpose(1, 2, 0, 3)
    g = grad_out.transpose(1, 2, 0, 3)
    wt = attend_weight.transpose(0, 2, 1)
    table = bias_table.transpose(1, 0, 2)
    count = lax.axis_size("lon")
    west = [(i, (i - 1) % count) for i in range(count)]
    east = [(i, (i + 1) % count) for i in range(count)]
    xe = lax.ppermute(x, "lon", west)
    ge = lax.ppermute(g, "lon", west)
    maps, bias = pl.pallas_call(
        bias_kernel,
        out_shape=(jax.ShapeDtypeStruct((12, 288, 256), BF16), jax.ShapeDtypeStruct((2, 1728, 128), F32)),
        in_specs=[SMEM, SMEM, VMEM],
        out_specs=(VMEM, VMEM),
        scratch_shapes=[pltpu.VMEM((16, TABLE_PAD), F32), pltpu.VMEM((12, 16, 288), F32)],
        compiler_params=pltpu.CompilerParams(vmem_limit_bytes=40 << 20),
        cost_estimate=pl.CostEstimate(flops=10**10, bytes_accessed=10**7, transcendentals=0),
        name="expand_bias",
    )(bias_type, window_shift, table)
    sums, folded, piece = pl.pallas_call(
        attend_kernel,
        out_shape=(
            jax.ShapeDtypeStruct((MODEL, MODEL), F32),
            jax.ShapeDtypeStruct((16, TABLE_PAD), F32),
            jax.ShapeDtypeStruct((MODEL, 640), BF16),
        ),
        in_specs=[SMEM] + [VMEM] * 8,
        out_specs=(VMEM, VMEM, VMEM),
        scratch_shapes=[
            pltpu.VMEM((3, 576, 128), F32),
            pltpu.VMEM((3, 576, 128), F32),
            pltpu.VMEM((MODEL, 288), BF16),
            pltpu.VMEM((2, 1728, 128), F32),
            pltpu.VMEM((3, TOKENS, 128), F32),
        ],
        compiler_params=pltpu.CompilerParams(vmem_limit_bytes=48 << 20),
        name="attend_backward",
    )(window_shift, x, xe, g, ge, wt, output_weight, maps, bias)
    blocks = lax.all_to_all(piece.reshape(4, WIDTH, 640), "head", 0, 0, tiled=True)
    own = jnp.sum(blocks.astype(F32), axis=0).astype(BF16)
    borrowed = lax.ppermute(own, "lon", east)
    sums = lax.psum(sums, ("lon", "lat"))
    folded = lax.psum(folded, "lon")
    folded = lax.all_gather(folded, "lat")
    types = lax.all_gather(bias_type[:, 0], "lat").T
    bias_grad, feat = pl.pallas_call(
        finish_kernel,
        out_shape=(jax.ShapeDtypeStruct((3, 64, TABLE), F32), jax.ShapeDtypeStruct((6, SLOTS, 8, WIDTH), BF16)),
        in_specs=[SMEM, SMEM, VMEM, VMEM, VMEM],
        out_specs=(VMEM, VMEM),
        scratch_shapes=[pltpu.VMEM((576, 128), F32)],
        compiler_params=pltpu.CompilerParams(vmem_limit_bytes=40 << 20),
        name="finish",
    )(types, window_shift, folded, own, borrowed)
    return (
        feat.transpose(2, 0, 1, 3),
        sums[0:288].reshape(3, WIDTH, MODEL).transpose(0, 2, 1),
        sums[288:384],
        bias_grad.transpose(1, 0, 2),
    )


def solution(mesh):
    placed = (
        P(None, "lat", "lon", None),
        P(None, None, "head"),
        P("head", None),
        P(None, "head", None),
        P(None, "lat"),
        P(),
        P(None, "lat", "lon", None),
    )
    return jax.shard_map(
        per_device,
        mesh=mesh,
        in_specs=placed,
        out_specs=(
            P(None, "lat", "lon", "head"),
            P(None, None, "head"),
            P("head", None),
            P(None, "head", None),
        ),
        check_vma=False,
    )
```

```python
import functools

import jax
import jax.numpy as jnp
from jax import lax
from jax.experimental import pallas as pl
from jax.experimental.pallas import tpu as pltpu
from jax.sharding import PartitionSpec as P

F32 = jnp.float32
BF16 = jnp.bfloat16
HEADS = 3
WINS = 4
WIDTH = 96
HEAD = 32
SLOTS = 12
GRID = 72
TOKENS = 144
MODEL = 384
SPAN = 23
TABLE = 3312
TABLE_PAD = 3328
GROUP = 138
SCALE = HEAD ** (-0.5)
VMEM = pl.BlockSpec(memory_space=pltpu.VMEM)
SMEM = pl.BlockSpec(memory_space=pltpu.SMEM)
ANY = pl.BlockSpec(memory_space=pl.ANY)


def dot(a, b, da, db):
    return lax.dot_general(a, b, (((da,), (db,)), ((), ())), preferred_element_type=F32)


def three(x):
    hi = x.astype(BF16)
    rest = x - hi.astype(F32)
    mid = rest.astype(BF16)
    return hi, mid, (rest - mid.astype(F32)).astype(BF16)


def fold_map(ci, shift):
    rows = lax.broadcasted_iota(jnp.int32, (288, 256), 0)
    lane = lax.broadcasted_iota(jnp.int32, (1, 256), 1)
    block = lane // SLOTS
    cj = lane - block * SLOTS
    wrap = jnp.where(ci < shift, 12, 0) - jnp.where(cj < shift, 12, 0)
    target = block * SPAN + (11 + ci) - cj + wrap
    target = jnp.where(lane < TOKENS, target, -1)
    return jnp.where(rows == target, 1.0, 0.0).astype(BF16)


def expand_bias(types, shift, table, tabw, spread, maps, bias):
    for h in range(HEADS):
        for w in range(WINS):
            n = h * WINS + w
            tabw[n : n + 1, 0:TABLE] = table[h, pl.ds(types[w], 1), :]
    spread[...] = jnp.zeros_like(spread)
    for zi in range(2):
        for ai in range(6):
            for zj in range(2):
                at = zi * 1656 + zj * 828 + ai * GROUP
                spread[zi * 6 + ai, 0:12, zj * GROUP : (zj + 1) * GROUP] = tabw[0:12, at : at + GROUP]
    parts = three(spread[...].reshape(192, 288))
    for ci in range(SLOTS):
        chosen = fold_map(ci, shift)
        maps[ci] = chosen
        full = dot(parts[0], chosen, 1, 0) + dot(parts[1], chosen, 1, 0) + dot(parts[2], chosen, 1, 0)
        for n in range(12):
            for k in range(2):
                bias[k, pl.ds(n * SLOTS + ci, 12, stride=TOKENS), :] = full[
                    n * 16 : n * 16 + 12, k * 128 : (k + 1) * 128
                ]


def bias_kernel(types_ref, shift_ref, table, maps, bias, tabw, spread):
    expand_bias([types_ref[w, 0] for w in range(WINS)], shift_ref[0], table, tabw, spread, maps, bias)


def gather_rows(own, east, shift, scratch):
    for c in range(SLOTS):
        mine = c >= shift
        for a in range(6):
            rows = jnp.where(mine, own[a, c].astype(F32), east[a, c].astype(F32))
            for k in range(3):
                scratch[k, (a * SLOTS + c) * 8 : (a * SLOTS + c + 1) * 8, :] = rows[:, k * 128 : (k + 1) * 128]


def window_rows(scratch, w):
    halves = []
    for z in range(2):
        lanes = [scratch[k, pl.ds(2 * w + z, GRID, stride=8), :] for k in range(3)]
        halves.append(jnp.concatenate(lanes, axis=1))
    return jnp.concatenate(halves, axis=0).astype(BF16)


def only(x, h):
    return jnp.concatenate([x[k * HEAD : (k + 1) * HEAD] if k == h else jnp.zeros((HEAD, x.shape[1]), x.dtype) for k in range(HEADS)], axis=0)


def attend(types, shift, x, xe, g, ge, wt, wo, maps, bias, sums_out, folded_out, piece, xs, gs, wflip, scores, fold, sums, folded):
    gather_rows(x, xe, shift, xs)
    gather_rows(g, ge, shift, gs)
    wts = wt[...].reshape(3 * WIDTH, MODEL)
    wos = wo[...]
    wflip[...] = wts.astype(F32).T.astype(BF16)
    grads = []
    for w in range(WINS):
        xw = window_rows(xs, w)
        gw = window_rows(gs, w)
        proj = dot(wts, xw, 1, 1).astype(BF16)
        qt, kt, vt = proj[0:96], proj[96:192], proj[192:288]
        q = dot(xw, wts[0:WIDTH], 1, 1).astype(BF16)
        dat = dot(wos, gw, 1, 1).astype(BF16)
        da = dot(gw, wos, 1, 1).astype(BF16)
        att, dq, dk, dv = [], [], [], []
        for h in range(HEADS):
            n = h * WINS + w
            rows = slice(n * TOKENS, (n + 1) * TOKENS)
            own = slice(h * HEAD, (h + 1) * HEAD)
            added = jnp.concatenate([bias[0, rows, :], bias[1, rows, 0:16]], axis=1)
            logits = dot(q, only(kt, h), 1, 0) * SCALE + added
            logits = jnp.exp(logits - jnp.max(logits, axis=1, keepdims=True))
            soft = logits / jnp.sum(logits, axis=1, keepdims=True)
            half = soft.astype(BF16)
            att.append(dot(vt[own], half, 1, 1))
            dv.append(dot(dat[own], half, 1, 0))
            gsoft = dot(da, only(vt, h), 1, 0)
            gsc = soft * (gsoft - jnp.sum(soft * gsoft, axis=1, keepdims=True))
            scores[0, rows, :] = gsc[:, 0:128]
            scores[1, rows, 0:16] = gsc[:, 128:144]
            gh = gsc.astype(BF16)
            dq.append(dot(kt[own], gh, 1, 1) * SCALE)
            dk.append(dot(qt[own], gh, 1, 0) * SCALE)
        dproj = jnp.concatenate(dq + dk + dv, axis=0).astype(BF16)
        attended = jnp.concatenate(att, axis=0).astype(BF16)
        top = dot(dproj, xw, 1, 0)
        low = dot(attended, gw, 1, 0)
        if w == 0:
            sums[0:288, :] = top
            sums[288:384, :] = low
        else:
            sums[0:288, :] += top
            sums[288:384, :] += low
        back = dot(wflip[...], dproj, 1, 0).astype(BF16)
        for r in range(4):
            piece[r, :, w * TOKENS : (w + 1) * TOKENS] = back[r * WIDTH : (r + 1) * WIDTH]
    for r in range(4):
        piece[r, :, 576:640] = jnp.zeros((WIDTH, 64), BF16)
    for i in range(8):
        sums_out[i] = sums[i * 48 : (i + 1) * 48, :].astype(BF16)
    total = None
    for ci in range(SLOTS):
        part = jnp.concatenate(
            [scores[0, pl.ds(ci, TOKENS, stride=SLOTS), :], scores[1, pl.ds(ci, TOKENS, stride=SLOTS), :][:, 0:16]], axis=1
        )
        hi = part.astype(BF16)
        lo = (part - hi.astype(F32)).astype(BF16)
        chosen = maps[ci][:, 0:TOKENS]
        term = dot(hi, chosen, 1, 1) + dot(lo, chosen, 1, 1)
        total = term if total is None else total + term
    for k in range(3):
        wide = min(128, 288 - k * 128)
        fold[k, :, 0:wide] = total[:, k * 128 : k * 128 + wide]
    folded[...] = jnp.zeros_like(folded)
    for zi in range(2):
        for ai in range(6):
            got = [fold[k, pl.ds(zi * 6 + ai, 12, stride=12), :] for k in range(3)]
            line = jnp.concatenate(got, axis=1)
            for zj in range(2):
                at = zi * 1656 + zj * 828 + ai * GROUP
                folded[0:12, at : at + GROUP] = line[:, zj * GROUP : (zj + 1) * GROUP]
    row = lax.broadcasted_iota(jnp.int32, (16, 512), 0)
    marks = jnp.zeros((16, 512), jnp.int32)
    for w in range(WINS):
        marks = jnp.where(row == 12 + w, types[w], marks)
    marks = marks.astype(F32)
    for z in range(8):
        part = folded[:, z * 512 : (z + 1) * 512]
        folded_out[z] = jnp.where(row < 12, part, marks).astype(BF16)


def attend_kernel(types_ref, shift_ref, *refs):
    attend([types_ref[w, 0] for w in range(WINS)], shift_ref[0], *refs)


def scatter_types(lines, out):
    marks = jnp.concatenate([lines[q][12:16, 0:1] for q in range(4)], axis=0) * 0.0625
    lane = lax.broadcasted_iota(jnp.int32, (16, 128), 1).astype(F32)
    pick = jnp.where(lane == marks, 1.0, 0.0).T[0:64].astype(BF16)
    for h in range(HEADS):
        rows = jnp.concatenate([lines[q][h * WINS : (h + 1) * WINS, 0:TABLE_PAD] for q in range(4)], axis=0)
        out[h] = dot(pick, rows.astype(BF16), 1, 0)[:, 0:TABLE]


def finish_kernel(shift_ref, sums, folded, own, west, attend_out, output_out, bias_out, feat_out, lines):
    for i in range(8):
        part = sums[i].astype(F32)
        if i < 6:
            attend_out[i // 2, (i % 2) * 48 : (i % 2) * 48 + 48, :] = part
        else:
            output_out[(i - 6) * 48 : (i - 5) * 48, :] = part
    whole = [
        jnp.concatenate([folded[xh * 4 + q, z] for z in range(7) for xh in range(2)], axis=1).astype(F32) for q in range(4)
    ]
    scatter_types(whole, bias_out)
    place_features(shift_ref[0], own, west, feat_out, lines)


def place_features(shift, own, west, feat_out, lines):
    lane = lax.broadcasted_iota(jnp.int32, (1, TOKENS), 1)
    mine = (lane - (lane // SLOTS) * SLOTS) >= shift
    for w in range(WINS):
        cols = slice(w * TOKENS, (w + 1) * TOKENS)
        both = jnp.where(mine, own[:, cols].astype(F32), west[:, cols].astype(F32))
        both = jnp.concatenate([both, jnp.zeros((32, TOKENS), F32)], axis=0).T
        for z in range(2):
            lines[pl.ds(2 * w + z, GRID, stride=8), :] = both[z * GRID : (z + 1) * GRID]
    for a in range(6):
        for c in range(SLOTS):
            at = (a * SLOTS + c) * 8
            feat_out[a, c] = lines[at : at + 8, 0:WIDTH].astype(BF16)


ATTEND_SCRATCH = [
    pltpu.VMEM((3, 576, 128), F32),
    pltpu.VMEM((3, 576, 128), F32),
    pltpu.VMEM((MODEL, 288), BF16),
    pltpu.VMEM((2, 1728, 128), F32),
    pltpu.VMEM((3, TOKENS, 128), F32),
    pltpu.VMEM((MODEL, MODEL), F32),
    pltpu.VMEM((16, 4096), F32),
]


class Links:
    def __init__(self, send, recv):
        self.send, self.recv, self.used, self.sent = send, recv, 0, []

    def copy(self, src, dst, to):
        k = self.used
        self.used += 1
        return pltpu.make_async_remote_copy(
            src_ref=src,
            dst_ref=dst,
            send_sem=self.send.at[k],
            recv_sem=self.recv.at[k],
            device_id=to,
            device_id_type=pl.DeviceIdType.MESH,
        )

    def start(self, src, dst, to):
        made = self.copy(src, dst, to)
        made.start()
        self.sent.append(made)
        return made

    def finish(self):
        for made in self.sent:
            made.wait_send()


def place():
    lon, lat, head = lax.axis_index("lon"), lax.axis_index("lat"), lax.axis_index("head")
    z, high = lon // 2, lon % 2
    low, core = lat // 2, lat % 2
    return lon, lat, head, z, high, high * 2 + low, core


def at_grid(z, x, core):
    return {"lon": z * 2 + x // 2, "lat": (x % 2) * 2 + core}


def meet(peers):
    barrier = pltpu.get_barrier_semaphore()
    for peer in peers:
        pl.semaphore_signal(barrier, inc=1, device_id=peer, device_id_type=pl.DeviceIdType.MESH)
    pl.semaphore_wait(barrier, len(peers))


def reduce_body(net, sums, folded, piece, a_out, f_out, own_out, west_out, a1, f1, p1, a2s, a2, f2s, f2, a3, f3):
    lon, lat, head, z, high, x, core = place()
    xc = x * 2 + core

    def zs(k):
        return {"lon": ((z + k) % 8) * 2 + high}

    def xcs(k):
        other = (xc + k) % 8
        return at_grid(z, other // 2, other % 2)

    one = []
    for k in range(1, 8):
        one.append(net.start(sums.at[(xc + k) % 8], a1.at[k - 1], xcs(k)))
    two = []
    for k in range(1, 8):
        two.append(net.start(folded.at[(z + k) % 8], f1.at[k - 1], zs(k)))
    pieces = []
    for k in range(1, 4):
        pieces.append(net.start(piece.at[(head + k) % 4], p1.at[k - 1], {"head": (head + k) % 4}))

    total = sums[xc].astype(F32)
    for k in range(7):
        one[k].wait_recv()
        total = total + a1[k].astype(F32)
    for k in range(8):
        a2s[k, 0:6, :] = total[k * 6 : (k + 1) * 6]
        a2s[k, 6:8, :] = jnp.zeros((2, MODEL), F32)
    three_ = []
    for k in range(1, 8):
        three_.append(net.start(a2s.at[(z + k) % 8], a2.at[k - 1], zs(k)))

    lines = folded[z].astype(F32)
    for k in range(7):
        two[k].wait_recv()
        lines = lines + f1[k].astype(F32)
    f2s[0] = lines[:, 0:256].astype(BF16)
    f2s[1] = lines[:, 256:512].astype(BF16)
    four = net.start(f2s.at[1 - high], f2, {"lon": z * 2 + 1 - high})

    feat = piece[head].astype(F32)
    for k in range(3):
        pieces[k].wait_recv()
        feat = feat + p1[k].astype(F32)
    own_out[...] = feat.astype(BF16)
    back = net.start(own_out, west_out, {"lon": (lon + 1) % 16})

    four.wait_recv()
    mine = jnp.where(high == 0, lines[:, 0:256], lines[:, 256:512]) + f2[...].astype(F32)
    f3[z] = mine.astype(BF16)
    five = []
    for k in range(1, 8):
        five.append(net.start(f3.at[z], f3.at[z], zs(k)))

    block = a2s[z]
    for k in range(7):
        three_[k].wait_recv()
        block = block + a2[k]
    a3[z] = block
    six = []
    for k in range(1, 8):
        six.append(net.start(a3.at[z], a3.at[z], zs(k)))

    for k in range(7):
        six[k].wait_recv()
    a_out[xc] = jnp.concatenate([a3[k][0:6] for k in range(8)], axis=0).astype(BF16)
    partner = at_grid(z, x, 1 - core)
    arrive = []
    for k in range(1, 4):
        arrive.append(net.start(a_out.at[xc], a_out.at[xc], at_grid(z, (x + k) % 4, core)))
    cross = [net.start(a_out.at[xc], a_out.at[xc], partner)]
    for k in range(7):
        five[k].wait_recv()
    f_out[xc] = f3[...]
    arrive_f = []
    for k in range(1, 4):
        arrive_f.append(net.start(f3, f_out.at[xc], at_grid(z, (x + k) % 4, core)))
    cross.append(net.start(f3, f_out.at[xc], partner))
    for k in range(1, 4):
        there = ((x + 4 - k) % 4) * 2 + core
        arrive[k - 1].wait_recv()
        cross.append(net.start(a_out.at[there], a_out.at[there], partner))
    for k in range(1, 4):
        there = ((x + 4 - k) % 4) * 2 + core
        arrive_f[k - 1].wait_recv()
        cross.append(net.start(f_out.at[there], f_out.at[there], partner))
    back.wait_recv()
    for made in cross:
        made.wait_recv()


REDUCE_SCRATCH = [
    pltpu.VMEM((7, 48, MODEL), BF16),
    pltpu.VMEM((7, 16, 512), BF16),
    pltpu.VMEM((3, WIDTH, 640), BF16),
    pltpu.VMEM((8, 8, MODEL), F32),
    pltpu.VMEM((7, 8, MODEL), F32),
    pltpu.VMEM((2, 16, 256), BF16),
    pltpu.VMEM((16, 256), BF16),
    pltpu.VMEM((8, 8, MODEL), F32),
    pltpu.VMEM((8, 16, 256), BF16),
]


def reduce_peers():
    lon, lat, head, z, high, x, core = place()
    xc = x * 2 + core
    peers = [{"lon": ((z + k) % 8) * 2 + high} for k in range(1, 8)]
    peers += [at_grid(z, ((xc + k) % 8) // 2, (xc + k) % 2) for k in range(1, 8)]
    peers += [{"head": (head + k) % 4} for k in range(1, 4)]
    peers += [{"lon": (lon + 1) % 16}, {"lon": (lon + 15) % 16}]
    return peers


def reduce_kernel(sums, folded, piece, a_out, f_out, own_out, west_out, *scratch):
    meet(reduce_peers())
    net = Links(*scratch[-2:])
    reduce_body(net, sums, folded, piece, a_out, f_out, own_out, west_out, *scratch[:-2])
    net.finish()


def per_device(features, attend_weight, output_weight, bias_table, bias_type, window_shift, grad_out):
    x = features.transpose(1, 2, 0, 3)
    g = grad_out.transpose(1, 2, 0, 3)
    wt = attend_weight.transpose(0, 2, 1)
    table = bias_table.transpose(1, 0, 2)
    count = lax.axis_size("lon")
    west = [(i, (i - 1) % count) for i in range(count)]
    xe = lax.ppermute(x, "lon", west)
    ge = lax.ppermute(g, "lon", west)
    maps, bias = pl.pallas_call(
        bias_kernel,
        out_shape=(jax.ShapeDtypeStruct((12, 288, 256), BF16), jax.ShapeDtypeStruct((2, 1728, 128), F32)),
        in_specs=[SMEM, SMEM, VMEM],
        out_specs=(VMEM, VMEM),
        scratch_shapes=[pltpu.VMEM((16, TABLE_PAD), F32), pltpu.VMEM((12, 16, 288), F32)],
        compiler_params=pltpu.CompilerParams(vmem_limit_bytes=40 << 20),
        cost_estimate=pl.CostEstimate(flops=10**10, bytes_accessed=10**7, transcendentals=0),
        name="expand_bias",
    )(bias_type, window_shift, table)
    sums, folded, piece = pl.pallas_call(
        attend_kernel,
        out_shape=(
            jax.ShapeDtypeStruct((8, 48, MODEL), BF16),
            jax.ShapeDtypeStruct((8, 16, 512), BF16),
            jax.ShapeDtypeStruct((4, WIDTH, 640), BF16),
        ),
        in_specs=[SMEM] * 2 + [VMEM] * 8,
        out_specs=(VMEM, VMEM, VMEM),
        scratch_shapes=ATTEND_SCRATCH,
        compiler_params=pltpu.CompilerParams(vmem_limit_bytes=48 << 20),
        name="attend_backward",
    )(bias_type, window_shift, x, xe, g, ge, wt, output_weight, maps, bias)
    sums, folded, own, borrowed = pl.pallas_call(
        reduce_kernel,
        out_shape=(
            jax.ShapeDtypeStruct((8, 48, MODEL), BF16),
            jax.ShapeDtypeStruct((8, 8, 16, 256), BF16),
            jax.ShapeDtypeStruct((WIDTH, 640), BF16),
            jax.ShapeDtypeStruct((WIDTH, 640), BF16),
        ),
        in_specs=[VMEM] * 3,
        out_specs=(VMEM,) * 4,
        scratch_shapes=REDUCE_SCRATCH + [pltpu.SemaphoreType.DMA((64,)), pltpu.SemaphoreType.DMA((64,))],
        compiler_params=pltpu.CompilerParams(vmem_limit_bytes=40 << 20, collective_id=1, has_side_effects=True),
        name="reduce_gradients",
    )(sums, folded, piece)
    return finish(window_shift, sums, folded, own, borrowed)


def finish(window_shift, sums, folded, own, borrowed):
    attend_grad, output_grad, bias_grad, feat = pl.pallas_call(
        finish_kernel,
        out_shape=(
            jax.ShapeDtypeStruct((3, WIDTH, MODEL), F32),
            jax.ShapeDtypeStruct((WIDTH, MODEL), F32),
            jax.ShapeDtypeStruct((3, 64, TABLE), F32),
            jax.ShapeDtypeStruct((6, SLOTS, 8, WIDTH), BF16),
        ),
        in_specs=[SMEM, VMEM, VMEM, VMEM, VMEM],
        out_specs=(VMEM,) * 4,
        scratch_shapes=[pltpu.VMEM((576, 128), F32)],
        compiler_params=pltpu.CompilerParams(vmem_limit_bytes=40 << 20),
        name="finish",
    )(window_shift, sums, folded, own, borrowed)
    return (
        feat.transpose(2, 0, 1, 3),
        attend_grad.transpose(0, 2, 1),
        output_grad,
        bias_grad.transpose(1, 0, 2),
    )


def solution(mesh):
    placed = (
        P(None, "lat", "lon", None),
        P(None, None, "head"),
        P("head", None),
        P(None, "head", None),
        P(None, "lat"),
        P(),
        P(None, "lat", "lon", None),
    )
    return jax.shard_map(
        per_device,
        mesh=mesh,
        in_specs=placed,
        out_specs=(
            P(None, "lat", "lon", "head"),
            P(None, None, "head"),
            P("head", None),
            P(None, "head", None),
        ),
        check_vma=False,
    )
```

```python
import functools

import jax
import jax.numpy as jnp
from jax import lax
from jax.experimental import pallas as pl
from jax.experimental.pallas import tpu as pltpu
from jax.sharding import PartitionSpec as P

F32 = jnp.float32
BF16 = jnp.bfloat16
HEADS = 3
WINS = 4
WIDTH = 96
HEAD = 32
SLOTS = 12
GRID = 72
TOKENS = 144
MODEL = 384
SPAN = 23
TABLE = 3312
TABLE_PAD = 3328
GROUP = 138
SCALE = HEAD ** (-0.5)
VMEM = pl.BlockSpec(memory_space=pltpu.VMEM)
SMEM = pl.BlockSpec(memory_space=pltpu.SMEM)
ANY = pl.BlockSpec(memory_space=pl.ANY)


def dot(a, b, da, db):
    return lax.dot_general(a, b, (((da,), (db,)), ((), ())), preferred_element_type=F32)


def three(x):
    hi = x.astype(BF16)
    rest = x - hi.astype(F32)
    mid = rest.astype(BF16)
    return hi, mid, (rest - mid.astype(F32)).astype(BF16)


def fold_map(ci, shift):
    rows = lax.broadcasted_iota(jnp.int32, (288, 256), 0)
    lane = lax.broadcasted_iota(jnp.int32, (1, 256), 1)
    block = lane // SLOTS
    cj = lane - block * SLOTS
    wrap = jnp.where(ci < shift, 12, 0) - jnp.where(cj < shift, 12, 0)
    target = block * SPAN + (11 + ci) - cj + wrap
    target = jnp.where(lane < TOKENS, target, -1)
    return jnp.where(rows == target, 1.0, 0.0).astype(BF16)


def expand_bias(types, shift, table, tabw, spread, maps, bias):
    for h in range(HEADS):
        for w in range(WINS):
            n = h * WINS + w
            tabw[n : n + 1, 0:TABLE] = table[h, pl.ds(types[w], 1), :]
    spread[...] = jnp.zeros_like(spread)
    for zi in range(2):
        for ai in range(6):
            for zj in range(2):
                at = zi * 1656 + zj * 828 + ai * GROUP
                spread[zi * 6 + ai, 0:12, zj * GROUP : (zj + 1) * GROUP] = tabw[0:12, at : at + GROUP]
    parts = three(spread[...].reshape(192, 288))
    for ci in range(SLOTS):
        chosen = fold_map(ci, shift)
        maps[ci] = chosen
        full = dot(parts[0], chosen, 1, 0) + dot(parts[1], chosen, 1, 0) + dot(parts[2], chosen, 1, 0)
        for n in range(12):
            for k in range(2):
                bias[k, pl.ds(n * SLOTS + ci, 12, stride=TOKENS), :] = full[
                    n * 16 : n * 16 + 12, k * 128 : (k + 1) * 128
                ]


def window_rows(scratch, w):
    halves = []
    for z in range(2):
        lanes = [scratch[k, pl.ds(2 * w + z, GRID, stride=8), :] for k in range(3)]
        halves.append(jnp.concatenate(lanes, axis=1))
    return jnp.concatenate(halves, axis=0).astype(BF16)


def place_rows(own, borrowed, shift, scratch, first, slots):
    for c in slots:
        for a in range(6):
            rows = own[a, c].astype(F32)
            if borrowed is not None:
                keep = c >= shift if first == 0 else c < shift
                rows = jnp.where(keep, rows, borrowed[a, c - first].astype(F32))
            for k in range(3):
                scratch[k, (a * SLOTS + c) * 8 : (a * SLOTS + c + 1) * 8, :] = rows[:, k * 128 : (k + 1) * 128]


def only(x, h):
    return jnp.concatenate([x[k * HEAD : (k + 1) * HEAD] if k == h else jnp.zeros((HEAD, x.shape[1]), x.dtype) for k in range(HEADS)], axis=0)


def forward(xs, wts, bias, qs, proj_out, softs, atts):
    for w in range(WINS):
        xw = window_rows(xs, w)
        proj = dot(wts, xw, 1, 1).astype(BF16)
        proj_out[w] = proj
        q = dot(xw, wts[0:WIDTH], 1, 1).astype(BF16)
        kt, vt = proj[96:192], proj[192:288]
        att = []
        for h in range(HEADS):
            n = h * WINS + w
            rows = slice(n * TOKENS, (n + 1) * TOKENS)
            added = jnp.concatenate([bias[0, rows, :], bias[1, rows, 0:16]], axis=1)
            logits = dot(q, only(kt, h), 1, 0) * SCALE + added
            logits = jnp.exp(logits - jnp.max(logits, axis=1, keepdims=True))
            soft = logits / jnp.sum(logits, axis=1, keepdims=True)
            softs[n] = soft
            att.append(dot(vt[h * HEAD : (h + 1) * HEAD], soft.astype(BF16), 1, 1))
        atts[w] = jnp.concatenate(att, axis=0).astype(BF16)


def backward(xs, gs, wos, proj_in, softs, atts, scores, sums, dprojs):
    for w in range(WINS):
        xw = window_rows(xs, w)
        gw = window_rows(gs, w)
        proj = proj_in[w]
        qt, kt, vt = proj[0:96], proj[96:192], proj[192:288]
        dat = dot(wos, gw, 1, 1).astype(BF16)
        da = dot(gw, wos, 1, 1).astype(BF16)
        dq, dk, dv = [], [], []
        for h in range(HEADS):
            n = h * WINS + w
            rows = slice(n * TOKENS, (n + 1) * TOKENS)
            own = slice(h * HEAD, (h + 1) * HEAD)
            soft = softs[n]
            dv.append(dot(dat[own], soft.astype(BF16), 1, 0))
            gsoft = dot(da, only(vt, h), 1, 0)
            gsc = soft * (gsoft - jnp.sum(soft * gsoft, axis=1, keepdims=True))
            scores[0, rows, :] = gsc[:, 0:128]
            scores[1, rows, 0:16] = gsc[:, 128:144]
            gh = gsc.astype(BF16)
            dq.append(dot(kt[own], gh, 1, 1) * SCALE)
            dk.append(dot(qt[own], gh, 1, 0) * SCALE)
        dproj = jnp.concatenate(dq + dk + dv, axis=0).astype(BF16)
        dprojs[w] = dproj
        top = dot(dproj, xw, 1, 0)
        low = dot(atts[w], gw, 1, 0)
        if w == 0:
            sums[0:288, :] = top
            sums[288:384, :] = low
        else:
            sums[0:288, :] += top
            sums[288:384, :] += low


def fold_scores(types, scores, maps, fold, folded, folded_out):
    total = None
    for ci in range(SLOTS):
        part = jnp.concatenate(
            [scores[0, pl.ds(ci, TOKENS, stride=SLOTS), :], scores[1, pl.ds(ci, TOKENS, stride=SLOTS), :][:, 0:16]], axis=1
        )
        hi = part.astype(BF16)
        lo = (part - hi.astype(F32)).astype(BF16)
        chosen = maps[ci][:, 0:TOKENS]
        term = dot(hi, chosen, 1, 1) + dot(lo, chosen, 1, 1)
        total = term if total is None else total + term
    for k in range(3):
        wide = min(128, 288 - k * 128)
        fold[k, :, 0:wide] = total[:, k * 128 : k * 128 + wide]
    folded[...] = jnp.zeros_like(folded)
    for zi in range(2):
        for ai in range(6):
            got = [fold[k, pl.ds(zi * 6 + ai, 12, stride=12), :] for k in range(3)]
            line = jnp.concatenate(got, axis=1)
            for zj in range(2):
                at = zi * 1656 + zj * 828 + ai * GROUP
                folded[0:12, at : at + GROUP] = line[:, zj * GROUP : (zj + 1) * GROUP]
    row = lax.broadcasted_iota(jnp.int32, (16, 512), 0)
    marks = jnp.zeros((16, 512), jnp.int32)
    for w in range(WINS):
        marks = jnp.where(row == 12 + w, types[w], marks)
    marks = marks.astype(F32)
    for z in range(8):
        part = folded[:, z * 512 : (z + 1) * 512]
        folded_out[z] = jnp.where(row < 12, part, marks).astype(BF16)


def pieces_out(wflip, dprojs, piece):
    for w in range(WINS):
        back = dot(wflip[...], dprojs[w], 1, 0).astype(BF16)
        for r in range(4):
            piece[r, :, w * TOKENS : (w + 1) * TOKENS] = back[r * WIDTH : (r + 1) * WIDTH]
    for r in range(4):
        piece[r, :, 576:640] = jnp.zeros((WIDTH, 64), BF16)


def scatter_types(lines, out):
    marks = jnp.concatenate([lines[q][12:16, 0:1] for q in range(4)], axis=0) * 0.0625
    lane = lax.broadcasted_iota(jnp.int32, (16, 128), 1).astype(F32)
    pick = jnp.where(lane == marks, 1.0, 0.0).T[0:64].astype(BF16)
    for h in range(HEADS):
        rows = jnp.concatenate([lines[q][h * WINS : (h + 1) * WINS, 0:TABLE_PAD] for q in range(4)], axis=0)
        out[h] = dot(pick, rows.astype(BF16), 1, 0)[:, 0:TABLE]


def finish_kernel(shift_ref, sums, folded, own, west, attend_out, output_out, bias_out, feat_out, lines):
    for i in range(8):
        part = sums[i].astype(F32)
        if i < 6:
            attend_out[i // 2, (i % 2) * 48 : (i % 2) * 48 + 48, :] = part
        else:
            output_out[(i - 6) * 48 : (i - 5) * 48, :] = part
    whole = [
        jnp.concatenate([folded[xh * 4 + q, z] for z in range(7) for xh in range(2)], axis=1).astype(F32) for q in range(4)
    ]
    scatter_types(whole, bias_out)
    place_features(shift_ref[0], own, west, feat_out, lines)


def place_features(shift, own, west, feat_out, lines):
    lane = lax.broadcasted_iota(jnp.int32, (1, TOKENS), 1)
    slot = lane - (lane // SLOTS) * SLOTS
    mine = jnp.where(shift <= 6, slot - shift, shift - 1 - slot) >= 0
    for w in range(WINS):
        cols = slice(w * TOKENS, (w + 1) * TOKENS)
        both = jnp.where(mine, own[:, cols].astype(F32), west[:, cols].astype(F32))
        both = jnp.concatenate([both, jnp.zeros((32, TOKENS), F32)], axis=0).T
        for z in range(2):
            lines[pl.ds(2 * w + z, GRID, stride=8), :] = both[z * GRID : (z + 1) * GRID]
    for a in range(6):
        for c in range(SLOTS):
            at = (a * SLOTS + c) * 8
            feat_out[a, c] = lines[at : at + 8, 0:WIDTH].astype(BF16)


class Links:
    def __init__(self, send, recv):
        self.send, self.recv, self.used, self.sent = send, recv, 0, []

    def copy(self, src, dst, to):
        k = self.used
        self.used += 1
        return pltpu.make_async_remote_copy(
            src_ref=src,
            dst_ref=dst,
            send_sem=self.send.at[k],
            recv_sem=self.recv.at[k],
            device_id=to,
            device_id_type=pl.DeviceIdType.MESH,
        )

    def start(self, src, dst, to):
        made = self.copy(src, dst, to)
        made.start()
        self.sent.append(made)
        return made

    def finish(self):
        for made in self.sent:
            made.wait_send()


def place():
    lon, lat, head = lax.axis_index("lon"), lax.axis_index("lat"), lax.axis_index("head")
    z, high = lon // 2, lon % 2
    low, core = lat // 2, lat % 2
    return lon, lat, head, z, high, high * 2 + low, core


def at_grid(z, x, core):
    return {"lon": z * 2 + x // 2, "lat": (x % 2) * 2 + core}


def meet(peers):
    barrier = pltpu.get_barrier_semaphore()
    for peer in peers:
        pl.semaphore_signal(barrier, inc=1, device_id=peer, device_id_type=pl.DeviceIdType.MESH)
    pl.semaphore_wait(barrier, len(peers))


def reduce_peers():
    lon, lat, head, z, high, x, core = place()
    xc = x * 2 + core
    peers = [{"lon": ((z + k) % 8) * 2 + high} for k in range(1, 8)]
    peers += [at_grid(z, ((xc + k) % 8) // 2, (xc + k) % 2) for k in range(1, 8)]
    peers += [{"head": (head + k) % 4} for k in range(1, 4)]
    peers += [{"lon": (lon + 1) % 16}, {"lon": (lon + 15) % 16}]
    return peers


NAMES = dict(
    xv=pltpu.VMEM((6, SLOTS, 8, MODEL), BF16),
    gv=pltpu.VMEM((6, SLOTS, 8, MODEL), BF16),
    xe=pltpu.VMEM((6, 6, 8, MODEL), BF16),
    ge=pltpu.VMEM((6, 6, 8, MODEL), BF16),
    tabv=pltpu.VMEM((3, 64, TABLE), F32),
    wtv=pltpu.VMEM((3, WIDTH, MODEL), BF16),
    wov=pltpu.VMEM((WIDTH, MODEL), BF16),
    tabw=pltpu.VMEM((16, TABLE_PAD), F32),
    spread=pltpu.VMEM((12, 16, 288), F32),
    maps=pltpu.VMEM((12, 288, 256), BF16),
    bias=pltpu.VMEM((2, 1728, 128), F32),
    xs=pltpu.VMEM((3, 576, 128), F32),
    gs=pltpu.VMEM((3, 576, 128), F32),
    wflip=pltpu.VMEM((MODEL, 288), BF16),
    projs=pltpu.VMEM((WINS, 288, TOKENS), BF16),
    softs=pltpu.VMEM((12, TOKENS, TOKENS), F32),
    atts=pltpu.VMEM((WINS, WIDTH, TOKENS), BF16),
    scores=pltpu.VMEM((2, 1728, 128), F32),
    dprojs=pltpu.VMEM((WINS, 288, TOKENS), BF16),
    fold=pltpu.VMEM((3, TOKENS, 128), F32),
    sums=pltpu.VMEM((MODEL, MODEL), F32),
    folded=pltpu.VMEM((16, 4096), F32),
    a0=pltpu.VMEM((8, 48, MODEL), BF16),
    f0=pltpu.VMEM((8, 16, 512), BF16),
    p0=pltpu.VMEM((4, WIDTH, 640), BF16),
    a1=pltpu.VMEM((7, 48, MODEL), BF16),
    f1=pltpu.VMEM((7, 16, 512), BF16),
    p1=pltpu.VMEM((3, WIDTH, 640), BF16),
    a2s=pltpu.VMEM((8, 8, MODEL), F32),
    a2=pltpu.VMEM((7, 8, MODEL), F32),
    f2s=pltpu.VMEM((2, 16, 256), BF16),
    f2=pltpu.VMEM((16, 256), BF16),
    a3=pltpu.VMEM((8, 8, MODEL), F32),
    f3=pltpu.VMEM((8, 16, 256), BF16),
    send=pltpu.SemaphoreType.DMA((72,)),
    recv=pltpu.SemaphoreType.DMA((72,)),
    load=pltpu.SemaphoreType.DMA((8,)),
)


def main_kernel(first, types_ref, shift_ref, x, g, table, wt, wo, a_out, f_out, own_out, west_out, *scratch):
    v = dict(zip(NAMES, scratch, strict=True))
    lon, lat, head, z, high, xpos, core = place()
    xc = xpos * 2 + core
    step = 1 if first == 0 else 15
    net = Links(v["send"], v["recv"])
    loads = []
    for src, dst in ((x, "xv"), (g, "gv"), (table, "tabv"), (wt, "wtv"), (wo, "wov")):
        made = pltpu.make_async_copy(src, v[dst], v["load"].at[len(loads)])
        made.start()
        loads.append(made)
    types = [types_ref[w, 0] for w in range(WINS)]
    shift = shift_ref[0]
    loads[0].wait()
    loads[1].wait()
    meet(reduce_peers())

    rows, cols = pl.ds((head // 2) * 3, 3), (head % 2) * 3
    giver = {"lon": (lon + 16 - step) % 16}
    halo = []
    for own, far in ((v["xv"], v["xe"]), (v["gv"], v["ge"])):
        part = own.at[rows, pl.ds(first + cols, 3)]
        halo.append(net.start(part, far.at[rows, pl.ds(cols, 3)], giver))
    loads[2].wait()
    expand_bias(types, shift, v["tabv"], v["tabw"], v["spread"], v["maps"], v["bias"])
    spread_out = []
    for k, far in ((0, v["xe"]), (1, v["ge"])):
        halo[k].wait_recv()
        part = far.at[rows, pl.ds(cols, 3)]
        spread_out.append([net.start(part, part, {"head": (head + j) % 4}) for j in range(1, 4)])
    mixed = [c for c in range(first, first + 6)]
    still = [c for c in range(SLOTS) if c not in mixed]
    place_rows(v["xv"], None, shift, v["xs"], first, still)
    place_rows(v["gv"], None, shift, v["gs"], first, still)
    loads[3].wait()
    loads[4].wait()
    wts = v["wtv"][...].reshape(3 * WIDTH, MODEL)
    wos = v["wov"][...]
    v["wflip"][...] = wts.astype(F32).T.astype(BF16)

    for made in spread_out[0]:
        made.wait_recv()
    place_rows(v["xv"], v["xe"], shift, v["xs"], first, mixed)
    forward(v["xs"], wts, v["bias"], None, v["projs"], v["softs"], v["atts"])
    for made in spread_out[1]:
        made.wait_recv()
    place_rows(v["gv"], v["ge"], shift, v["gs"], first, mixed)
    backward(v["xs"], v["gs"], wos, v["projs"], v["softs"], v["atts"], v["scores"], v["sums"], v["dprojs"])

    def zs(k):
        return {"lon": ((z + k) % 8) * 2 + high}

    def xcs(k):
        other = (xc + k) % 8
        return at_grid(z, other // 2, other % 2)

    a0, f0, p0 = v["a0"], v["f0"], v["p0"]
    a1, f1, p1 = v["a1"], v["f1"], v["p1"]
    a2s, a2, f2s, f2, a3, f3 = (v[n] for n in ("a2s", "a2", "f2s", "f2", "a3", "f3"))
    for i in range(8):
        a0[i] = v["sums"][i * 48 : (i + 1) * 48, :].astype(BF16)
    one = [net.start(a0.at[(xc + k) % 8], a1.at[k - 1], xcs(k)) for k in range(1, 8)]
    fold_scores(types, v["scores"], v["maps"], v["fold"], v["folded"], f0)
    two = [net.start(f0.at[(z + k) % 8], f1.at[k - 1], zs(k)) for k in range(1, 8)]
    pieces_out(v["wflip"], v["dprojs"], p0)
    pieces = [net.start(p0.at[(head + k) % 4], p1.at[k - 1], {"head": (head + k) % 4}) for k in range(1, 4)]

    total = a0[xc].astype(F32)
    for k in range(7):
        one[k].wait_recv()
        total = total + a1[k].astype(F32)
    for k in range(8):
        a2s[k, 0:6, :] = total[k * 6 : (k + 1) * 6]
        a2s[k, 6:8, :] = jnp.zeros((2, MODEL), F32)
    three_ = [net.start(a2s.at[(z + k) % 8], a2.at[k - 1], zs(k)) for k in range(1, 8)]

    lines = f0[z].astype(F32)
    for k in range(7):
        two[k].wait_recv()
        lines = lines + f1[k].astype(F32)
    f2s[0] = lines[:, 0:256].astype(BF16)
    f2s[1] = lines[:, 256:512].astype(BF16)
    four = net.start(f2s.at[1 - high], f2, {"lon": z * 2 + 1 - high})

    feat = p0[head].astype(F32)
    for k in range(3):
        pieces[k].wait_recv()
        feat = feat + p1[k].astype(F32)
    own_out[...] = feat.astype(BF16)
    back = net.start(own_out, west_out, {"lon": (lon + step) % 16})

    four.wait_recv()
    mine = jnp.where(high == 0, lines[:, 0:256], lines[:, 256:512]) + f2[...].astype(F32)
    f3[z] = mine.astype(BF16)
    five = [net.start(f3.at[z], f3.at[z], zs(k)) for k in range(1, 8)]

    block = a2s[z]
    for k in range(7):
        three_[k].wait_recv()
        block = block + a2[k]
    a3[z] = block
    six = [net.start(a3.at[z], a3.at[z], zs(k)) for k in range(1, 8)]

    partner = at_grid(z, xpos, 1 - core)
    for k in range(7):
        five[k].wait_recv()
    arrive_f = [net.start(f3, f_out.at[xc], at_grid(z, (xpos + k) % 4, core)) for k in range(1, 4)]
    cross = [net.start(f3, f_out.at[xc], partner)]
    f_out[xc] = f3[...]
    for k in range(7):
        six[k].wait_recv()
    a_out[xc] = jnp.concatenate([a3[k][0:6] for k in range(8)], axis=0).astype(BF16)
    arrive = [net.start(a_out.at[xc], a_out.at[xc], at_grid(z, (xpos + k) % 4, core)) for k in range(1, 4)]
    cross.append(net.start(a_out.at[xc], a_out.at[xc], partner))
    for arrived, out in ((arrive_f, f_out), (arrive, a_out)):
        for k in range(1, 4):
            there = ((xpos + 4 - k) % 4) * 2 + core
            arrived[k - 1].wait_recv()
            cross.append(net.start(out.at[there], out.at[there], partner))
    back.wait_recv()
    for made in cross:
        made.wait_recv()
    net.finish()


def per_device(features, attend_weight, output_weight, bias_table, bias_type, window_shift, grad_out):
    x = features.transpose(1, 2, 0, 3)
    g = grad_out.transpose(1, 2, 0, 3)
    wt = attend_weight.transpose(0, 2, 1)
    table = bias_table.transpose(1, 0, 2)

    def run(first):
        return pl.pallas_call(
            functools.partial(main_kernel, first),
            out_shape=(
                jax.ShapeDtypeStruct((8, 48, MODEL), BF16),
                jax.ShapeDtypeStruct((8, 8, 16, 256), BF16),
                jax.ShapeDtypeStruct((WIDTH, 640), BF16),
                jax.ShapeDtypeStruct((WIDTH, 640), BF16),
            ),
            in_specs=[SMEM] * 2 + [ANY] * 5,
            out_specs=(VMEM,) * 4,
            scratch_shapes=list(NAMES.values()),
            compiler_params=pltpu.CompilerParams(
                vmem_limit_bytes=56 << 20, collective_id=1 if first == 0 else 2, has_side_effects=True
            ),
            name="block_east" if first == 0 else "block_west",
        )

    args = (bias_type, window_shift, x, g, table, wt, output_weight)
    sums, folded, own, borrowed = lax.cond(window_shift[0] <= 6, run(0), run(6), *args)
    return finish(window_shift, sums, folded, own, borrowed)


def finish(window_shift, sums, folded, own, borrowed):
    attend_grad, output_grad, bias_grad, feat = pl.pallas_call(
        finish_kernel,
        out_shape=(
            jax.ShapeDtypeStruct((3, WIDTH, MODEL), F32),
            jax.ShapeDtypeStruct((WIDTH, MODEL), F32),
            jax.ShapeDtypeStruct((3, 64, TABLE), F32),
            jax.ShapeDtypeStruct((6, SLOTS, 8, WIDTH), BF16),
        ),
        in_specs=[SMEM, VMEM, VMEM, VMEM, VMEM],
        out_specs=(VMEM,) * 4,
        scratch_shapes=[pltpu.VMEM((576, 128), F32)],
        compiler_params=pltpu.CompilerParams(vmem_limit_bytes=40 << 20),
        name="finish",
    )(window_shift, sums, folded, own, borrowed)
    return (
        feat.transpose(2, 0, 1, 3),
        attend_grad.transpose(0, 2, 1),
        output_grad,
        bias_grad.transpose(1, 0, 2),
    )


def solution(mesh):
    placed = (
        P(None, "lat", "lon", None),
        P(None, None, "head"),
        P("head", None),
        P(None, "head", None),
        P(None, "lat"),
        P(),
        P(None, "lat", "lon", None),
    )
    return jax.shard_map(
        per_device,
        mesh=mesh,
        in_specs=placed,
        out_specs=(
            P(None, "lat", "lon", "head"),
            P(None, None, "head"),
            P("head", None),
            P(None, "head", None),
        ),
        check_vma=False,
    )
```

```python
import functools

import jax
import jax.numpy as jnp
from jax import lax
from jax.experimental import pallas as pl
from jax.experimental.pallas import tpu as pltpu
from jax.sharding import PartitionSpec as P

F32 = jnp.float32
BF16 = jnp.bfloat16
HEADS = 3
WINS = 4
WIDTH = 96
HEAD = 32
SLOTS = 12
GRID = 72
TOKENS = 144
MODEL = 384
SPAN = 23
TABLE = 3312
TABLE_PAD = 3328
GROUP = 138
SCALE = HEAD ** (-0.5)
VMEM = pl.BlockSpec(memory_space=pltpu.VMEM)
SMEM = pl.BlockSpec(memory_space=pltpu.SMEM)
ANY = pl.BlockSpec(memory_space=pl.ANY)


def dot(a, b, da, db):
    return lax.dot_general(a, b, (((da,), (db,)), ((), ())), preferred_element_type=F32)


def three(x):
    hi = x.astype(BF16)
    rest = x - hi.astype(F32)
    mid = rest.astype(BF16)
    return hi, mid, (rest - mid.astype(F32)).astype(BF16)


def fold_map(ci, shift):
    rows = lax.broadcasted_iota(jnp.int32, (288, 256), 0)
    lane = lax.broadcasted_iota(jnp.int32, (1, 256), 1)
    block = lane // SLOTS
    cj = lane - block * SLOTS
    wrap = jnp.where(ci < shift, 12, 0) - jnp.where(cj < shift, 12, 0)
    target = block * SPAN + (11 + ci) - cj + wrap
    target = jnp.where(lane < TOKENS, target, -1)
    return jnp.where(rows == target, 1.0, 0.0).astype(BF16)


def expand_bias(types, shift, table, tabw, spread, maps, bias):
    for h in range(HEADS):
        for w in range(WINS):
            n = h * WINS + w
            tabw[n : n + 1, 0:TABLE] = table[h, pl.ds(types[w], 1), :]
    spread[...] = jnp.zeros_like(spread)
    for zi in range(2):
        for ai in range(6):
            for zj in range(2):
                at = zi * 1656 + zj * 828 + ai * GROUP
                spread[zi * 6 + ai, 0:12, zj * GROUP : (zj + 1) * GROUP] = tabw[0:12, at : at + GROUP]
    parts = three(spread[...].reshape(192, 288))
    for ci in range(SLOTS):
        chosen = fold_map(ci, shift)
        maps[ci] = chosen
        full = dot(parts[0], chosen, 1, 0) + dot(parts[1], chosen, 1, 0) + dot(parts[2], chosen, 1, 0)
        for n in range(12):
            for k in range(2):
                bias[k, pl.ds(n * SLOTS + ci, 12, stride=TOKENS), :] = full[
                    n * 16 : n * 16 + 12, k * 128 : (k + 1) * 128
                ]


def window_rows(scratch, w):
    halves = []
    for z in range(2):
        lanes = [scratch[k, pl.ds(2 * w + z, GRID, stride=8), :] for k in range(3)]
        halves.append(jnp.concatenate(lanes, axis=1))
    return jnp.concatenate(halves, axis=0).astype(BF16)


def place_rows(own, borrowed, shift, scratch, first, slots):
    for c in slots:
        for a in range(6):
            rows = own[a, c].astype(F32)
            if borrowed is not None:
                keep = c >= shift if first == 0 else c < shift
                rows = jnp.where(keep, rows, borrowed[a, c - first].astype(F32))
            for k in range(3):
                scratch[k, (a * SLOTS + c) * 8 : (a * SLOTS + c + 1) * 8, :] = rows[:, k * 128 : (k + 1) * 128]


def only(x, h):
    return jnp.concatenate([x[k * HEAD : (k + 1) * HEAD] if k == h else jnp.zeros((HEAD, x.shape[1]), x.dtype) for k in range(HEADS)], axis=0)


def forward(xs, wts, bias, proj_out, softs, atts):
    tops = {}
    for w in range(WINS):
        xw = window_rows(xs, w)
        proj = dot(wts, xw, 1, 1).astype(BF16)
        proj_out[w] = proj
        q = dot(xw, wts[0:WIDTH], 1, 1).astype(BF16)
        for h in range(HEADS):
            n = h * WINS + w
            rows = slice(n * TOKENS, (n + 1) * TOKENS)
            added = jnp.concatenate([bias[0, rows, :], bias[1, rows, 0:16]], axis=1)
            logits = dot(q, only(proj[96:192], h), 1, 0) * SCALE + added
            softs[n] = logits
            tops[n] = jnp.max(logits, axis=1, keepdims=True)
    for w in range(WINS):
        sums = []
        for h in range(HEADS):
            n = h * WINS + w
            raised = jnp.exp(softs[n] - tops[n])
            softs[n] = raised
            sums.append(1.0 / jnp.sum(raised, axis=1, keepdims=True))
        att = []
        for h in range(HEADS):
            n = h * WINS + w
            soft = softs[n] * sums[h]
            softs[n] = soft
            att.append(dot(proj_out[w, 192 + h * HEAD : 192 + (h + 1) * HEAD, :], soft.astype(BF16), 1, 1))
        atts[w] = jnp.concatenate(att, axis=0).astype(BF16)


def backward(xs, gs, wos, proj_in, softs, gsofts, atts, scores, sums, dprojs):
    rowsums, dats = {}, {}
    for w in range(WINS):
        gw = window_rows(gs, w)
        dats[w] = dot(wos, gw, 1, 1).astype(BF16)
        da = dot(gw, wos, 1, 1).astype(BF16)
        vt = proj_in[w, 192:288, :]
        for h in range(HEADS):
            n = h * WINS + w
            gsoft = dot(da, only(vt, h), 1, 0)
            gsofts[n] = gsoft
            rowsums[n] = jnp.sum(softs[n] * gsoft, axis=1, keepdims=True)
        low = dot(atts[w], gw, 1, 0)
        if w == 0:
            sums[288:384, :] = low
        else:
            sums[288:384, :] += low
    for w in range(WINS):
        dq, dk, dv = [], [], []
        for h in range(HEADS):
            n = h * WINS + w
            rows = slice(n * TOKENS, (n + 1) * TOKENS)
            own = slice(h * HEAD, (h + 1) * HEAD)
            soft = softs[n]
            gsc = soft * (gsofts[n] - rowsums[n])
            scores[0, rows, :] = gsc[:, 0:128]
            scores[1, rows, 0:16] = gsc[:, 128:144]
            gh = gsc.astype(BF16)
            dv.append(dot(dats[w][own], soft.astype(BF16), 1, 0))
            dq.append(dot(proj_in[w, 96 + h * HEAD : 96 + (h + 1) * HEAD, :], gh, 1, 1) * SCALE)
            dk.append(dot(proj_in[w, own, :], gh, 1, 0) * SCALE)
        dproj = jnp.concatenate(dq + dk + dv, axis=0).astype(BF16)
        dprojs[w] = dproj
        top = dot(dproj, window_rows(xs, w), 1, 0)
        if w == 0:
            sums[0:288, :] = top
        else:
            sums[0:288, :] += top


def fold_scores(types, scores, maps, fold, folded, folded_out):
    total = None
    for ci in range(SLOTS):
        part = jnp.concatenate(
            [scores[0, pl.ds(ci, TOKENS, stride=SLOTS), :], scores[1, pl.ds(ci, TOKENS, stride=SLOTS), :][:, 0:16]], axis=1
        )
        term = dot(part.astype(BF16), maps[ci][:, 0:TOKENS], 1, 1)
        total = term if total is None else total + term
    for k in range(3):
        wide = min(128, 288 - k * 128)
        fold[k, :, 0:wide] = total[:, k * 128 : k * 128 + wide]
    folded[...] = jnp.zeros_like(folded)
    for zi in range(2):
        for ai in range(6):
            got = [fold[k, pl.ds(zi * 6 + ai, 12, stride=12), :] for k in range(3)]
            line = jnp.concatenate(got, axis=1)
            for zj in range(2):
                at = zi * 1656 + zj * 828 + ai * GROUP
                folded[0:12, at : at + GROUP] = line[:, zj * GROUP : (zj + 1) * GROUP]
    row = lax.broadcasted_iota(jnp.int32, (16, 256), 0)
    marks = jnp.zeros((16, 256), jnp.int32)
    for w in range(WINS):
        marks = jnp.where(row == 12 + w, types[w], marks)
    marks = marks.astype(F32)
    for z in range(16):
        part = folded[:, z * 256 : (z + 1) * 256]
        folded_out[z] = jnp.where(row < 12, part, marks).astype(BF16)


def pieces_out(wflip, dprojs, piece):
    for w in range(WINS):
        back = dot(wflip[...], dprojs[w], 1, 0).astype(BF16)
        for r in range(4):
            piece[r, :, w * TOKENS : (w + 1) * TOKENS] = back[r * WIDTH : (r + 1) * WIDTH]
    for r in range(4):
        piece[r, :, 576:640] = jnp.zeros((WIDTH, 64), BF16)


def pick_types(lines):
    marks = jnp.concatenate([lines[q][12:16, 0:1] for q in range(4)], axis=0) * 0.0625
    lane = lax.broadcasted_iota(jnp.int32, (16, 128), 1).astype(F32)
    return jnp.where(lane == marks, 1.0, 0.0).T[0:64].astype(BF16)


def finish_kernel(shift_ref, sums, folded, own, far, attend_out, output_out, bias_out, feat_out):
    whole = [
        jnp.concatenate([folded[xh * 4 + q, z] for z in range(7) for xh in range(2)], axis=1).astype(F32) for q in range(4)
    ]
    pick = pick_types(whole)
    for h in range(HEADS):
        rows = jnp.concatenate([whole[q][h * WINS : (h + 1) * WINS, 0:TABLE_PAD] for q in range(4)], axis=0)
        bias_out[h] = dot(pick, rows.astype(BF16), 1, 0)[:, 0:TABLE]
    for i in range(8):
        for r in range(3):
            for k in range(3):
                part = sums[i, r * 3 + k].astype(F32)
                at, lanes = (i % 2) * 48 + r * 16, slice(k * 128, (k + 1) * 128)
                if i < 6:
                    attend_out[i // 2, at : at + 16, lanes] = part
                else:
                    output_out[at : at + 16, lanes] = part
    shift = shift_ref[0]
    for c in range(SLOTS):
        mine = jnp.where(shift <= 6, c - shift, shift - 1 - c) >= 0
        for a in range(6):
            feat_out[a, c] = jnp.where(mine, own[a, c].astype(F32), far[a, c % 6].astype(F32)).astype(BF16)[:, 0:WIDTH]


def place_features(feat, lines, out):
    for w in range(WINS):
        both = jnp.concatenate([feat[:, w * TOKENS : (w + 1) * TOKENS], jnp.zeros((32, TOKENS), F32)], axis=0).T
        for z in range(2):
            lines[pl.ds(2 * w + z, GRID, stride=8), :] = both[z * GRID : (z + 1) * GRID]
    for a in range(6):
        for c in range(SLOTS):
            at = (a * SLOTS + c) * 8
            out[a, c] = lines[at : at + 8, :].astype(BF16)


class Links:
    def __init__(self, send, recv):
        self.send, self.recv, self.used, self.sent = send, recv, 0, []

    def copy(self, src, dst, to):
        k = self.used
        self.used += 1
        return pltpu.make_async_remote_copy(
            src_ref=src,
            dst_ref=dst,
            send_sem=self.send.at[k],
            recv_sem=self.recv.at[k],
            device_id=to,
            device_id_type=pl.DeviceIdType.MESH,
        )

    def start(self, src, dst, to):
        made = self.copy(src, dst, to)
        made.start()
        self.sent.append(made)
        return made

    def settle(self):
        for made in self.sent:
            made.wait_send()
        self.sent = []


def place():
    lon, lat, head = lax.axis_index("lon"), lax.axis_index("lat"), lax.axis_index("head")
    z, high = lon // 2, lon % 2
    low, core = lat // 2, lat % 2
    return lon, lat, head, z, high, high * 2 + low, core


def at_grid(z, x, core):
    return {"lon": z * 2 + x // 2, "lat": (x % 2) * 2 + core}


def greet(peers):
    barrier = pltpu.get_barrier_semaphore()
    for peer in peers:
        pl.semaphore_signal(barrier, inc=1, device_id=peer, device_id_type=pl.DeviceIdType.MESH)
    return len(peers)


def reduce_peers():
    lon, lat, head, z, high, x, core = place()
    xc = x * 2 + core
    peers = [{"lon": (lon + k) % 16} for k in range(1, 16)]
    peers += [at_grid(z, ((xc + k) % 8) // 2, (xc + k) % 2) for k in range(1, 8)]
    peers += [{"head": (head + k) % 4} for k in range(1, 4)]
    return peers


NAMES = dict(
    xv=pltpu.VMEM((6, SLOTS, 8, MODEL), BF16),
    gv=pltpu.VMEM((6, SLOTS, 8, MODEL), BF16),
    xe=pltpu.VMEM((6, 6, 8, MODEL), BF16),
    ge=pltpu.VMEM((6, 6, 8, MODEL), BF16),
    tabv=pltpu.VMEM((3, 64, TABLE), F32),
    wtv=pltpu.VMEM((3, WIDTH, MODEL), BF16),
    wov=pltpu.VMEM((WIDTH, MODEL), BF16),
    tabw=pltpu.VMEM((16, TABLE_PAD), F32),
    spread=pltpu.VMEM((12, 16, 288), F32),
    maps=pltpu.VMEM((12, 288, 256), BF16),
    bias=pltpu.VMEM((2, 1728, 128), F32),
    xs=pltpu.VMEM((3, 576, 128), F32),
    gs=pltpu.VMEM((3, 576, 128), F32),
    wflip=pltpu.VMEM((MODEL, 288), BF16),
    projs=pltpu.VMEM((WINS, 288, TOKENS), BF16),
    gsofts=pltpu.VMEM((12, TOKENS, TOKENS), F32),
    softs=pltpu.VMEM((12, TOKENS, TOKENS), F32),
    atts=pltpu.VMEM((WINS, WIDTH, TOKENS), BF16),
    scores=pltpu.VMEM((2, 1728, 128), F32),
    dprojs=pltpu.VMEM((WINS, 288, TOKENS), BF16),
    fold=pltpu.VMEM((3, TOKENS, 128), F32),
    sums=pltpu.VMEM((MODEL, MODEL), F32),
    folded=pltpu.VMEM((16, 4096), F32),
    a0=pltpu.VMEM((4, 48, MODEL), BF16),
    ad=pltpu.VMEM((4, 48, MODEL), BF16),
    ax=pltpu.VMEM((4, 48, MODEL), BF16),
    f0=pltpu.VMEM((16, 16, 256), BF16),
    p0=pltpu.VMEM((4, WIDTH, 640), BF16),
    a1=pltpu.VMEM((3, 48, MODEL), BF16),
    f1=pltpu.VMEM((15, 16, 256), BF16),
    p1=pltpu.VMEM((3, WIDTH, 640), BF16),
    a2s=pltpu.VMEM((8, 2, 16, 128), BF16),
    a2=pltpu.VMEM((7, 2, 16, 128), BF16),
    a3=pltpu.VMEM((8, 16, 128), BF16),
    lines=pltpu.VMEM((576, 128), F32),
    f3=pltpu.VMEM((8, 16, 256), BF16),
    send=pltpu.SemaphoreType.DMA((72,)),
    recv=pltpu.SemaphoreType.DMA((72,)),
    load=pltpu.SemaphoreType.DMA((8,)),
    types=pltpu.SMEM((1, 4), jnp.int32),
    shift=pltpu.SMEM((1,), jnp.int32),
)


def main_kernel(first, types_ref, shift_ref, x, g, table, wt, wo, a_out, f_out, own_out, west_out, *scratch):
    v = dict(zip(NAMES, scratch, strict=True))
    lon, lat, head, z, high, xpos, core = place()
    xc = xpos * 2 + core
    step = 1 if first == 0 else 15
    net = Links(v["send"], v["recv"])
    met = greet(reduce_peers())
    loads = []
    given = ((types_ref, "types"), (shift_ref, "shift"), (table, "tabv"), (x, "xv"), (g, "gv"), (wt, "wtv"), (wo, "wov"))
    for src, dst in given:
        made = pltpu.make_async_copy(src, v[dst], v["load"].at[len(loads)])
        made.start()
        loads.append(made)
    with jax.named_scope("bias"):
        for made in loads[0:3]:
            made.wait()
        types = [v["types"][0, w] for w in range(WINS)]
        shift = v["shift"][0]
        expand_bias(types, shift, v["tabv"], v["tabw"], v["spread"], v["maps"], v["bias"])
    with jax.named_scope("enter"):
        for made in loads[3:5]:
            made.wait()
        pl.semaphore_wait(pltpu.get_barrier_semaphore(), met)

    giver = {"lon": (lon + 16 - step) % 16}
    rows, cols = pl.ds((head // 2) * 3, 3), (head % 2) * 3
    quarter = v["ge"].at[rows, pl.ds(cols, 3)]
    halo = [net.start(v["gv"].at[rows, pl.ds(first + cols, 3)], quarter, giver)]
    halo.append(net.start(v["xv"].at[:, pl.ds(first, 6)], v["xe"], giver))
    mixed = [c for c in range(first, first + 6)]
    still = [c for c in range(SLOTS) if c not in mixed]
    place_rows(v["xv"], None, shift, v["xs"], first, still)
    place_rows(v["gv"], None, shift, v["gs"], first, still)
    with jax.named_scope("still"):
        loads[5].wait()
        loads[6].wait()
        wts = v["wtv"][...].reshape(3 * WIDTH, MODEL)
        wos = v["wov"][...]
        v["wflip"][...] = wts.astype(F32).T.astype(BF16)

    with jax.named_scope("halo_q"):
        halo[0].wait_recv()
    handed = [net.start(quarter, quarter, {"head": (head + j) % 4}) for j in range(1, 4)]
    with jax.named_scope("halo_x"):
        halo[1].wait_recv()
    with jax.named_scope("forward"):
        place_rows(v["xv"], v["xe"], shift, v["xs"], first, mixed)
        forward(v["xs"], wts, v["bias"], v["projs"], v["softs"], v["atts"])
    with jax.named_scope("halo_g"):
        for made in handed:
            made.wait_recv()
    with jax.named_scope("backward"):
        place_rows(v["gv"], v["ge"], shift, v["gs"], first, mixed)
        backward(v["xs"], v["gs"], wos, v["projs"], v["softs"], v["gsofts"], v["atts"], v["scores"], v["sums"], v["dprojs"])

    def zs(k):
        return {"lon": ((z + k) % 8) * 2 + high}

    a0, f0, p0 = v["a0"], v["f0"], v["p0"]
    a1, f1, p1 = v["a1"], v["f1"], v["p1"]
    ad, ax, a2s, a2, a3, f3 = (v[n] for n in ("ad", "ax", "a2s", "a2", "a3", "f3"))
    partner = at_grid(z, xpos, 1 - core)

    def chunk(i, side):
        return v["sums"][pl.ds(pl.multiple_of((2 * i + side) * 48, 16), 48), :]

    for i in range(4):
        a0[i] = chunk(i, 1 - core).astype(BF16)
    twin = net.start(a0, ad, partner)
    with jax.named_scope("fold"):
        fold_scores(types, v["scores"], v["maps"], v["fold"], v["folded"], f0)
    with jax.named_scope("sum_d"):
        twin.wait_recv()
        for i in range(4):
            ax[i] = (chunk(i, core) + ad[i].astype(F32)).astype(BF16)
    one = [net.start(ax.at[(xpos + k) % 4], a1.at[k - 1], at_grid(z, (xpos + k) % 4, core)) for k in range(1, 4)]
    two = [net.start(f0.at[(lon + k) % 16], f1.at[k - 1], {"lon": (lon + k) % 16}) for k in range(1, 16)]
    with jax.named_scope("pieces"):
        pieces_out(v["wflip"], v["dprojs"], p0)
    pieces = [net.start(p0.at[(head + k) % 4], p1.at[k - 1], {"head": (head + k) % 4}) for k in range(1, 4)]

    with jax.named_scope("sum_a"):
        total = chunk(xpos, core) + ad[xpos].astype(F32)
        for k in range(3):
            one[k].wait_recv()
            total = total + a1[k].astype(F32)
        tiles = [total[r * 16 : (r + 1) * 16, k * 128 : (k + 1) * 128].astype(BF16) for r in range(3) for k in range(3)]
        for k in range(8):
            a2s[k, 0] = tiles[k]
            a2s[k, 1] = tiles[8]
    three_ = [net.start(a2s.at[(z + k) % 8], a2.at[k - 1], zs(k)) for k in range(1, 8)]

    with jax.named_scope("sum_f"):
        lines = f0[lon].astype(F32)
        for k in range(15):
            two[k].wait_recv()
            lines = lines + f1[k].astype(F32)
        f3[z] = lines.astype(BF16)
    five = [net.start(f3.at[z], f3.at[z], zs(k)) for k in range(1, 8)]

    with jax.named_scope("sum_z"):
        block = a2s[z].astype(F32)
        for k in range(7):
            three_[k].wait_recv()
            block = block + a2[k].astype(F32)
        a3[z] = block[0].astype(BF16)
    six = [net.start(a3.at[z], a3.at[z], zs(k)) for k in range(1, 8)]
    a_out[xc, 8] = block[1].astype(BF16)

    with jax.named_scope("sum_p"):
        feat = p0[head].astype(F32)
        for k in range(3):
            pieces[k].wait_recv()
            feat = feat + p1[k].astype(F32)
        place_features(feat, v["lines"], own_out)
    net.settle()
    back = net.start(own_out.at[:, pl.ds(first, 6)], west_out, {"lon": (lon + step) % 16})

    with jax.named_scope("all_f"):
        for k in range(7):
            five[k].wait_recv()
    part = f3.at[pl.ds(0, 7)]
    mine = f_out.at[xc, pl.ds(0, 7)]
    arrive_f = [net.start(part, mine, at_grid(z, (xpos + k) % 4, core)) for k in range(1, 4)]
    cross = [net.start(part, mine, partner)]
    f_out[xc] = f3[...]
    with jax.named_scope("all_a"):
        for k in range(7):
            six[k].wait_recv()
    a_out[xc, 0:8] = a3[...]
    arrive = [net.start(a_out.at[xc], a_out.at[xc], at_grid(z, (xpos + k) % 4, core)) for k in range(1, 4)]
    cross.append(net.start(a_out.at[xc], a_out.at[xc], partner))
    with jax.named_scope("forward_x"):
        for arrived, out, whole in ((arrive_f, f_out, False), (arrive, a_out, True)):
            for k in range(1, 4):
                there = ((xpos + 4 - k) % 4) * 2 + core
                arrived[k - 1].wait_recv()
                ref = out.at[there] if whole else out.at[there, pl.ds(0, 7)]
                cross.append(net.start(ref, ref, partner))
    net.settle()
    with jax.named_scope("last"):
        back.wait_recv()
        for made in cross:
            made.wait_recv()


def per_device(features, attend_weight, output_weight, bias_table, bias_type, window_shift, grad_out):
    x = features.transpose(1, 2, 0, 3)
    g = grad_out.transpose(1, 2, 0, 3)
    wt = attend_weight.transpose(0, 2, 1)
    table = bias_table.transpose(1, 0, 2)

    def run(first):
        return pl.pallas_call(
            functools.partial(main_kernel, first),
            out_shape=(
                jax.ShapeDtypeStruct((8, 9, 16, 128), BF16),
                jax.ShapeDtypeStruct((8, 8, 16, 256), BF16),
                jax.ShapeDtypeStruct((6, SLOTS, 8, 128), BF16),
                jax.ShapeDtypeStruct((6, 6, 8, 128), BF16),
            ),
            in_specs=[ANY] * 7,
            out_specs=(VMEM,) * 4,
            scratch_shapes=list(NAMES.values()),
            compiler_params=pltpu.CompilerParams(
                vmem_limit_bytes=56 << 20, collective_id=1 if first == 0 else 2, has_side_effects=True
            ),
            name="block_east" if first == 0 else "block_west",
        )

    args = (bias_type.T, window_shift, x, g, table, wt, output_weight)
    sums, folded, own, borrowed = lax.cond(window_shift[0] <= 6, run(0), run(6), *args)
    return finish(window_shift, sums, folded, own, borrowed)


def finish(window_shift, sums, folded, own, borrowed):
    attend_grad, output_grad, bias_grad, feat = pl.pallas_call(
        finish_kernel,
        out_shape=(
            jax.ShapeDtypeStruct((3, WIDTH, MODEL), F32),
            jax.ShapeDtypeStruct((WIDTH, MODEL), F32),
            jax.ShapeDtypeStruct((3, 64, TABLE), F32),
            jax.ShapeDtypeStruct((6, SLOTS, 8, WIDTH), BF16),
        ),
        in_specs=[SMEM, VMEM, VMEM, VMEM, VMEM],
        out_specs=(VMEM,) * 4,
        compiler_params=pltpu.CompilerParams(vmem_limit_bytes=40 << 20),
        name="finish",
    )(window_shift, sums, folded, own, borrowed)
    return (
        feat.transpose(2, 0, 1, 3),
        attend_grad.transpose(0, 2, 1),
        output_grad,
        bias_grad.transpose(1, 0, 2),
    )


def solution(mesh):
    placed = (
        P(None, "lat", "lon", None),
        P(None, None, "head"),
        P("head", None),
        P(None, "head", None),
        P(None, "lat"),
        P(),
        P(None, "lat", "lon", None),
    )
    return jax.shard_map(
        per_device,
        mesh=mesh,
        in_specs=placed,
        out_specs=(
            P(None, "lat", "lon", "head"),
            P(None, None, "head"),
            P("head", None),
            P(None, "head", None),
        ),
        check_vma=False,
    )
```

```python
import functools

import jax
import jax.numpy as jnp
from jax import lax
from jax.experimental import pallas as pl
from jax.experimental.pallas import tpu as pltpu
from jax.sharding import PartitionSpec as P

F32 = jnp.float32
BF16 = jnp.bfloat16
HEADS = 3
WINS = 4
WIDTH = 96
HEAD = 32
SLOTS = 12
GRID = 72
TOKENS = 144
MODEL = 384
SPAN = 23
TABLE = 3312
TABLE_PAD = 3328
GROUP = 138
SCALE = HEAD ** (-0.5)
VMEM = pl.BlockSpec(memory_space=pltpu.VMEM)
SMEM = pl.BlockSpec(memory_space=pltpu.SMEM)
ANY = pl.BlockSpec(memory_space=pl.ANY)


def dot(a, b, da, db):
    return lax.dot_general(a, b, (((da,), (db,)), ((), ())), preferred_element_type=F32)


def three(x):
    hi = x.astype(BF16)
    rest = x - hi.astype(F32)
    mid = rest.astype(BF16)
    return hi, mid, (rest - mid.astype(F32)).astype(BF16)


def fold_map(ci, shift):
    rows = lax.broadcasted_iota(jnp.int32, (288, 256), 0)
    lane = lax.broadcasted_iota(jnp.int32, (1, 256), 1)
    block = lane // SLOTS
    cj = lane - block * SLOTS
    wrap = jnp.where(ci < shift, 12, 0) - jnp.where(cj < shift, 12, 0)
    target = block * SPAN + (11 + ci) - cj + wrap
    target = jnp.where(lane < TOKENS, target, -1)
    return jnp.where(rows == target, 1.0, 0.0).astype(BF16)


def expand_bias(types, shift, table, tabw, spread, maps, bias):
    for h in range(HEADS):
        for w in range(WINS):
            n = h * WINS + w
            tabw[n : n + 1, 0:TABLE] = table[h, pl.ds(types[w], 1), :]
    spread[...] = jnp.zeros_like(spread)
    for zi in range(2):
        for ai in range(6):
            for zj in range(2):
                at = zi * 1656 + zj * 828 + ai * GROUP
                spread[zi * 6 + ai, 0:12, zj * GROUP : (zj + 1) * GROUP] = tabw[0:12, at : at + GROUP]
    parts = three(spread[...].reshape(192, 288))
    for ci in range(SLOTS):
        chosen = fold_map(ci, shift)
        maps[ci] = chosen
        full = dot(parts[0], chosen, 1, 0) + dot(parts[1], chosen, 1, 0) + dot(parts[2], chosen, 1, 0)
        for n in range(12):
            for k in range(2):
                bias[k, pl.ds(n * SLOTS + ci, 12, stride=TOKENS), :] = full[
                    n * 16 : n * 16 + 12, k * 128 : (k + 1) * 128
                ]


def window_rows(scratch, w):
    halves = []
    for z in range(2):
        lanes = [scratch[k, pl.ds(2 * w + z, GRID, stride=8), :] for k in range(3)]
        halves.append(jnp.concatenate(lanes, axis=1))
    return jnp.concatenate(halves, axis=0).astype(BF16)


def place_rows(own, borrowed, shift, scratch, first, slots):
    for c in slots:
        for a in range(6):
            rows = own[a, c].astype(F32)
            if borrowed is not None:
                keep = c >= shift if first == 0 else c < shift
                rows = jnp.where(keep, rows, borrowed[a, c - first].astype(F32))
            for k in range(3):
                scratch[k, (a * SLOTS + c) * 8 : (a * SLOTS + c + 1) * 8, :] = rows[:, k * 128 : (k + 1) * 128]


def only(x, h):
    return jnp.concatenate([x[k * HEAD : (k + 1) * HEAD] if k == h else jnp.zeros((HEAD, x.shape[1]), x.dtype) for k in range(HEADS)], axis=0)


def forward(xs, wts, bias, proj_out, softs, atts):
    tops = {}
    for w in range(WINS):
        xw = window_rows(xs, w)
        proj = dot(wts, xw, 1, 1).astype(BF16)
        proj_out[w] = proj
        q = dot(xw, wts[0:WIDTH], 1, 1).astype(BF16)
        for h in range(HEADS):
            n = h * WINS + w
            rows = slice(n * TOKENS, (n + 1) * TOKENS)
            added = jnp.concatenate([bias[0, rows, :], bias[1, rows, 0:16]], axis=1)
            logits = dot(q, only(proj[96:192], h), 1, 0) * SCALE + added
            softs[n] = logits
            tops[n] = jnp.max(logits, axis=1, keepdims=True)
    for w in range(WINS):
        sums = []
        for h in range(HEADS):
            n = h * WINS + w
            raised = jnp.exp(softs[n] - tops[n])
            softs[n] = raised
            sums.append(1.0 / jnp.sum(raised, axis=1, keepdims=True))
        att = []
        for h in range(HEADS):
            n = h * WINS + w
            soft = softs[n] * sums[h]
            softs[n] = soft
            att.append(dot(proj_out[w, 192 + h * HEAD : 192 + (h + 1) * HEAD, :], soft.astype(BF16), 1, 1))
        atts[w] = jnp.concatenate(att, axis=0).astype(BF16)


def backward(xs, gs, wos, proj_in, softs, gsofts, atts, scores, sums, dprojs):
    rowsums, dats = {}, {}
    for w in range(WINS):
        gw = window_rows(gs, w)
        dats[w] = dot(wos, gw, 1, 1).astype(BF16)
        da = dot(gw, wos, 1, 1).astype(BF16)
        vt = proj_in[w, 192:288, :]
        for h in range(HEADS):
            n = h * WINS + w
            gsoft = dot(da, only(vt, h), 1, 0)
            gsofts[n] = gsoft
            rowsums[n] = jnp.sum(softs[n] * gsoft, axis=1, keepdims=True)
        low = dot(atts[w], gw, 1, 0)
        if w == 0:
            sums[288:384, :] = low
        else:
            sums[288:384, :] += low
    for w in range(WINS):
        dq, dk, dv = [], [], []
        for h in range(HEADS):
            n = h * WINS + w
            rows = slice(n * TOKENS, (n + 1) * TOKENS)
            own = slice(h * HEAD, (h + 1) * HEAD)
            soft = softs[n]
            gsc = soft * (gsofts[n] - rowsums[n])
            scores[0, rows, :] = gsc[:, 0:128]
            scores[1, rows, 0:16] = gsc[:, 128:144]
            gh = gsc.astype(BF16)
            dv.append(dot(dats[w][own], soft.astype(BF16), 1, 0))
            dq.append(dot(proj_in[w, 96 + h * HEAD : 96 + (h + 1) * HEAD, :], gh, 1, 1) * SCALE)
            dk.append(dot(proj_in[w, own, :], gh, 1, 0) * SCALE)
        dproj = jnp.concatenate(dq + dk + dv, axis=0).astype(BF16)
        dprojs[w] = dproj
        top = dot(dproj, window_rows(xs, w), 1, 0)
        if w == 0:
            sums[0:288, :] = top
        else:
            sums[0:288, :] += top


def fold_scores(types, scores, maps, fold, folded, folded_out):
    total = None
    for ci in range(SLOTS):
        part = jnp.concatenate(
            [scores[0, pl.ds(ci, TOKENS, stride=SLOTS), :], scores[1, pl.ds(ci, TOKENS, stride=SLOTS), :][:, 0:16]], axis=1
        )
        term = dot(part.astype(BF16), maps[ci][:, 0:TOKENS], 1, 1)
        total = term if total is None else total + term
    for k in range(3):
        wide = min(128, 288 - k * 128)
        fold[k, :, 0:wide] = total[:, k * 128 : k * 128 + wide]
    folded[...] = jnp.zeros_like(folded)
    for zi in range(2):
        for ai in range(6):
            got = [fold[k, pl.ds(zi * 6 + ai, 12, stride=12), :] for k in range(3)]
            line = jnp.concatenate(got, axis=1)
            for zj in range(2):
                at = zi * 1656 + zj * 828 + ai * GROUP
                folded[0:12, at : at + GROUP] = line[:, zj * GROUP : (zj + 1) * GROUP]
    row = lax.broadcasted_iota(jnp.int32, (16, 128), 0)
    lane = lax.broadcasted_iota(jnp.int32, (16, 128), 1)
    marks = jnp.zeros((16, 128), jnp.int32)
    for w in range(WINS):
        marks = jnp.where(row == w, types[w], marks)
    folded[:, 3200:TABLE_PAD] = jnp.where(lane >= 112, marks.astype(F32), folded[:, 3200:TABLE_PAD])
    for i in range(16):
        left, right = (folded[:, i * 256 + k * 128 : i * 256 + (k + 1) * 128] for k in range(2))
        folded_out[i, 0] = left[0:8].astype(BF16)
        folded_out[i, 1] = right[0:8].astype(BF16)
        folded_out[i, 2] = jnp.concatenate([left[8:12], right[8:12]], axis=0).astype(BF16)


def pieces_out(wflip, dprojs, piece):
    for w in range(WINS):
        back = dot(wflip[...], dprojs[w], 1, 0).astype(BF16)
        for r in range(4):
            piece[r, :, w * TOKENS : (w + 1) * TOKENS] = back[r * WIDTH : (r + 1) * WIDTH]
    for r in range(4):
        piece[r, :, 576:640] = jnp.zeros((WIDTH, 64), BF16)


def finish_kernel(shift_ref, sums, folded, own, far, attend_out, output_out, bias_out, feat_out):
    first, last = [], []
    for q in range(4):
        high, low = [], []
        for z in range(7):
            for xh in range(2):
                part = folded[xh * 4 + q, z].astype(F32)
                high += [part[0], part[1]]
                low += [part[2, 0:4], part[2, 4:8]]
        first.append(jnp.concatenate(high[0:26], axis=1))
        last.append(jnp.concatenate(low[0:26], axis=1))
    marks = jnp.concatenate([first[q][0:4, TABLE : TABLE + 1] for q in range(4)], axis=0) * 0.0625
    lane = lax.broadcasted_iota(jnp.int32, (16, 128), 1).astype(F32)
    pick = jnp.where(lane == marks, 1.0, 0.0).T[0:64].astype(BF16)
    for h in range(HEADS):
        rows = [first[q][h * WINS : (h + 1) * WINS] if h < 2 else last[q] for q in range(4)]
        bias_out[h] = dot(pick, jnp.concatenate(rows, axis=0).astype(BF16), 1, 0)[:, 0:TABLE]
    for i in range(8):
        for r in range(3):
            for k in range(3):
                part = sums[i, r * 3 + k].astype(F32)
                at, lanes = (i % 2) * 48 + r * 16, slice(k * 128, (k + 1) * 128)
                if i < 6:
                    attend_out[i // 2, at : at + 16, lanes] = part
                else:
                    output_out[at : at + 16, lanes] = part
    shift = shift_ref[0]
    for c in range(SLOTS):
        mine = jnp.where(shift <= 6, c - shift, shift - 1 - c) >= 0
        for a in range(6):
            feat_out[a, c] = jnp.where(mine, own[a, c].astype(F32), far[a, c % 6].astype(F32)).astype(BF16)[:, 0:WIDTH]


def place_features(feat, lines, out):
    for w in range(WINS):
        both = jnp.concatenate([feat[:, w * TOKENS : (w + 1) * TOKENS], jnp.zeros((32, TOKENS), F32)], axis=0).T
        for z in range(2):
            lines[pl.ds(2 * w + z, GRID, stride=8), :] = both[z * GRID : (z + 1) * GRID]
    for a in range(6):
        for c in range(SLOTS):
            at = (a * SLOTS + c) * 8
            out[a, c] = lines[at : at + 8, :].astype(BF16)


class Links:
    def __init__(self, send, recv):
        self.send, self.recv, self.used, self.sent = send, recv, 0, []

    def slot(self):
        self.used += 1
        return self.used - 1

    def copy(self, k, src, dst, to):
        return pltpu.make_async_remote_copy(
            src_ref=src,
            dst_ref=dst,
            send_sem=self.send.at[k],
            recv_sem=self.recv.at[k],
            device_id=to,
            device_id_type=pl.DeviceIdType.MESH,
        )

    def start(self, src, dst, to, k=None):
        made = self.copy(self.slot() if k is None else k, src, dst, to)
        made.start()
        if k is None:
            self.sent.append(made)
        return made

    def group(self, k, whole, to):
        made = self.copy(k, whole, whole, to)
        self.sent.append(made)
        return made

    def many(self, whole, moves):
        k = self.slot()
        for src, dst, to in moves:
            self.start(src, dst, to, k)
        return self.group(k, whole, moves[-1][2])

    def settle(self):
        for made in self.sent:
            made.wait_send()
        self.sent = []


def place():
    lon, lat, head = lax.axis_index("lon"), lax.axis_index("lat"), lax.axis_index("head")
    z, high = lon // 2, lon % 2
    low, core = lat // 2, lat % 2
    return lon, lat, head, z, high, high * 2 + low, core


def at_grid(z, x, core):
    return {"lon": z * 2 + x // 2, "lat": (x % 2) * 2 + core}


def greet(peers):
    barrier = pltpu.get_barrier_semaphore()
    for peer in peers:
        pl.semaphore_signal(barrier, inc=1, device_id=peer, device_id_type=pl.DeviceIdType.MESH)
    return len(peers)


def reduce_peers():
    lon, lat, head, z, high, x, core = place()
    xc = x * 2 + core
    peers = [{"lon": (lon + k) % 16} for k in range(1, 16)]
    peers += [at_grid(z, ((xc + k) % 8) // 2, (xc + k) % 2) for k in range(1, 8)]
    peers += [{"head": (head + k) % 4} for k in range(1, 4)]
    return peers


NAMES = dict(
    xv=pltpu.VMEM((6, SLOTS, 8, MODEL), BF16),
    gv=pltpu.VMEM((6, SLOTS, 8, MODEL), BF16),
    xe=pltpu.VMEM((6, 6, 8, MODEL), BF16),
    ge=pltpu.VMEM((6, 6, 8, MODEL), BF16),
    tabv=pltpu.VMEM((3, 64, TABLE), F32),
    wtv=pltpu.VMEM((3, WIDTH, MODEL), BF16),
    wov=pltpu.VMEM((WIDTH, MODEL), BF16),
    tabw=pltpu.VMEM((16, TABLE_PAD), F32),
    spread=pltpu.VMEM((12, 16, 288), F32),
    maps=pltpu.VMEM((12, 288, 256), BF16),
    bias=pltpu.VMEM((2, 1728, 128), F32),
    xs=pltpu.VMEM((3, 576, 128), F32),
    gs=pltpu.VMEM((3, 576, 128), F32),
    wflip=pltpu.VMEM((MODEL, 288), BF16),
    projs=pltpu.VMEM((WINS, 288, TOKENS), BF16),
    gsofts=pltpu.VMEM((12, TOKENS, TOKENS), F32),
    softs=pltpu.VMEM((12, TOKENS, TOKENS), F32),
    atts=pltpu.VMEM((WINS, WIDTH, TOKENS), BF16),
    scores=pltpu.VMEM((2, 1728, 128), F32),
    dprojs=pltpu.VMEM((WINS, 288, TOKENS), BF16),
    fold=pltpu.VMEM((3, TOKENS, 128), F32),
    sums=pltpu.VMEM((MODEL, MODEL), F32),
    folded=pltpu.VMEM((16, 4096), F32),
    a0=pltpu.VMEM((4, 48, MODEL), BF16),
    ad=pltpu.VMEM((4, 48, MODEL), BF16),
    ax=pltpu.VMEM((4, 48, MODEL), BF16),
    f0=pltpu.VMEM((16, 3, 8, 128), BF16),
    p0=pltpu.VMEM((4, WIDTH, 640), BF16),
    a1=pltpu.VMEM((3, 48, MODEL), BF16),
    f1=pltpu.VMEM((15, 3, 8, 128), BF16),
    p1=pltpu.VMEM((3, WIDTH, 640), BF16),
    a2s=pltpu.VMEM((8, 2, 16, 128), BF16),
    a2=pltpu.VMEM((7, 2, 16, 128), BF16),
    a3=pltpu.VMEM((8, 16, 128), BF16),
    lines=pltpu.VMEM((576, 128), F32),
    f3=pltpu.VMEM((8, 3, 8, 128), BF16),
    send=pltpu.SemaphoreType.DMA((21,)),
    recv=pltpu.SemaphoreType.DMA((21,)),
    load=pltpu.SemaphoreType.DMA((7,)),
    types=pltpu.SMEM((1, 4), jnp.int32),
    shift=pltpu.SMEM((1,), jnp.int32),
)


def main_kernel(first, types_ref, shift_ref, x, g, table, wt, wo, a_out, f_out, own_out, west_out, *scratch):
    v = dict(zip(NAMES, scratch, strict=True))
    lon, lat, head, z, high, xpos, core = place()
    xc = xpos * 2 + core
    step = 1 if first == 0 else 15
    net = Links(v["send"], v["recv"])
    met = greet(reduce_peers())
    loads = []
    given = ((g, "gv"), (x, "xv"), (types_ref, "types"), (shift_ref, "shift"), (table, "tabv"), (wt, "wtv"), (wo, "wov"))
    for src, dst in given:
        made = pltpu.make_async_copy(src, v[dst], v["load"].at[len(loads)])
        made.start()
        loads.append(made)
    with jax.named_scope("enter"):
        for made in loads[0:2]:
            made.wait()
        pl.semaphore_wait(pltpu.get_barrier_semaphore(), met)

    giver = {"lon": (lon + 16 - step) % 16}
    rows, cols = pl.ds((head // 2) * 3, 3), (head % 2) * 3
    quarter = v["ge"].at[rows, pl.ds(cols, 3)]
    halo = [net.start(v["gv"].at[rows, pl.ds(first + cols, 3)], quarter, giver)]
    halo.append(net.start(v["xv"].at[:, pl.ds(first, 6)], v["xe"], giver))
    with jax.named_scope("bias"):
        for made in loads[2:5]:
            made.wait()
        types = [v["types"][0, w] for w in range(WINS)]
        shift = v["shift"][0]
        expand_bias(types, shift, v["tabv"], v["tabw"], v["spread"], v["maps"], v["bias"])
    mixed = [c for c in range(first, first + 6)]
    still = [c for c in range(SLOTS) if c not in mixed]
    place_rows(v["xv"], None, shift, v["xs"], first, still)
    place_rows(v["gv"], None, shift, v["gs"], first, still)
    with jax.named_scope("still"):
        loads[5].wait()
        loads[6].wait()
        wts = v["wtv"][...].reshape(3 * WIDTH, MODEL)
        wos = v["wov"][...]
        v["wflip"][...] = wts.astype(F32).T.astype(BF16)

    with jax.named_scope("halo_q"):
        halo[0].wait_recv()
    handed = [net.start(quarter, quarter, {"head": (head + j) % 4}) for j in range(1, 4)]
    with jax.named_scope("halo_x"):
        halo[1].wait_recv()
    with jax.named_scope("forward"):
        place_rows(v["xv"], v["xe"], shift, v["xs"], first, mixed)
        forward(v["xs"], wts, v["bias"], v["projs"], v["softs"], v["atts"])
    with jax.named_scope("halo_g"):
        for made in handed:
            made.wait_recv()
    with jax.named_scope("backward"):
        place_rows(v["gv"], v["ge"], shift, v["gs"], first, mixed)
        backward(v["xs"], v["gs"], wos, v["projs"], v["softs"], v["gsofts"], v["atts"], v["scores"], v["sums"], v["dprojs"])

    def zs(k):
        return {"lon": ((z + k) % 8) * 2 + high}

    a0, f0, p0 = v["a0"], v["f0"], v["p0"]
    a1, f1, p1 = v["a1"], v["f1"], v["p1"]
    ad, ax, a2s, a2, a3, f3 = (v[n] for n in ("ad", "ax", "a2s", "a2", "a3", "f3"))
    partner = at_grid(z, xpos, 1 - core)

    def chunk(i, side):
        return v["sums"][pl.ds(pl.multiple_of((2 * i + side) * 48, 16), 48), :]

    for i in range(4):
        a0[i] = chunk(i, 1 - core).astype(BF16)
    twin = net.start(a0, ad, partner)
    with jax.named_scope("fold"):
        fold_scores(types, v["scores"], v["maps"], v["fold"], v["folded"], f0)
    with jax.named_scope("sum_d"):
        twin.wait_recv()
        for i in range(4):
            ax[i] = (chunk(i, core) + ad[i].astype(F32)).astype(BF16)
    one = net.many(a1, [(ax.at[(xpos + k) % 4], a1.at[k - 1], at_grid(z, (xpos + k) % 4, core)) for k in range(1, 4)])
    two = net.many(f1, [(f0.at[(lon + k) % 16], f1.at[k - 1], {"lon": (lon + k) % 16}) for k in range(1, 16)])
    with jax.named_scope("pieces"):
        pieces_out(v["wflip"], v["dprojs"], p0)
    pieces = net.many(p1, [(p0.at[(head + k) % 4], p1.at[k - 1], {"head": (head + k) % 4}) for k in range(1, 4)])

    with jax.named_scope("sum_a"):
        total = chunk(xpos, core) + ad[xpos].astype(F32)
        one.wait_recv()
        for k in range(3):
            total = total + a1[k].astype(F32)
        tiles = [total[r * 16 : (r + 1) * 16, k * 128 : (k + 1) * 128].astype(BF16) for r in range(3) for k in range(3)]
        for k in range(8):
            a2s[k, 0] = tiles[k]
            a2s[k, 1] = tiles[8]
    three_ = net.many(a2, [(a2s.at[(z + k) % 8], a2.at[k - 1], zs(k)) for k in range(1, 8)])

    with jax.named_scope("sum_f"):
        lines = f0[lon].astype(F32)
        two.wait_recv()
        for k in range(15):
            lines = lines + f1[k].astype(F32)
        f3[z] = lines.astype(BF16)
    part = f3.at[pl.ds(0, 7)]
    five = net.many(part, [(f3.at[z], f3.at[z], zs(k)) for k in range(1, 8)])

    with jax.named_scope("sum_z"):
        block = a2s[z].astype(F32)
        three_.wait_recv()
        for k in range(7):
            block = block + a2[k].astype(F32)
        a3[z] = block[0].astype(BF16)
    six = net.many(a3.at[pl.ds(0, 7)], [(a3.at[z], a3.at[z], zs(k)) for k in range(1, 8)])
    a_out[xc, 8] = block[1].astype(BF16)

    with jax.named_scope("sum_p"):
        feat = p0[head].astype(F32)
        pieces.wait_recv()
        for k in range(3):
            feat = feat + p1[k].astype(F32)
        place_features(feat, v["lines"], own_out)
    net.settle()
    back = net.start(own_out.at[:, pl.ds(first, 6)], west_out, {"lon": (lon + step) % 16})

    with jax.named_scope("all_f"):
        five.wait_recv()
    mine = f_out.at[xc, pl.ds(0, 7)]
    arrive_f = [net.start(part, mine, at_grid(z, (xpos + k) % 4, core)) for k in range(1, 4)]
    cross_f, cross_a = net.slot(), net.slot()
    net.start(part, mine, partner, cross_f)
    f_out[xc] = f3[...]
    with jax.named_scope("all_a"):
        six.wait_recv()
    a_out[xc, 0:8] = a3[...]
    arrive = [net.start(a_out.at[xc], a_out.at[xc], at_grid(z, (xpos + k) % 4, core)) for k in range(1, 4)]
    net.start(a_out.at[xc], a_out.at[xc], partner, cross_a)
    with jax.named_scope("forward_x"):
        for k in range(1, 4):
            there = ((xpos + 4 - k) % 4) * 2 + core
            arrive_f[k - 1].wait_recv()
            ref = f_out.at[there, pl.ds(0, 7)]
            net.start(ref, ref, partner, cross_f)
        for k in range(1, 4):
            there = ((xpos + 4 - k) % 4) * 2 + core
            arrive[k - 1].wait_recv()
            net.start(a_out.at[there], a_out.at[there], partner, cross_a)
    cross = [net.group(cross_f, f_out.at[pl.ds(0, 4), pl.ds(0, 7)], partner), net.group(cross_a, a_out.at[pl.ds(0, 4)], partner)]
    net.settle()
    with jax.named_scope("last"):
        back.wait_recv()
        for made in cross:
            made.wait_recv()


def per_device(features, attend_weight, output_weight, bias_table, bias_type, window_shift, grad_out):
    x = features.transpose(1, 2, 0, 3)
    g = grad_out.transpose(1, 2, 0, 3)
    wt = attend_weight.transpose(0, 2, 1)
    table = bias_table.transpose(1, 0, 2)

    def run(first):
        return pl.pallas_call(
            functools.partial(main_kernel, first),
            out_shape=(
                jax.ShapeDtypeStruct((8, 9, 16, 128), BF16),
                jax.ShapeDtypeStruct((8, 8, 3, 8, 128), BF16),
                jax.ShapeDtypeStruct((6, SLOTS, 8, 128), BF16),
                jax.ShapeDtypeStruct((6, 6, 8, 128), BF16),
            ),
            in_specs=[ANY] * 7,
            out_specs=(VMEM,) * 4,
            scratch_shapes=list(NAMES.values()),
            compiler_params=pltpu.CompilerParams(
                vmem_limit_bytes=56 << 20, collective_id=1 if first == 0 else 2, has_side_effects=True
            ),
            name="block_east" if first == 0 else "block_west",
        )

    args = (bias_type.T, window_shift, x, g, table, wt, output_weight)
    sums, folded, own, borrowed = lax.cond(window_shift[0] <= 6, run(0), run(6), *args)
    return finish(window_shift, sums, folded, own, borrowed)


def finish(window_shift, sums, folded, own, borrowed):
    attend_grad, output_grad, bias_grad, feat = pl.pallas_call(
        finish_kernel,
        out_shape=(
            jax.ShapeDtypeStruct((3, WIDTH, MODEL), F32),
            jax.ShapeDtypeStruct((WIDTH, MODEL), F32),
            jax.ShapeDtypeStruct((3, 64, TABLE), F32),
            jax.ShapeDtypeStruct((6, SLOTS, 8, WIDTH), BF16),
        ),
        in_specs=[SMEM, VMEM, VMEM, VMEM, VMEM],
        out_specs=(VMEM,) * 4,
        compiler_params=pltpu.CompilerParams(vmem_limit_bytes=40 << 20),
        name="finish",
    )(window_shift, sums, folded, own, borrowed)
    return (
        feat.transpose(2, 0, 1, 3),
        attend_grad.transpose(0, 2, 1),
        output_grad,
        bias_grad.transpose(1, 0, 2),
    )


def solution(mesh):
    placed = (
        P(None, "lat", "lon", None),
        P(None, None, "head"),
        P("head", None),
        P(None, "head", None),
        P(None, "lat"),
        P(),
        P(None, "lat", "lon", None),
    )
    return jax.shard_map(
        per_device,
        mesh=mesh,
        in_specs=placed,
        out_specs=(
            P(None, "lat", "lon", "head"),
            P(None, None, "head"),
            P("head", None),
            P(None, "head", None),
        ),
        check_vma=False,
    )
```

```python
import functools

import jax
import jax.numpy as jnp
from jax import lax
from jax.experimental import pallas as pl
from jax.experimental.pallas import tpu as pltpu
from jax.sharding import PartitionSpec as P

F32 = jnp.float32
BF16 = jnp.bfloat16
HEADS = 3
WINS = 4
WIDTH = 96
HEAD = 32
SLOTS = 12
GRID = 72
TOKENS = 144
MODEL = 384
SPAN = 23
TABLE = 3312
TABLE_PAD = 3328
GROUP = 138
SCALE = HEAD ** (-0.5)
VMEM = pl.BlockSpec(memory_space=pltpu.VMEM)
SMEM = pl.BlockSpec(memory_space=pltpu.SMEM)
ANY = pl.BlockSpec(memory_space=pl.ANY)


def dot(a, b, da, db):
    return lax.dot_general(a, b, (((da,), (db,)), ((), ())), preferred_element_type=F32)


def three(x):
    hi = x.astype(BF16)
    rest = x - hi.astype(F32)
    mid = rest.astype(BF16)
    return hi, mid, (rest - mid.astype(F32)).astype(BF16)


def fold_map(ci, shift):
    rows = lax.broadcasted_iota(jnp.int32, (288, 256), 0)
    lane = lax.broadcasted_iota(jnp.int32, (1, 256), 1)
    block = lane // SLOTS
    cj = lane - block * SLOTS
    wrap = jnp.where(ci < shift, 12, 0) - jnp.where(cj < shift, 12, 0)
    target = block * SPAN + (11 + ci) - cj + wrap
    target = jnp.where(lane < TOKENS, target, -1)
    return jnp.where(rows == target, 1.0, 0.0).astype(BF16)


def expand_bias(types, shift, table, tabw, spread, maps, bias):
    for h in range(HEADS):
        for w in range(WINS):
            n = h * WINS + w
            tabw[n : n + 1, 0:TABLE] = table[h, pl.ds(types[w], 1), :]
    spread[...] = jnp.zeros_like(spread)
    for zi in range(2):
        for ai in range(6):
            for zj in range(2):
                at = zi * 1656 + zj * 828 + ai * GROUP
                spread[zi * 6 + ai, 0:12, zj * GROUP : (zj + 1) * GROUP] = tabw[0:12, at : at + GROUP]
    parts = three(spread[...].reshape(192, 288))
    for ci in range(SLOTS):
        chosen = fold_map(ci, shift)
        maps[ci] = chosen
        full = dot(parts[0], chosen, 1, 0) + dot(parts[1], chosen, 1, 0) + dot(parts[2], chosen, 1, 0)
        for n in range(12):
            for k in range(2):
                bias[k, pl.ds(n * SLOTS + ci, 12, stride=TOKENS), :] = full[
                    n * 16 : n * 16 + 12, k * 128 : (k + 1) * 128
                ]


def window_rows(scratch, w):
    halves = []
    for z in range(2):
        lanes = [scratch[k, pl.ds(2 * w + z, GRID, stride=8), :] for k in range(3)]
        halves.append(jnp.concatenate(lanes, axis=1))
    return jnp.concatenate(halves, axis=0).astype(BF16)


def place_rows(own, borrowed, shift, scratch, first, slots):
    for c in slots:
        for a in range(6):
            rows = own[a, c].astype(F32)
            if borrowed is not None:
                keep = c >= shift if first == 0 else c < shift
                rows = jnp.where(keep, rows, borrowed[a, c - first].astype(F32))
            for k in range(3):
                scratch[k, (a * SLOTS + c) * 8 : (a * SLOTS + c + 1) * 8, :] = rows[:, k * 128 : (k + 1) * 128]


def only(x, h):
    return jnp.concatenate([x[k * HEAD : (k + 1) * HEAD] if k == h else jnp.zeros((HEAD, x.shape[1]), x.dtype) for k in range(HEADS)], axis=0)


def forward(xs, wts, bias, proj_out, softs, atts):
    tops = {}
    for w in range(WINS):
        xw = window_rows(xs, w)
        proj = dot(wts, xw, 1, 1).astype(BF16)
        proj_out[w] = proj
        q = dot(xw, wts[0:WIDTH], 1, 1).astype(BF16)
        for h in range(HEADS):
            n = h * WINS + w
            rows = slice(n * TOKENS, (n + 1) * TOKENS)
            added = jnp.concatenate([bias[0, rows, :], bias[1, rows, 0:16]], axis=1)
            logits = dot(q, only(proj[96:192], h), 1, 0) * SCALE + added
            softs[n] = logits
            tops[n] = jnp.max(logits, axis=1, keepdims=True)
    for w in range(WINS):
        sums = []
        for h in range(HEADS):
            n = h * WINS + w
            raised = jnp.exp(softs[n] - tops[n])
            softs[n] = raised
            sums.append(1.0 / jnp.sum(raised, axis=1, keepdims=True))
        att = []
        for h in range(HEADS):
            n = h * WINS + w
            soft = softs[n] * sums[h]
            softs[n] = soft
            att.append(dot(proj_out[w, 192 + h * HEAD : 192 + (h + 1) * HEAD, :], soft.astype(BF16), 1, 1))
        atts[w] = jnp.concatenate(att, axis=0).astype(BF16)


def backward(xs, gs, wos, proj_in, softs, gsofts, atts, scores, sums, dprojs):
    rowsums, dats = {}, {}
    for w in range(WINS):
        gw = window_rows(gs, w)
        dats[w] = dot(wos, gw, 1, 1).astype(BF16)
        da = dot(gw, wos, 1, 1).astype(BF16)
        vt = proj_in[w, 192:288, :]
        for h in range(HEADS):
            n = h * WINS + w
            gsoft = dot(da, only(vt, h), 1, 0)
            gsofts[n] = gsoft
            rowsums[n] = jnp.sum(softs[n] * gsoft, axis=1, keepdims=True)
        low = dot(atts[w], gw, 1, 0)
        if w == 0:
            sums[288:384, :] = low
        else:
            sums[288:384, :] += low
    for w in range(WINS):
        dq, dk, dv = [], [], []
        for h in range(HEADS):
            n = h * WINS + w
            rows = slice(n * TOKENS, (n + 1) * TOKENS)
            own = slice(h * HEAD, (h + 1) * HEAD)
            soft = softs[n]
            gsc = soft * (gsofts[n] - rowsums[n])
            scores[0, rows, :] = gsc[:, 0:128]
            scores[1, rows, 0:16] = gsc[:, 128:144]
            gh = gsc.astype(BF16)
            dv.append(dot(dats[w][own], soft.astype(BF16), 1, 0))
            dq.append(dot(proj_in[w, 96 + h * HEAD : 96 + (h + 1) * HEAD, :], gh, 1, 1) * SCALE)
            dk.append(dot(proj_in[w, own, :], gh, 1, 0) * SCALE)
        dproj = jnp.concatenate(dq + dk + dv, axis=0).astype(BF16)
        dprojs[w] = dproj
        top = dot(dproj, window_rows(xs, w), 1, 0)
        if w == 0:
            sums[0:288, :] = top
        else:
            sums[0:288, :] += top


def fold_scores(types, scores, maps, fold, folded, folded_out):
    total = None
    for ci in range(SLOTS):
        part = jnp.concatenate(
            [scores[0, pl.ds(ci, TOKENS, stride=SLOTS), :], scores[1, pl.ds(ci, TOKENS, stride=SLOTS), :][:, 0:16]], axis=1
        )
        term = dot(part.astype(BF16), maps[ci][:, 0:TOKENS], 1, 1)
        total = term if total is None else total + term
    for k in range(3):
        wide = min(128, 288 - k * 128)
        fold[k, :, 0:wide] = total[:, k * 128 : k * 128 + wide]
    folded[...] = jnp.zeros_like(folded)
    for zi in range(2):
        for ai in range(6):
            got = [fold[k, pl.ds(zi * 6 + ai, 12, stride=12), :] for k in range(3)]
            line = jnp.concatenate(got, axis=1)
            for zj in range(2):
                at = zi * 1656 + zj * 828 + ai * GROUP
                folded[0:12, at : at + GROUP] = line[:, zj * GROUP : (zj + 1) * GROUP]
    row = lax.broadcasted_iota(jnp.int32, (16, 128), 0)
    lane = lax.broadcasted_iota(jnp.int32, (16, 128), 1)
    marks = jnp.zeros((16, 128), jnp.int32)
    for w in range(WINS):
        marks = jnp.where(row == w, types[w], marks)
    folded[:, 3200:TABLE_PAD] = jnp.where(lane >= 112, marks.astype(F32), folded[:, 3200:TABLE_PAD])
    for i in range(16):
        left, right = (folded[:, i * 256 + k * 128 : i * 256 + (k + 1) * 128] for k in range(2))
        folded_out[i, 0] = left[0:8].astype(BF16)
        folded_out[i, 1] = right[0:8].astype(BF16)
        folded_out[i, 2] = jnp.concatenate([left[8:12], right[8:12]], axis=0).astype(BF16)


def pieces_out(wflip, dprojs, piece):
    for w in range(WINS):
        back = dot(wflip[...], dprojs[w], 1, 0).astype(BF16)
        for r in range(4):
            piece[r, :, w * TOKENS : (w + 1) * TOKENS] = back[r * WIDTH : (r + 1) * WIDTH]
    for r in range(4):
        piece[r, :, 576:640] = jnp.zeros((WIDTH, 64), BF16)


def finish_kernel(shift_ref, sums, folded, own, far, attend_out, output_out, bias_out, feat_out):
    first, last = [], []
    for q in range(4):
        high, low = [], []
        for z in range(7):
            for xh in range(2):
                part = folded[xh * 4 + q, z].astype(F32)
                high += [part[0], part[1]]
                low += [part[2, 0:4], part[2, 4:8]]
        first.append(jnp.concatenate(high[0:26], axis=1))
        last.append(jnp.concatenate(low[0:26], axis=1))
    marks = jnp.concatenate([first[q][0:4, TABLE : TABLE + 1] for q in range(4)], axis=0) * 0.0625
    lane = lax.broadcasted_iota(jnp.int32, (16, 128), 1).astype(F32)
    pick = jnp.where(lane == marks, 1.0, 0.0).T[0:64].astype(BF16)
    for h in range(HEADS):
        rows = [first[q][h * WINS : (h + 1) * WINS] if h < 2 else last[q] for q in range(4)]
        bias_out[h] = dot(pick, jnp.concatenate(rows, axis=0).astype(BF16), 1, 0)[:, 0:TABLE]
    for i in range(8):
        for r in range(3):
            for k in range(3):
                part = sums[i, r * 3 + k].astype(F32)
                at, lanes = (i % 2) * 48 + r * 16, slice(k * 128, (k + 1) * 128)
                if i < 6:
                    attend_out[i // 2, at : at + 16, lanes] = part
                else:
                    output_out[at : at + 16, lanes] = part
    shift = shift_ref[0]
    for c in range(SLOTS):
        mine = jnp.where(shift <= 6, c - shift, shift - 1 - c) >= 0
        for a in range(6):
            feat_out[a, c] = jnp.where(mine, own[a, c].astype(F32), far[a, c % 6].astype(F32)).astype(BF16)[:, 0:WIDTH]


def place_features(feat, lines, out):
    for w in range(WINS):
        both = jnp.concatenate([feat[:, w * TOKENS : (w + 1) * TOKENS], jnp.zeros((32, TOKENS), F32)], axis=0).T
        for z in range(2):
            lines[pl.ds(2 * w + z, GRID, stride=8), :] = both[z * GRID : (z + 1) * GRID]
    for a in range(6):
        for c in range(SLOTS):
            at = (a * SLOTS + c) * 8
            out[a, c] = lines[at : at + 8, :].astype(BF16)


class Links:
    def __init__(self, send, recv):
        self.send, self.recv, self.used, self.sent = send, recv, 0, []

    def slot(self):
        self.used += 1
        return self.used - 1

    def copy(self, k, src, dst, to):
        return pltpu.make_async_remote_copy(
            src_ref=src,
            dst_ref=dst,
            send_sem=self.send.at[k],
            recv_sem=self.recv.at[k],
            device_id=to,
            device_id_type=pl.DeviceIdType.MESH,
        )

    def start(self, src, dst, to, k=None):
        made = self.copy(self.slot() if k is None else k, src, dst, to)
        made.start()
        if k is None:
            self.sent.append(made)
        return made

    def group(self, k, whole, to):
        made = self.copy(k, whole, whole, to)
        self.sent.append(made)
        return made

    def many(self, whole, moves):
        k = self.slot()
        for src, dst, to in moves:
            self.start(src, dst, to, k)
        return self.group(k, whole, moves[-1][2])

    def settle(self):
        for made in self.sent:
            made.wait_send()
        self.sent = []


def place():
    lon, lat, head = lax.axis_index("lon"), lax.axis_index("lat"), lax.axis_index("head")
    z, high = lon // 2, lon % 2
    low, core = lat // 2, lat % 2
    return lon, lat, head, z, high, high * 2 + low, core


def at_grid(z, x, core):
    return {"lon": z * 2 + x // 2, "lat": (x % 2) * 2 + core}


def greet(peers):
    barrier = pltpu.get_barrier_semaphore()
    for peer in peers:
        pl.semaphore_signal(barrier, inc=1, device_id=peer, device_id_type=pl.DeviceIdType.MESH)
    return len(peers)


def reduce_peers():
    lon, lat, head, z, high, x, core = place()
    xc = x * 2 + core
    peers = [{"lon": (lon + k) % 16} for k in range(1, 16)]
    peers += [at_grid(z, ((xc + k) % 8) // 2, (xc + k) % 2) for k in range(1, 8)]
    peers += [{"head": (head + k) % 4} for k in range(1, 4)]
    return peers


NAMES = dict(
    xv=pltpu.VMEM((6, SLOTS, 8, MODEL), BF16),
    gv=pltpu.VMEM((6, SLOTS, 8, MODEL), BF16),
    xe=pltpu.VMEM((6, 6, 8, MODEL), BF16),
    ge=pltpu.VMEM((6, 6, 8, MODEL), BF16),
    tabv=pltpu.VMEM((3, 64, TABLE), F32),
    wtv=pltpu.VMEM((3, WIDTH, MODEL), BF16),
    wov=pltpu.VMEM((WIDTH, MODEL), BF16),
    tabw=pltpu.VMEM((16, TABLE_PAD), F32),
    spread=pltpu.VMEM((12, 16, 288), F32),
    maps=pltpu.VMEM((12, 288, 256), BF16),
    bias=pltpu.VMEM((2, 1728, 128), F32),
    xs=pltpu.VMEM((3, 576, 128), F32),
    gs=pltpu.VMEM((3, 576, 128), F32),
    wflip=pltpu.VMEM((MODEL, 288), BF16),
    projs=pltpu.VMEM((WINS, 288, TOKENS), BF16),
    gsofts=pltpu.VMEM((12, TOKENS, TOKENS), F32),
    softs=pltpu.VMEM((12, TOKENS, TOKENS), F32),
    atts=pltpu.VMEM((WINS, WIDTH, TOKENS), BF16),
    scores=pltpu.VMEM((2, 1728, 128), F32),
    dprojs=pltpu.VMEM((WINS, 288, TOKENS), BF16),
    fold=pltpu.VMEM((3, TOKENS, 128), F32),
    sums=pltpu.VMEM((MODEL, MODEL), F32),
    folded=pltpu.VMEM((16, 4096), F32),
    a0=pltpu.VMEM((4, 48, MODEL), BF16),
    ad=pltpu.VMEM((4, 48, MODEL), BF16),
    ax=pltpu.VMEM((4, 48, MODEL), BF16),
    f0=pltpu.VMEM((16, 3, 8, 128), BF16),
    p0=pltpu.VMEM((4, WIDTH, 640), BF16),
    a1=pltpu.VMEM((3, 48, MODEL), BF16),
    f1=pltpu.VMEM((15, 3, 8, 128), BF16),
    p1=pltpu.VMEM((3, WIDTH, 640), BF16),
    a2s=pltpu.VMEM((8, 2, 16, 128), BF16),
    a2=pltpu.VMEM((7, 2, 16, 128), BF16),
    a3=pltpu.VMEM((8, 16, 128), BF16),
    lines=pltpu.VMEM((576, 128), F32),
    f3=pltpu.VMEM((8, 3, 8, 128), BF16),
    send=pltpu.SemaphoreType.DMA((22,)),
    recv=pltpu.SemaphoreType.DMA((22,)),
    load=pltpu.SemaphoreType.DMA((7,)),
    types=pltpu.SMEM((1, 4), jnp.int32),
    shift=pltpu.SMEM((1,), jnp.int32),
)


def main_kernel(first, types_ref, shift_ref, x, g, table, wt, wo, a_out, f_out, own_out, west_out, *scratch):
    v = dict(zip(NAMES, scratch, strict=True))
    lon, lat, head, z, high, xpos, core = place()
    xc = xpos * 2 + core
    step = 1 if first == 0 else 15
    net = Links(v["send"], v["recv"])
    met = greet(reduce_peers())
    loads = []
    given = ((g, "gv"), (x, "xv"), (types_ref, "types"), (shift_ref, "shift"), (table, "tabv"), (wt, "wtv"), (wo, "wov"))
    for src, dst in given:
        made = pltpu.make_async_copy(src, v[dst], v["load"].at[len(loads)])
        made.start()
        loads.append(made)
    with jax.named_scope("enter"):
        for made in loads[0:2]:
            made.wait()
        pl.semaphore_wait(pltpu.get_barrier_semaphore(), met)

    giver = {"lon": (lon + 16 - step) % 16}
    reach, tail = pl.ds(first, 6), pl.ds(4, 2)
    row = v["ge"].at[head]
    halo = [net.start(v["gv"].at[head, reach], row, giver)]
    halo.append(net.start(v["xv"].at[:, reach], v["xe"], giver))
    halo.append(net.start(v["gv"].at[tail, reach], v["ge"].at[tail], giver))
    with jax.named_scope("bias"):
        for made in loads[2:5]:
            made.wait()
        types = [v["types"][0, w] for w in range(WINS)]
        shift = v["shift"][0]
        expand_bias(types, shift, v["tabv"], v["tabw"], v["spread"], v["maps"], v["bias"])
    mixed = [c for c in range(first, first + 6)]
    still = [c for c in range(SLOTS) if c not in mixed]
    place_rows(v["xv"], None, shift, v["xs"], first, still)
    place_rows(v["gv"], None, shift, v["gs"], first, still)
    with jax.named_scope("still"):
        loads[5].wait()
        loads[6].wait()
        wts = v["wtv"][...].reshape(3 * WIDTH, MODEL)
        wos = v["wov"][...]
        v["wflip"][...] = wts.astype(F32).T.astype(BF16)

    with jax.named_scope("halo_q"):
        halo[0].wait_recv()
    handed = [net.start(row, row, {"head": (head + j) % 4}) for j in range(1, 4)]
    with jax.named_scope("halo_x"):
        halo[1].wait_recv()
    with jax.named_scope("forward"):
        place_rows(v["xv"], v["xe"], shift, v["xs"], first, mixed)
        forward(v["xs"], wts, v["bias"], v["projs"], v["softs"], v["atts"])
    with jax.named_scope("halo_g"):
        for made in [halo[2], *handed]:
            made.wait_recv()
    with jax.named_scope("backward"):
        place_rows(v["gv"], v["ge"], shift, v["gs"], first, mixed)
        backward(v["xs"], v["gs"], wos, v["projs"], v["softs"], v["gsofts"], v["atts"], v["scores"], v["sums"], v["dprojs"])

    def zs(k):
        return {"lon": ((z + k) % 8) * 2 + high}

    a0, f0, p0 = v["a0"], v["f0"], v["p0"]
    a1, f1, p1 = v["a1"], v["f1"], v["p1"]
    ad, ax, a2s, a2, a3, f3 = (v[n] for n in ("ad", "ax", "a2s", "a2", "a3", "f3"))
    partner = at_grid(z, xpos, 1 - core)

    def chunk(i, side):
        return v["sums"][pl.ds(pl.multiple_of((2 * i + side) * 48, 16), 48), :]

    for i in range(4):
        a0[i] = chunk(i, 1 - core).astype(BF16)
    twin = net.start(a0, ad, partner)
    with jax.named_scope("fold"):
        fold_scores(types, v["scores"], v["maps"], v["fold"], v["folded"], f0)
    with jax.named_scope("sum_d"):
        twin.wait_recv()
        for i in range(4):
            ax[i] = (chunk(i, core) + ad[i].astype(F32)).astype(BF16)
    one = net.many(a1, [(ax.at[(xpos + k) % 4], a1.at[k - 1], at_grid(z, (xpos + k) % 4, core)) for k in range(1, 4)])
    two = net.many(f1, [(f0.at[(lon + k) % 16], f1.at[k - 1], {"lon": (lon + k) % 16}) for k in range(1, 16)])
    with jax.named_scope("pieces"):
        pieces_out(v["wflip"], v["dprojs"], p0)
    pieces = net.many(p1, [(p0.at[(head + k) % 4], p1.at[k - 1], {"head": (head + k) % 4}) for k in range(1, 4)])

    with jax.named_scope("sum_a"):
        total = chunk(xpos, core) + ad[xpos].astype(F32)
        one.wait_recv()
        for k in range(3):
            total = total + a1[k].astype(F32)
        tiles = [total[r * 16 : (r + 1) * 16, k * 128 : (k + 1) * 128].astype(BF16) for r in range(3) for k in range(3)]
        for k in range(8):
            a2s[k, 0] = tiles[k]
            a2s[k, 1] = tiles[8]
    three_ = net.many(a2, [(a2s.at[(z + k) % 8], a2.at[k - 1], zs(k)) for k in range(1, 8)])

    with jax.named_scope("sum_f"):
        lines = f0[lon].astype(F32)
        two.wait_recv()
        for k in range(15):
            lines = lines + f1[k].astype(F32)
        f3[z] = lines.astype(BF16)
    part = f3.at[pl.ds(0, 7)]
    five = net.many(part, [(f3.at[z], f3.at[z], zs(k)) for k in range(1, 8)])

    with jax.named_scope("sum_z"):
        block = a2s[z].astype(F32)
        three_.wait_recv()
        for k in range(7):
            block = block + a2[k].astype(F32)
        a3[z] = block[0].astype(BF16)
    six = net.many(a3.at[pl.ds(0, 7)], [(a3.at[z], a3.at[z], zs(k)) for k in range(1, 8)])
    a_out[xc, 8] = block[1].astype(BF16)

    with jax.named_scope("sum_p"):
        feat = p0[head].astype(F32)
        pieces.wait_recv()
        for k in range(3):
            feat = feat + p1[k].astype(F32)
        place_features(feat, v["lines"], own_out)
    net.settle()
    back = net.start(own_out.at[:, pl.ds(first, 6)], west_out, {"lon": (lon + step) % 16})

    with jax.named_scope("all_f"):
        five.wait_recv()
    mine = f_out.at[xc, pl.ds(0, 7)]
    arrive_f = [net.start(part, mine, at_grid(z, (xpos + k) % 4, core)) for k in range(1, 4)]
    cross_f, cross_a = net.slot(), net.slot()
    net.start(part, mine, partner, cross_f)
    f_out[xc] = f3[...]
    with jax.named_scope("all_a"):
        six.wait_recv()
    a_out[xc, 0:8] = a3[...]
    arrive = [net.start(a_out.at[xc], a_out.at[xc], at_grid(z, (xpos + k) % 4, core)) for k in range(1, 4)]
    net.start(a_out.at[xc], a_out.at[xc], partner, cross_a)
    with jax.named_scope("forward_x"):
        for k in range(1, 4):
            there = ((xpos + 4 - k) % 4) * 2 + core
            arrive_f[k - 1].wait_recv()
            ref = f_out.at[there, pl.ds(0, 7)]
            net.start(ref, ref, partner, cross_f)
        for k in range(1, 4):
            there = ((xpos + 4 - k) % 4) * 2 + core
            arrive[k - 1].wait_recv()
            net.start(a_out.at[there], a_out.at[there], partner, cross_a)
    cross = [net.group(cross_f, f_out.at[pl.ds(0, 4), pl.ds(0, 7)], partner), net.group(cross_a, a_out.at[pl.ds(0, 4)], partner)]
    net.settle()
    with jax.named_scope("last"):
        back.wait_recv()
        for made in cross:
            made.wait_recv()


def per_device(features, attend_weight, output_weight, bias_table, bias_type, window_shift, grad_out):
    x = features.transpose(1, 2, 0, 3)
    g = grad_out.transpose(1, 2, 0, 3)
    wt = attend_weight.transpose(0, 2, 1)
    table = bias_table.transpose(1, 0, 2)

    def run(first):
        return pl.pallas_call(
            functools.partial(main_kernel, first),
            out_shape=(
                jax.ShapeDtypeStruct((8, 9, 16, 128), BF16),
                jax.ShapeDtypeStruct((8, 8, 3, 8, 128), BF16),
                jax.ShapeDtypeStruct((6, SLOTS, 8, 128), BF16),
                jax.ShapeDtypeStruct((6, 6, 8, 128), BF16),
            ),
            in_specs=[ANY] * 7,
            out_specs=(VMEM,) * 4,
            scratch_shapes=list(NAMES.values()),
            compiler_params=pltpu.CompilerParams(
                vmem_limit_bytes=56 << 20, collective_id=1 if first == 0 else 2, has_side_effects=True
            ),
            name="block_east" if first == 0 else "block_west",
        )

    args = (bias_type.T, window_shift, x, g, table, wt, output_weight)
    sums, folded, own, borrowed = lax.cond(window_shift[0] <= 6, run(0), run(6), *args)
    return finish(window_shift, sums, folded, own, borrowed)


def finish(window_shift, sums, folded, own, borrowed):
    attend_grad, output_grad, bias_grad, feat = pl.pallas_call(
        finish_kernel,
        out_shape=(
            jax.ShapeDtypeStruct((3, WIDTH, MODEL), F32),
            jax.ShapeDtypeStruct((WIDTH, MODEL), F32),
            jax.ShapeDtypeStruct((3, 64, TABLE), F32),
            jax.ShapeDtypeStruct((6, SLOTS, 8, WIDTH), BF16),
        ),
        in_specs=[SMEM, VMEM, VMEM, VMEM, VMEM],
        out_specs=(VMEM,) * 4,
        compiler_params=pltpu.CompilerParams(vmem_limit_bytes=40 << 20),
        name="finish",
    )(window_shift, sums, folded, own, borrowed)
    return (
        feat.transpose(2, 0, 1, 3),
        attend_grad.transpose(0, 2, 1),
        output_grad,
        bias_grad.transpose(1, 0, 2),
    )


def solution(mesh):
    placed = (
        P(None, "lat", "lon", None),
        P(None, None, "head"),
        P("head", None),
        P(None, "head", None),
        P(None, "lat"),
        P(),
        P(None, "lat", "lon", None),
    )
    return jax.shard_map(
        per_device,
        mesh=mesh,
        in_specs=placed,
        out_specs=(
            P(None, "lat", "lon", "head"),
            P(None, None, "head"),
            P("head", None),
            P(None, "head", None),
        ),
        check_vma=False,
    )
```

```python
import functools

import jax
import jax.numpy as jnp
from jax import lax
from jax.experimental import pallas as pl
from jax.experimental.pallas import tpu as pltpu
from jax.sharding import PartitionSpec as P

F32 = jnp.float32
BF16 = jnp.bfloat16
HEADS = 3
WINS = 4
WIDTH = 96
HEAD = 32
SLOTS = 12
GRID = 72
TOKENS = 144
MODEL = 384
SPAN = 23
TABLE = 3312
TABLE_PAD = 3328
GROUP = 138
SCALE = HEAD ** (-0.5)
VMEM = pl.BlockSpec(memory_space=pltpu.VMEM)
SMEM = pl.BlockSpec(memory_space=pltpu.SMEM)
ANY = pl.BlockSpec(memory_space=pl.ANY)


def dot(a, b, da, db):
    return lax.dot_general(a, b, (((da,), (db,)), ((), ())), preferred_element_type=F32)


def three(x):
    hi = x.astype(BF16)
    rest = x - hi.astype(F32)
    mid = rest.astype(BF16)
    return hi, mid, (rest - mid.astype(F32)).astype(BF16)


def fold_map(ci, shift):
    rows = lax.broadcasted_iota(jnp.int32, (288, 256), 0)
    lane = lax.broadcasted_iota(jnp.int32, (1, 256), 1)
    block = lane // SLOTS
    cj = lane - block * SLOTS
    wrap = jnp.where(ci < shift, 12, 0) - jnp.where(cj < shift, 12, 0)
    target = block * SPAN + (11 + ci) - cj + wrap
    target = jnp.where(lane < TOKENS, target, -1)
    return jnp.where(rows == target, 1.0, 0.0).astype(BF16)


def expand_bias(types, shift, table, tabw, spread, maps, bias):
    for h in range(HEADS):
        for w in range(WINS):
            n = h * WINS + w
            tabw[n : n + 1, 0:TABLE] = table[h, pl.ds(types[w], 1), :]
    spread[...] = jnp.zeros_like(spread)
    for zi in range(2):
        for ai in range(6):
            for zj in range(2):
                at = zi * 1656 + zj * 828 + ai * GROUP
                spread[zi * 6 + ai, 0:12, zj * GROUP : (zj + 1) * GROUP] = tabw[0:12, at : at + GROUP]
    parts = three(spread[...].reshape(192, 288))
    for ci in range(SLOTS):
        chosen = fold_map(ci, shift)
        maps[ci] = chosen
        full = dot(parts[0], chosen, 1, 0) + dot(parts[1], chosen, 1, 0) + dot(parts[2], chosen, 1, 0)
        for n in range(12):
            for k in range(2):
                bias[k, pl.ds(n * SLOTS + ci, 12, stride=TOKENS), :] = full[
                    n * 16 : n * 16 + 12, k * 128 : (k + 1) * 128
                ]


def window_rows(scratch, w):
    halves = []
    for z in range(2):
        lanes = [scratch[k, pl.ds(2 * w + z, GRID, stride=8), :] for k in range(3)]
        halves.append(jnp.concatenate(lanes, axis=1))
    return jnp.concatenate(halves, axis=0).astype(BF16)


def place_rows(own, borrowed, shift, scratch, first, slots):
    for c in slots:
        for a in range(6):
            rows = own[a, c].astype(F32)
            if borrowed is not None:
                keep = c >= shift if first == 0 else c < shift
                rows = jnp.where(keep, rows, borrowed[a, c - first].astype(F32))
            for k in range(3):
                scratch[k, (a * SLOTS + c) * 8 : (a * SLOTS + c + 1) * 8, :] = rows[:, k * 128 : (k + 1) * 128]


def only(x, h):
    return jnp.concatenate([x[k * HEAD : (k + 1) * HEAD] if k == h else jnp.zeros((HEAD, x.shape[1]), x.dtype) for k in range(HEADS)], axis=0)


def forward(xs, wts, bias, proj_out, softs, atts):
    tops = {}
    for w in range(WINS):
        xw = window_rows(xs, w)
        proj = dot(wts, xw, 1, 1).astype(BF16)
        proj_out[w] = proj
        q = dot(xw, wts[0:WIDTH], 1, 1).astype(BF16)
        for h in range(HEADS):
            n = h * WINS + w
            rows = slice(n * TOKENS, (n + 1) * TOKENS)
            added = jnp.concatenate([bias[0, rows, :], bias[1, rows, 0:16]], axis=1)
            logits = dot(q, only(proj[96:192], h), 1, 0) * SCALE + added
            softs[n] = logits
            tops[n] = jnp.max(logits, axis=1, keepdims=True)
    for w in range(WINS):
        sums = []
        for h in range(HEADS):
            n = h * WINS + w
            raised = jnp.exp(softs[n] - tops[n])
            softs[n] = raised
            sums.append(1.0 / jnp.sum(raised, axis=1, keepdims=True))
        att = []
        for h in range(HEADS):
            n = h * WINS + w
            soft = softs[n] * sums[h]
            softs[n] = soft
            att.append(dot(proj_out[w, 192 + h * HEAD : 192 + (h + 1) * HEAD, :], soft.astype(BF16), 1, 1))
        atts[w] = jnp.concatenate(att, axis=0).astype(BF16)


def backward(xs, gs, wos, proj_in, softs, gsofts, atts, scores, sums, dprojs):
    rowsums, dats = {}, {}
    for w in range(WINS):
        gw = window_rows(gs, w)
        dats[w] = dot(wos, gw, 1, 1).astype(BF16)
        da = dot(gw, wos, 1, 1).astype(BF16)
        vt = proj_in[w, 192:288, :]
        for h in range(HEADS):
            n = h * WINS + w
            gsoft = dot(da, only(vt, h), 1, 0)
            gsofts[n] = gsoft
            rowsums[n] = jnp.sum(softs[n] * gsoft, axis=1, keepdims=True)
        low = dot(atts[w], gw, 1, 0)
        if w == 0:
            sums[288:384, :] = low
        else:
            sums[288:384, :] += low
    for w in range(WINS):
        dq, dk, dv = [], [], []
        for h in range(HEADS):
            n = h * WINS + w
            rows = slice(n * TOKENS, (n + 1) * TOKENS)
            own = slice(h * HEAD, (h + 1) * HEAD)
            soft = softs[n]
            gsc = soft * (gsofts[n] - rowsums[n])
            scores[0, rows, :] = gsc[:, 0:128]
            scores[1, rows, 0:16] = gsc[:, 128:144]
            gh = gsc.astype(BF16)
            dv.append(dot(dats[w][own], soft.astype(BF16), 1, 0))
            dq.append(dot(proj_in[w, 96 + h * HEAD : 96 + (h + 1) * HEAD, :], gh, 1, 1) * SCALE)
            dk.append(dot(proj_in[w, own, :], gh, 1, 0) * SCALE)
        dproj = jnp.concatenate(dq + dk + dv, axis=0).astype(BF16)
        dprojs[w] = dproj
        top = dot(dproj, window_rows(xs, w), 1, 0)
        if w == 0:
            sums[0:288, :] = top
        else:
            sums[0:288, :] += top


def fold_scores(types, scores, maps, fold, folded, folded_out):
    total = None
    for ci in range(SLOTS):
        part = jnp.concatenate(
            [scores[0, pl.ds(ci, TOKENS, stride=SLOTS), :], scores[1, pl.ds(ci, TOKENS, stride=SLOTS), :][:, 0:16]], axis=1
        )
        term = dot(part.astype(BF16), maps[ci][:, 0:TOKENS], 1, 1)
        total = term if total is None else total + term
    for k in range(3):
        wide = min(128, 288 - k * 128)
        fold[k, :, 0:wide] = total[:, k * 128 : k * 128 + wide]
    folded[...] = jnp.zeros_like(folded)
    for zi in range(2):
        for ai in range(6):
            got = [fold[k, pl.ds(zi * 6 + ai, 12, stride=12), :] for k in range(3)]
            line = jnp.concatenate(got, axis=1)
            for zj in range(2):
                at = zi * 1656 + zj * 828 + ai * GROUP
                folded[0:12, at : at + GROUP] = line[:, zj * GROUP : (zj + 1) * GROUP]
    row = lax.broadcasted_iota(jnp.int32, (16, 128), 0)
    lane = lax.broadcasted_iota(jnp.int32, (16, 128), 1)
    marks = jnp.zeros((16, 128), jnp.int32)
    for w in range(WINS):
        marks = jnp.where(row == w, types[w], marks)
    folded[:, 3200:TABLE_PAD] = jnp.where(lane >= 112, marks.astype(F32), folded[:, 3200:TABLE_PAD])
    for i in range(16):
        left, right = (folded[:, i * 256 + k * 128 : i * 256 + (k + 1) * 128] for k in range(2))
        folded_out[i, 0] = left[0:8].astype(BF16)
        folded_out[i, 1] = right[0:8].astype(BF16)
        folded_out[i, 2] = jnp.concatenate([left[8:12], right[8:12]], axis=0).astype(BF16)


def pieces_out(wflip, dprojs, piece):
    for w in range(WINS):
        back = dot(wflip[...], dprojs[w], 1, 0).astype(BF16)
        for r in range(4):
            piece[r, :, w * TOKENS : (w + 1) * TOKENS] = back[r * WIDTH : (r + 1) * WIDTH]
    for r in range(4):
        piece[r, :, 576:640] = jnp.zeros((WIDTH, 64), BF16)


def finish_kernel(shift_ref, sums, folded, own, far, attend_out, output_out, bias_out, feat_out):
    first, last = [], []
    for q in range(4):
        high, low = [], []
        for z in range(7):
            for xh in range(2):
                part = folded[xh * 4 + q, z].astype(F32)
                high += [part[0], part[1]]
                low += [part[2, 0:4], part[2, 4:8]]
        first.append(jnp.concatenate(high[0:26], axis=1))
        last.append(jnp.concatenate(low[0:26], axis=1))
    marks = jnp.concatenate([first[q][0:4, TABLE : TABLE + 1] for q in range(4)], axis=0) * 0.0625
    lane = lax.broadcasted_iota(jnp.int32, (16, 128), 1).astype(F32)
    pick = jnp.where(lane == marks, 1.0, 0.0).T[0:64].astype(BF16)
    for h in range(HEADS):
        rows = [first[q][h * WINS : (h + 1) * WINS] if h < 2 else last[q] for q in range(4)]
        bias_out[h] = dot(pick, jnp.concatenate(rows, axis=0).astype(BF16), 1, 0)[:, 0:TABLE]
    for i in range(8):
        for r in range(3):
            for k in range(3):
                part = sums[i, r * 3 + k].astype(F32)
                at, lanes = (i % 2) * 48 + r * 16, slice(k * 128, (k + 1) * 128)
                if i < 6:
                    attend_out[i // 2, at : at + 16, lanes] = part
                else:
                    output_out[at : at + 16, lanes] = part
    shift = shift_ref[0]
    for c in range(SLOTS):
        mine = jnp.where(shift <= 6, c - shift, shift - 1 - c) >= 0
        for a in range(6):
            feat_out[a, c] = jnp.where(mine, own[a, c].astype(F32), far[a, c % 6].astype(F32)).astype(BF16)[:, 0:WIDTH]


def place_features(feat, lines, out):
    for w in range(WINS):
        both = jnp.concatenate([feat[:, w * TOKENS : (w + 1) * TOKENS], jnp.zeros((32, TOKENS), F32)], axis=0).T
        for z in range(2):
            lines[pl.ds(2 * w + z, GRID, stride=8), :] = both[z * GRID : (z + 1) * GRID]
    for a in range(6):
        for c in range(SLOTS):
            at = (a * SLOTS + c) * 8
            out[a, c] = lines[at : at + 8, :].astype(BF16)


class Links:
    def __init__(self, send, recv):
        self.send, self.recv, self.used, self.sent = send, recv, 0, []

    def slot(self):
        self.used += 1
        return self.used - 1

    def copy(self, k, src, dst, to):
        return pltpu.make_async_remote_copy(
            src_ref=src,
            dst_ref=dst,
            send_sem=self.send.at[k],
            recv_sem=self.recv.at[k],
            device_id=to,
            device_id_type=pl.DeviceIdType.MESH,
        )

    def start(self, src, dst, to, k=None):
        made = self.copy(self.slot() if k is None else k, src, dst, to)
        made.start()
        if k is None:
            self.sent.append(made)
        return made

    def group(self, k, whole, to):
        made = self.copy(k, whole, whole, to)
        self.sent.append(made)
        return made

    def many(self, whole, moves):
        k = self.slot()
        for src, dst, to in moves:
            self.start(src, dst, to, k)
        return self.group(k, whole, moves[-1][2])

    def settle(self):
        for made in self.sent:
            made.wait_send()
        self.sent = []


def place():
    lon, lat, head = lax.axis_index("lon"), lax.axis_index("lat"), lax.axis_index("head")
    z, high = lon // 2, lon % 2
    low, core = lat // 2, lat % 2
    return lon, lat, head, z, high, high * 2 + low, core


def at_grid(z, x, core):
    return {"lon": z * 2 + x // 2, "lat": (x % 2) * 2 + core}


def greet(peers):
    barrier = pltpu.get_barrier_semaphore()
    for peer in peers:
        pl.semaphore_signal(barrier, inc=1, device_id=peer, device_id_type=pl.DeviceIdType.MESH)
    return len(peers)


def reduce_peers():
    lon, lat, head, z, high, x, core = place()
    xc = x * 2 + core
    peers = [{"lon": (lon + k) % 16} for k in (1, 15)]
    peers += [{"head": (head + k) % 4} for k in range(1, 4)]
    peers += [{"lon": (lon + k) % 16} for k in (8, 7, 9, 6, 10, 5, 11, 4, 12, 3, 13, 2, 14)]
    peers += [at_grid(z, ((xc + k) % 8) // 2, (xc + k) % 2) for k in range(1, 8)]
    return peers


NAMES = dict(
    xv=pltpu.VMEM((6, SLOTS, 8, MODEL), BF16),
    gv=pltpu.VMEM((6, SLOTS, 8, MODEL), BF16),
    xe=pltpu.VMEM((6, 6, 8, MODEL), BF16),
    ge=pltpu.VMEM((6, 6, 8, MODEL), BF16),
    tabv=pltpu.VMEM((3, 64, TABLE), F32),
    wtv=pltpu.VMEM((3, WIDTH, MODEL), BF16),
    wov=pltpu.VMEM((WIDTH, MODEL), BF16),
    tabw=pltpu.VMEM((16, TABLE_PAD), F32),
    spread=pltpu.VMEM((12, 16, 288), F32),
    maps=pltpu.VMEM((12, 288, 256), BF16),
    bias=pltpu.VMEM((2, 1728, 128), F32),
    xs=pltpu.VMEM((3, 576, 128), F32),
    gs=pltpu.VMEM((3, 576, 128), F32),
    wflip=pltpu.VMEM((MODEL, 288), BF16),
    projs=pltpu.VMEM((WINS, 288, TOKENS), BF16),
    gsofts=pltpu.VMEM((12, TOKENS, TOKENS), F32),
    softs=pltpu.VMEM((12, TOKENS, TOKENS), F32),
    atts=pltpu.VMEM((WINS, WIDTH, TOKENS), BF16),
    scores=pltpu.VMEM((2, 1728, 128), F32),
    dprojs=pltpu.VMEM((WINS, 288, TOKENS), BF16),
    fold=pltpu.VMEM((3, TOKENS, 128), F32),
    sums=pltpu.VMEM((MODEL, MODEL), F32),
    folded=pltpu.VMEM((16, 4096), F32),
    a0=pltpu.VMEM((4, 48, MODEL), BF16),
    ad=pltpu.VMEM((4, 48, MODEL), BF16),
    ax=pltpu.VMEM((4, 48, MODEL), BF16),
    f0=pltpu.VMEM((16, 3, 8, 128), BF16),
    p0=pltpu.VMEM((4, WIDTH, 640), BF16),
    a1=pltpu.VMEM((3, 48, MODEL), BF16),
    f1=pltpu.VMEM((15, 3, 8, 128), BF16),
    p1=pltpu.VMEM((3, WIDTH, 640), BF16),
    a2s=pltpu.VMEM((8, 2, 16, 128), BF16),
    a2=pltpu.VMEM((7, 2, 16, 128), BF16),
    a3=pltpu.VMEM((8, 16, 128), BF16),
    lines=pltpu.VMEM((576, 128), F32),
    f3=pltpu.VMEM((8, 3, 8, 128), BF16),
    send=pltpu.SemaphoreType.DMA((21,)),
    recv=pltpu.SemaphoreType.DMA((21,)),
    load=pltpu.SemaphoreType.DMA((7,)),
    types=pltpu.SMEM((1, 4), jnp.int32),
    shift=pltpu.SMEM((1,), jnp.int32),
)


def main_kernel(first, types_ref, shift_ref, x, g, table, wt, wo, a_out, f_out, own_out, west_out, *scratch):
    v = dict(zip(NAMES, scratch, strict=True))
    lon, lat, head, z, high, xpos, core = place()
    xc = xpos * 2 + core
    step = 1 if first == 0 else 15
    net = Links(v["send"], v["recv"])
    loads = []
    given = ((g, "gv"), (x, "xv"), (types_ref, "types"), (shift_ref, "shift"), (table, "tabv"), (wt, "wtv"), (wo, "wov"))
    for src, dst in given:
        loads.append(pltpu.make_async_copy(src, v[dst], v["load"].at[len(loads)]))
    loads[0].start()
    loads[1].start()
    met = greet(reduce_peers())
    for made in loads[2:]:
        made.start()
    with jax.named_scope("enter"):
        for made in loads[0:2]:
            made.wait()
        pl.semaphore_wait(pltpu.get_barrier_semaphore(), met)

    giver = {"lon": (lon + 16 - step) % 16}
    rows, cols = pl.ds((head // 2) * 3, 3), (head % 2) * 3
    quarter = v["ge"].at[rows, pl.ds(cols, 3)]
    halo = [net.start(v["gv"].at[rows, pl.ds(first + cols, 3)], quarter, giver)]
    halo.append(net.start(v["xv"].at[:, pl.ds(first, 6)], v["xe"], giver))
    with jax.named_scope("bias"):
        for made in loads[2:5]:
            made.wait()
        types = [v["types"][0, w] for w in range(WINS)]
        shift = v["shift"][0]
        expand_bias(types, shift, v["tabv"], v["tabw"], v["spread"], v["maps"], v["bias"])
    mixed = [c for c in range(first, first + 6)]
    still = [c for c in range(SLOTS) if c not in mixed]
    place_rows(v["xv"], None, shift, v["xs"], first, still)
    place_rows(v["gv"], None, shift, v["gs"], first, still)
    with jax.named_scope("still"):
        loads[5].wait()
        loads[6].wait()
        wts = v["wtv"][...].reshape(3 * WIDTH, MODEL)
        wos = v["wov"][...]
        v["wflip"][...] = wts.astype(F32).T.astype(BF16)

    with jax.named_scope("halo_q"):
        halo[0].wait_recv()
    handed = [net.start(quarter, quarter, {"head": (head + j) % 4}) for j in range(1, 4)]
    with jax.named_scope("halo_x"):
        halo[1].wait_recv()
    with jax.named_scope("forward"):
        place_rows(v["xv"], v["xe"], shift, v["xs"], first, mixed)
        forward(v["xs"], wts, v["bias"], v["projs"], v["softs"], v["atts"])
    with jax.named_scope("halo_g"):
        for made in handed:
            made.wait_recv()
    with jax.named_scope("backward"):
        place_rows(v["gv"], v["ge"], shift, v["gs"], first, mixed)
        backward(v["xs"], v["gs"], wos, v["projs"], v["softs"], v["gsofts"], v["atts"], v["scores"], v["sums"], v["dprojs"])

    def zs(k):
        return {"lon": ((z + k) % 8) * 2 + high}

    a0, f0, p0 = v["a0"], v["f0"], v["p0"]
    a1, f1, p1 = v["a1"], v["f1"], v["p1"]
    ad, ax, a2s, a2, a3, f3 = (v[n] for n in ("ad", "ax", "a2s", "a2", "a3", "f3"))
    partner = at_grid(z, xpos, 1 - core)

    def chunk(i, side):
        return v["sums"][pl.ds(pl.multiple_of((2 * i + side) * 48, 16), 48), :]

    for i in range(4):
        a0[i] = chunk(i, 1 - core).astype(BF16)
    twin = net.start(a0, ad, partner)
    with jax.named_scope("fold"):
        fold_scores(types, v["scores"], v["maps"], v["fold"], v["folded"], f0)
    with jax.named_scope("sum_d"):
        twin.wait_recv()
        for i in range(4):
            ax[i] = (chunk(i, core) + ad[i].astype(F32)).astype(BF16)
    one = net.many(a1, [(ax.at[(xpos + k) % 4], a1.at[k - 1], at_grid(z, (xpos + k) % 4, core)) for k in range(1, 4)])
    two = net.many(f1, [(f0.at[(lon + k) % 16], f1.at[k - 1], {"lon": (lon + k) % 16}) for k in range(1, 16)])
    with jax.named_scope("pieces"):
        pieces_out(v["wflip"], v["dprojs"], p0)
    pieces = net.many(p1, [(p0.at[(head + k) % 4], p1.at[k - 1], {"head": (head + k) % 4}) for k in range(1, 4)])

    with jax.named_scope("sum_a"):
        total = chunk(xpos, core) + ad[xpos].astype(F32)
        one.wait_recv()
        for k in range(3):
            total = total + a1[k].astype(F32)
        tiles = [total[r * 16 : (r + 1) * 16, k * 128 : (k + 1) * 128].astype(BF16) for r in range(3) for k in range(3)]
        for k in range(8):
            a2s[k, 0] = tiles[k]
            a2s[k, 1] = tiles[8]
    three_ = net.many(a2, [(a2s.at[(z + k) % 8], a2.at[k - 1], zs(k)) for k in range(1, 8)])

    with jax.named_scope("sum_f"):
        lines = f0[lon].astype(F32)
        two.wait_recv()
        for k in range(15):
            lines = lines + f1[k].astype(F32)
        f3[z] = lines.astype(BF16)
    part = f3.at[pl.ds(0, 7)]
    five = net.many(part, [(f3.at[z], f3.at[z], zs(k)) for k in range(1, 8)])

    with jax.named_scope("sum_z"):
        block = a2s[z].astype(F32)
        three_.wait_recv()
        for k in range(7):
            block = block + a2[k].astype(F32)
        a3[z] = block[0].astype(BF16)
    six = net.many(a3.at[pl.ds(0, 7)], [(a3.at[z], a3.at[z], zs(k)) for k in range(1, 8)])
    a_out[xc, 8] = block[1].astype(BF16)

    with jax.named_scope("sum_p"):
        feat = p0[head].astype(F32)
        pieces.wait_recv()
        for k in range(3):
            feat = feat + p1[k].astype(F32)
        place_features(feat, v["lines"], own_out)
    net.settle()
    back = net.start(own_out.at[:, pl.ds(first, 6)], west_out, {"lon": (lon + step) % 16})

    with jax.named_scope("all_f"):
        five.wait_recv()
    mine = f_out.at[xc, pl.ds(0, 7)]
    arrive_f = [net.start(part, mine, at_grid(z, (xpos + k) % 4, core)) for k in range(1, 4)]
    cross_f, cross_a = net.slot(), net.slot()
    net.start(part, mine, partner, cross_f)
    f_out[xc] = f3[...]
    with jax.named_scope("all_a"):
        six.wait_recv()
    a_out[xc, 0:8] = a3[...]
    arrive = [net.start(a_out.at[xc], a_out.at[xc], at_grid(z, (xpos + k) % 4, core)) for k in range(1, 4)]
    net.start(a_out.at[xc], a_out.at[xc], partner, cross_a)
    with jax.named_scope("forward_x"):
        for k in range(1, 4):
            there = ((xpos + 4 - k) % 4) * 2 + core
            arrive_f[k - 1].wait_recv()
            ref = f_out.at[there, pl.ds(0, 7)]
            net.start(ref, ref, partner, cross_f)
        for k in range(1, 4):
            there = ((xpos + 4 - k) % 4) * 2 + core
            arrive[k - 1].wait_recv()
            net.start(a_out.at[there], a_out.at[there], partner, cross_a)
    cross = [net.group(cross_f, f_out.at[pl.ds(0, 4), pl.ds(0, 7)], partner), net.group(cross_a, a_out.at[pl.ds(0, 4)], partner)]
    with jax.named_scope("last"):
        back.wait_recv()
        for made in cross:
            made.wait_recv()
    net.settle()


def per_device(features, attend_weight, output_weight, bias_table, bias_type, window_shift, grad_out):
    x = features.transpose(1, 2, 0, 3)
    g = grad_out.transpose(1, 2, 0, 3)
    wt = attend_weight.transpose(0, 2, 1)
    table = bias_table.transpose(1, 0, 2)

    def run(first):
        return pl.pallas_call(
            functools.partial(main_kernel, first),
            out_shape=(
                jax.ShapeDtypeStruct((8, 9, 16, 128), BF16),
                jax.ShapeDtypeStruct((8, 8, 3, 8, 128), BF16),
                jax.ShapeDtypeStruct((6, SLOTS, 8, 128), BF16),
                jax.ShapeDtypeStruct((6, 6, 8, 128), BF16),
            ),
            in_specs=[ANY] * 7,
            out_specs=(VMEM,) * 4,
            scratch_shapes=list(NAMES.values()),
            compiler_params=pltpu.CompilerParams(
                vmem_limit_bytes=56 << 20, collective_id=1 if first == 0 else 2, has_side_effects=True
            ),
            name="block_east" if first == 0 else "block_west",
        )

    args = (bias_type.T, window_shift, x, g, table, wt, output_weight)
    sums, folded, own, borrowed = lax.cond(window_shift[0] <= 6, run(0), run(6), *args)
    return finish(window_shift, sums, folded, own, borrowed)


def finish(window_shift, sums, folded, own, borrowed):
    attend_grad, output_grad, bias_grad, feat = pl.pallas_call(
        finish_kernel,
        out_shape=(
            jax.ShapeDtypeStruct((3, WIDTH, MODEL), F32),
            jax.ShapeDtypeStruct((WIDTH, MODEL), F32),
            jax.ShapeDtypeStruct((3, 64, TABLE), F32),
            jax.ShapeDtypeStruct((6, SLOTS, 8, WIDTH), BF16),
        ),
        in_specs=[SMEM, VMEM, VMEM, VMEM, VMEM],
        out_specs=(VMEM,) * 4,
        compiler_params=pltpu.CompilerParams(vmem_limit_bytes=40 << 20),
        name="finish",
    )(window_shift, sums, folded, own, borrowed)
    return (
        feat.transpose(2, 0, 1, 3),
        attend_grad.transpose(0, 2, 1),
        output_grad,
        bias_grad.transpose(1, 0, 2),
    )


def solution(mesh):
    placed = (
        P(None, "lat", "lon", None),
        P(None, None, "head"),
        P("head", None),
        P(None, "head", None),
        P(None, "lat"),
        P(),
        P(None, "lat", "lon", None),
    )
    return jax.shard_map(
        per_device,
        mesh=mesh,
        in_specs=placed,
        out_specs=(
            P(None, "lat", "lon", "head"),
            P(None, None, "head"),
            P("head", None),
            P(None, "head", None),
        ),
        check_vma=False,
    )
```

```python
import functools

import jax
import jax.numpy as jnp
from jax import lax
from jax.experimental import pallas as pl
from jax.experimental.pallas import tpu as pltpu
from jax.sharding import PartitionSpec as P

F32 = jnp.float32
BF16 = jnp.bfloat16
HEADS = 3
WINS = 4
WIDTH = 96
HEAD = 32
SLOTS = 12
GRID = 72
TOKENS = 144
MODEL = 384
SPAN = 23
TABLE = 3312
TABLE_PAD = 3328
GROUP = 138
SCALE = HEAD ** (-0.5)
VMEM = pl.BlockSpec(memory_space=pltpu.VMEM)
SMEM = pl.BlockSpec(memory_space=pltpu.SMEM)
ANY = pl.BlockSpec(memory_space=pl.ANY)


def dot(a, b, da, db):
    return lax.dot_general(a, b, (((da,), (db,)), ((), ())), preferred_element_type=F32)


def three(x):
    hi = x.astype(BF16)
    rest = x - hi.astype(F32)
    mid = rest.astype(BF16)
    return hi, mid, (rest - mid.astype(F32)).astype(BF16)


def fold_map(ci, shift):
    rows = lax.broadcasted_iota(jnp.int32, (288, 256), 0)
    lane = lax.broadcasted_iota(jnp.int32, (1, 256), 1)
    block = lane // SLOTS
    cj = lane - block * SLOTS
    wrap = jnp.where(ci < shift, 12, 0) - jnp.where(cj < shift, 12, 0)
    target = block * SPAN + (11 + ci) - cj + wrap
    target = jnp.where(lane < TOKENS, target, -1)
    return jnp.where(rows == target, 1.0, 0.0).astype(BF16)


def expand_bias(types, shift, table, tabw, spread, maps, bias):
    for h in range(HEADS):
        for w in range(WINS):
            n = h * WINS + w
            tabw[n : n + 1, 0:TABLE] = table[h, pl.ds(types[w], 1), :]
    spread[...] = jnp.zeros_like(spread)
    for zi in range(2):
        for ai in range(6):
            for zj in range(2):
                at = zi * 1656 + zj * 828 + ai * GROUP
                spread[zi * 6 + ai, 0:12, zj * GROUP : (zj + 1) * GROUP] = tabw[0:12, at : at + GROUP]
    parts = three(spread[...].reshape(192, 288))
    for ci in range(SLOTS):
        chosen = fold_map(ci, shift)
        maps[ci] = chosen
        full = dot(parts[0], chosen, 1, 0) + dot(parts[1], chosen, 1, 0) + dot(parts[2], chosen, 1, 0)
        for n in range(12):
            for k in range(2):
                bias[k, pl.ds(n * SLOTS + ci, 12, stride=TOKENS), :] = full[
                    n * 16 : n * 16 + 12, k * 128 : (k + 1) * 128
                ]


def window_rows(scratch, w):
    halves = []
    for z in range(2):
        lanes = [scratch[k, pl.ds(2 * w + z, GRID, stride=8), :] for k in range(3)]
        halves.append(jnp.concatenate(lanes, axis=1))
    return jnp.concatenate(halves, axis=0).astype(BF16)


def place_rows(own, borrowed, shift, scratch, first, slots):
    for c in slots:
        for a in range(6):
            rows = own[a, c].astype(F32)
            if borrowed is not None:
                keep = c >= shift if first == 0 else c < shift
                rows = jnp.where(keep, rows, borrowed[a, c - first].astype(F32))
            for k in range(3):
                scratch[k, (a * SLOTS + c) * 8 : (a * SLOTS + c + 1) * 8, :] = rows[:, k * 128 : (k + 1) * 128]


def only(x, h):
    return jnp.concatenate([x[k * HEAD : (k + 1) * HEAD] if k == h else jnp.zeros((HEAD, x.shape[1]), x.dtype) for k in range(HEADS)], axis=0)


def forward(xs, wts, bias, proj_out, softs, atts):
    tops = {}
    for w in range(WINS):
        xw = window_rows(xs, w)
        proj = dot(wts, xw, 1, 1).astype(BF16)
        proj_out[w] = proj
        q = dot(xw, wts[0:WIDTH], 1, 1).astype(BF16)
        for h in range(HEADS):
            n = h * WINS + w
            rows = slice(n * TOKENS, (n + 1) * TOKENS)
            added = jnp.concatenate([bias[0, rows, :], bias[1, rows, 0:16]], axis=1)
            logits = dot(q, only(proj[96:192], h), 1, 0) * SCALE + added
            softs[n] = logits
            tops[n] = jnp.max(logits, axis=1, keepdims=True)
    for w in range(WINS):
        sums = []
        for h in range(HEADS):
            n = h * WINS + w
            raised = jnp.exp(softs[n] - tops[n])
            softs[n] = raised
            sums.append(1.0 / jnp.sum(raised, axis=1, keepdims=True))
        att = []
        for h in range(HEADS):
            n = h * WINS + w
            soft = softs[n] * sums[h]
            softs[n] = soft
            att.append(dot(proj_out[w, 192 + h * HEAD : 192 + (h + 1) * HEAD, :], soft.astype(BF16), 1, 1))
        atts[w] = jnp.concatenate(att, axis=0).astype(BF16)


def backward(xs, gs, wos, proj_in, softs, gsofts, atts, scores, sums, dprojs):
    rowsums, dats = {}, {}
    for w in range(WINS):
        gw = window_rows(gs, w)
        dats[w] = dot(wos, gw, 1, 1).astype(BF16)
        da = dot(gw, wos, 1, 1).astype(BF16)
        vt = proj_in[w, 192:288, :]
        for h in range(HEADS):
            n = h * WINS + w
            gsoft = dot(da, only(vt, h), 1, 0)
            gsofts[n] = gsoft
            rowsums[n] = jnp.sum(softs[n] * gsoft, axis=1, keepdims=True)
        low = dot(atts[w], gw, 1, 0)
        if w == 0:
            sums[288:384, :] = low
        else:
            sums[288:384, :] += low
    for w in range(WINS):
        dq, dk, dv = [], [], []
        for h in range(HEADS):
            n = h * WINS + w
            rows = slice(n * TOKENS, (n + 1) * TOKENS)
            own = slice(h * HEAD, (h + 1) * HEAD)
            soft = softs[n]
            gsc = soft * (gsofts[n] - rowsums[n])
            scores[0, rows, :] = gsc[:, 0:128]
            scores[1, rows, 0:16] = gsc[:, 128:144]
            gh = gsc.astype(BF16)
            dv.append(dot(dats[w][own], soft.astype(BF16), 1, 0))
            dq.append(dot(proj_in[w, 96 + h * HEAD : 96 + (h + 1) * HEAD, :], gh, 1, 1) * SCALE)
            dk.append(dot(proj_in[w, own, :], gh, 1, 0) * SCALE)
        dproj = jnp.concatenate(dq + dk + dv, axis=0).astype(BF16)
        dprojs[w] = dproj
        top = dot(dproj, window_rows(xs, w), 1, 0)
        if w == 0:
            sums[0:288, :] = top
        else:
            sums[0:288, :] += top


def fold_scores(types, scores, maps, fold, folded, folded_out):
    total = None
    for ci in range(SLOTS):
        part = jnp.concatenate(
            [scores[0, pl.ds(ci, TOKENS, stride=SLOTS), :], scores[1, pl.ds(ci, TOKENS, stride=SLOTS), :][:, 0:16]], axis=1
        )
        term = dot(part.astype(BF16), maps[ci][:, 0:TOKENS], 1, 1)
        total = term if total is None else total + term
    for k in range(3):
        wide = min(128, 288 - k * 128)
        fold[k, :, 0:wide] = total[:, k * 128 : k * 128 + wide]
    folded[...] = jnp.zeros_like(folded)
    for zi in range(2):
        for ai in range(6):
            got = [fold[k, pl.ds(zi * 6 + ai, 12, stride=12), :] for k in range(3)]
            line = jnp.concatenate(got, axis=1)
            for zj in range(2):
                at = zi * 1656 + zj * 828 + ai * GROUP
                folded[0:12, at : at + GROUP] = line[:, zj * GROUP : (zj + 1) * GROUP]
    row = lax.broadcasted_iota(jnp.int32, (16, 128), 0)
    lane = lax.broadcasted_iota(jnp.int32, (16, 128), 1)
    marks = jnp.zeros((16, 128), jnp.int32)
    for w in range(WINS):
        marks = jnp.where(row == w, types[w], marks)
    folded[:, 3200:TABLE_PAD] = jnp.where(lane >= 112, marks.astype(F32), folded[:, 3200:TABLE_PAD])
    for i in range(16):
        left, right = (folded[:, i * 256 + k * 128 : i * 256 + (k + 1) * 128] for k in range(2))
        folded_out[i, 0] = left[0:8].astype(BF16)
        folded_out[i, 1] = right[0:8].astype(BF16)
        folded_out[i, 2] = jnp.concatenate([left[8:12], right[8:12]], axis=0).astype(BF16)


def pieces_out(wflip, dprojs, piece):
    for w in range(WINS):
        back = dot(wflip[...], dprojs[w], 1, 0).astype(BF16)
        for r in range(4):
            piece[r, :, w * TOKENS : (w + 1) * TOKENS] = back[r * WIDTH : (r + 1) * WIDTH]
    for r in range(4):
        piece[r, :, 576:640] = jnp.zeros((WIDTH, 64), BF16)


def finish_kernel(shift_ref, sums, folded, own, far, attend_out, output_out, bias_out, feat_out):
    first, last = [], []
    for q in range(4):
        high, low = [], []
        for z in range(7):
            for xh in range(2):
                part = folded[xh * 4 + q, z].astype(F32)
                high += [part[0], part[1]]
                low += [part[2, 0:4], part[2, 4:8]]
        first.append(jnp.concatenate(high[0:26], axis=1))
        last.append(jnp.concatenate(low[0:26], axis=1))
    marks = jnp.concatenate([first[q][0:4, TABLE : TABLE + 1] for q in range(4)], axis=0) * 0.0625
    lane = lax.broadcasted_iota(jnp.int32, (16, 128), 1).astype(F32)
    pick = jnp.where(lane == marks, 1.0, 0.0).T[0:64].astype(BF16)
    for h in range(HEADS):
        rows = [first[q][h * WINS : (h + 1) * WINS] if h < 2 else last[q] for q in range(4)]
        bias_out[h] = dot(pick, jnp.concatenate(rows, axis=0).astype(BF16), 1, 0)[:, 0:TABLE]
    for i in range(8):
        for r in range(3):
            for k in range(3):
                part = sums[i, r * 3 + k].astype(F32)
                at, lanes = (i % 2) * 48 + r * 16, slice(k * 128, (k + 1) * 128)
                if i < 6:
                    attend_out[i // 2, at : at + 16, lanes] = part
                else:
                    output_out[at : at + 16, lanes] = part
    shift = shift_ref[0]
    for c in range(SLOTS):
        mine = jnp.where(shift <= 6, c - shift, shift - 1 - c) >= 0
        for a in range(6):
            feat_out[a, c] = jnp.where(mine, own[a, c].astype(F32), far[a, c % 6].astype(F32)).astype(BF16)[:, 0:WIDTH]


def place_features(feat, lines, out):
    for w in range(WINS):
        both = jnp.concatenate([feat[:, w * TOKENS : (w + 1) * TOKENS], jnp.zeros((32, TOKENS), F32)], axis=0).T
        for z in range(2):
            lines[pl.ds(2 * w + z, GRID, stride=8), :] = both[z * GRID : (z + 1) * GRID]
    for a in range(6):
        for c in range(SLOTS):
            at = (a * SLOTS + c) * 8
            out[a, c] = lines[at : at + 8, :].astype(BF16)


class Links:
    def __init__(self, send, recv):
        self.send, self.recv, self.used, self.sent = send, recv, 0, []

    def slot(self):
        self.used += 1
        return self.used - 1

    def copy(self, k, src, dst, to):
        return pltpu.make_async_remote_copy(
            src_ref=src,
            dst_ref=dst,
            send_sem=self.send.at[k],
            recv_sem=self.recv.at[k],
            device_id=to,
            device_id_type=pl.DeviceIdType.MESH,
        )

    def start(self, src, dst, to, k=None):
        made = self.copy(self.slot() if k is None else k, src, dst, to)
        made.start()
        if k is None:
            self.sent.append(made)
        return made

    def group(self, k, whole, to):
        made = self.copy(k, whole, whole, to)
        self.sent.append(made)
        return made

    def many(self, whole, moves):
        k = self.slot()
        for src, dst, to in moves:
            self.start(src, dst, to, k)
        return self.group(k, whole, moves[-1][2])

    def settle(self):
        for made in self.sent:
            made.wait_send()
        self.sent = []


def place():
    lon, lat, head = lax.axis_index("lon"), lax.axis_index("lat"), lax.axis_index("head")
    z, high = lon // 2, lon % 2
    low, core = lat // 2, lat % 2
    return lon, lat, head, z, high, high * 2 + low, core


def at_grid(z, x, core):
    return {"lon": z * 2 + x // 2, "lat": (x % 2) * 2 + core}


def greet(peers):
    barrier = pltpu.get_barrier_semaphore()
    for peer in peers:
        pl.semaphore_signal(barrier, inc=1, device_id=peer, device_id_type=pl.DeviceIdType.MESH)
    return len(peers)


def reduce_peers():
    lon, lat, head, z, high, x, core = place()
    xc = x * 2 + core
    peers = [{"lon": (lon + k) % 16} for k in range(1, 16)]
    peers += [at_grid(z, ((xc + k) % 8) // 2, (xc + k) % 2) for k in range(1, 8)]
    peers += [{"head": (head + k) % 4} for k in range(1, 4)]
    return peers


NAMES = dict(
    xv=pltpu.VMEM((6, SLOTS, 8, MODEL), BF16),
    gv=pltpu.VMEM((6, SLOTS, 8, MODEL), BF16),
    xe=pltpu.VMEM((6, 6, 8, MODEL), BF16),
    ge=pltpu.VMEM((6, 6, 8, MODEL), BF16),
    tabv=pltpu.VMEM((3, 64, TABLE), F32),
    wtv=pltpu.VMEM((3, WIDTH, MODEL), BF16),
    wov=pltpu.VMEM((WIDTH, MODEL), BF16),
    tabw=pltpu.VMEM((16, TABLE_PAD), F32),
    spread=pltpu.VMEM((12, 16, 288), F32),
    maps=pltpu.VMEM((12, 288, 256), BF16),
    bias=pltpu.VMEM((2, 1728, 128), F32),
    xs=pltpu.VMEM((3, 576, 128), F32),
    gs=pltpu.VMEM((3, 576, 128), F32),
    wflip=pltpu.VMEM((MODEL, 288), BF16),
    projs=pltpu.VMEM((WINS, 288, TOKENS), BF16),
    gsofts=pltpu.VMEM((12, TOKENS, TOKENS), F32),
    softs=pltpu.VMEM((12, TOKENS, TOKENS), F32),
    atts=pltpu.VMEM((WINS, WIDTH, TOKENS), BF16),
    scores=pltpu.VMEM((2, 1728, 128), F32),
    dprojs=pltpu.VMEM((WINS, 288, TOKENS), BF16),
    fold=pltpu.VMEM((3, TOKENS, 128), F32),
    sums=pltpu.VMEM((MODEL, MODEL), F32),
    folded=pltpu.VMEM((16, 4096), F32),
    a0=pltpu.VMEM((4, 48, MODEL), BF16),
    ad=pltpu.VMEM((4, 48, MODEL), BF16),
    ax=pltpu.VMEM((4, 48, MODEL), BF16),
    f0=pltpu.VMEM((16, 3, 8, 128), BF16),
    p0=pltpu.VMEM((4, WIDTH, 640), BF16),
    a1=pltpu.VMEM((3, 48, MODEL), BF16),
    f1=pltpu.VMEM((15, 3, 8, 128), BF16),
    p1=pltpu.VMEM((3, WIDTH, 640), BF16),
    a2s=pltpu.VMEM((8, 2, 16, 128), BF16),
    a2=pltpu.VMEM((7, 2, 16, 128), BF16),
    a3=pltpu.VMEM((8, 16, 128), BF16),
    lines=pltpu.VMEM((576, 128), F32),
    f3=pltpu.VMEM((8, 3, 8, 128), BF16),
    send=pltpu.SemaphoreType.DMA((21,)),
    recv=pltpu.SemaphoreType.DMA((21,)),
    load=pltpu.SemaphoreType.DMA((7,)),
    types=pltpu.SMEM((1, 4), jnp.int32),
    shift=pltpu.SMEM((1,), jnp.int32),
)


def main_kernel(first, types_ref, shift_ref, x, g, table, wt, wo, a_out, f_out, own_out, west_out, *scratch):
    v = dict(zip(NAMES, scratch, strict=True))
    lon, lat, head, z, high, xpos, core = place()
    xc = xpos * 2 + core
    step = 1 if first == 0 else 15
    net = Links(v["send"], v["recv"])
    met = greet(reduce_peers())
    loads = []
    given = ((g, "gv"), (x, "xv"), (types_ref, "types"), (shift_ref, "shift"), (table, "tabv"), (wt, "wtv"), (wo, "wov"))
    for src, dst in given:
        made = pltpu.make_async_copy(src, v[dst], v["load"].at[len(loads)])
        made.start()
        loads.append(made)
    with jax.named_scope("enter"):
        for made in loads[0:2]:
            made.wait()
        pl.semaphore_wait(pltpu.get_barrier_semaphore(), met)

    giver = {"lon": (lon + 16 - step) % 16}
    rows, cols = pl.ds((head // 2) * 3, 3), (head % 2) * 3
    quarter = v["ge"].at[rows, pl.ds(cols, 3)]
    halo = [net.start(v["gv"].at[rows, pl.ds(first + cols, 3)], quarter, giver)]
    skip = 0 if first == 0 else 1
    near, spot = pl.ds(first + skip, 6 - skip), pl.ds(skip, 6 - skip)
    halo.append(net.start(v["xv"].at[:, near], v["xe"].at[:, spot], giver))
    with jax.named_scope("bias"):
        for made in loads[2:5]:
            made.wait()
        types = [v["types"][0, w] for w in range(WINS)]
        shift = v["shift"][0]
        expand_bias(types, shift, v["tabv"], v["tabw"], v["spread"], v["maps"], v["bias"])
    mixed = [c for c in range(first, first + 6)]
    still = [c for c in range(SLOTS) if c not in mixed]
    place_rows(v["xv"], None, shift, v["xs"], first, still + mixed[:skip])
    place_rows(v["gv"], None, shift, v["gs"], first, still)
    with jax.named_scope("still"):
        loads[5].wait()
        loads[6].wait()
        wts = v["wtv"][...].reshape(3 * WIDTH, MODEL)
        wos = v["wov"][...]
        v["wflip"][...] = wts.astype(F32).T.astype(BF16)

    with jax.named_scope("halo_q"):
        halo[0].wait_recv()
    handed = [net.start(quarter, quarter, {"head": (head + j) % 4}) for j in range(1, 4)]
    with jax.named_scope("halo_x"):
        halo[1].wait_recv()
    with jax.named_scope("forward"):
        place_rows(v["xv"], v["xe"], shift, v["xs"], first, mixed[skip:])
        forward(v["xs"], wts, v["bias"], v["projs"], v["softs"], v["atts"])
    with jax.named_scope("halo_g"):
        for made in handed:
            made.wait_recv()
    with jax.named_scope("backward"):
        place_rows(v["gv"], v["ge"], shift, v["gs"], first, mixed)
        backward(v["xs"], v["gs"], wos, v["projs"], v["softs"], v["gsofts"], v["atts"], v["scores"], v["sums"], v["dprojs"])

    def zs(k):
        return {"lon": ((z + k) % 8) * 2 + high}

    a0, f0, p0 = v["a0"], v["f0"], v["p0"]
    a1, f1, p1 = v["a1"], v["f1"], v["p1"]
    ad, ax, a2s, a2, a3, f3 = (v[n] for n in ("ad", "ax", "a2s", "a2", "a3", "f3"))
    partner = at_grid(z, xpos, 1 - core)

    def chunk(i, side):
        return v["sums"][pl.ds(pl.multiple_of((2 * i + side) * 48, 16), 48), :]

    for i in range(4):
        a0[i] = chunk(i, 1 - core).astype(BF16)
    twin = net.start(a0, ad, partner)
    with jax.named_scope("fold"):
        fold_scores(types, v["scores"], v["maps"], v["fold"], v["folded"], f0)
    with jax.named_scope("sum_d"):
        twin.wait_recv()
        for i in range(4):
            ax[i] = (chunk(i, core) + ad[i].astype(F32)).astype(BF16)
    one = net.many(a1, [(ax.at[(xpos + k) % 4], a1.at[k - 1], at_grid(z, (xpos + k) % 4, core)) for k in range(1, 4)])
    two = net.many(f1, [(f0.at[(lon + k) % 16], f1.at[k - 1], {"lon": (lon + k) % 16}) for k in range(1, 16)])
    with jax.named_scope("pieces"):
        pieces_out(v["wflip"], v["dprojs"], p0)
    pieces = net.many(p1, [(p0.at[(head + k) % 4], p1.at[k - 1], {"head": (head + k) % 4}) for k in range(1, 4)])

    with jax.named_scope("sum_a"):
        total = chunk(xpos, core) + ad[xpos].astype(F32)
        one.wait_recv()
        for k in range(3):
            total = total + a1[k].astype(F32)
        tiles = [total[r * 16 : (r + 1) * 16, k * 128 : (k + 1) * 128].astype(BF16) for r in range(3) for k in range(3)]
        for k in range(8):
            a2s[k, 0] = tiles[k]
            a2s[k, 1] = tiles[8]
    three_ = net.many(a2, [(a2s.at[(z + k) % 8], a2.at[k - 1], zs(k)) for k in range(1, 8)])

    with jax.named_scope("sum_f"):
        lines = f0[lon].astype(F32)
        two.wait_recv()
        for k in range(15):
            lines = lines + f1[k].astype(F32)
        f3[z] = lines.astype(BF16)
    part = f3.at[pl.ds(0, 7)]
    five = net.many(part, [(f3.at[z], f3.at[z], zs(k)) for k in range(1, 8)])

    with jax.named_scope("sum_z"):
        block = a2s[z].astype(F32)
        three_.wait_recv()
        for k in range(7):
            block = block + a2[k].astype(F32)
        a3[z] = block[0].astype(BF16)
    six = net.many(a3.at[pl.ds(0, 7)], [(a3.at[z], a3.at[z], zs(k)) for k in range(1, 8)])
    a_out[xc, 8] = block[1].astype(BF16)

    with jax.named_scope("sum_p"):
        feat = p0[head].astype(F32)
        pieces.wait_recv()
        for k in range(3):
            feat = feat + p1[k].astype(F32)
        place_features(feat, v["lines"], own_out)
    net.settle()
    back = net.start(own_out.at[:, near], west_out.at[:, spot], {"lon": (lon + step) % 16})

    with jax.named_scope("all_f"):
        five.wait_recv()
    mine = f_out.at[xc, pl.ds(0, 7)]
    arrive_f = [net.start(part, mine, at_grid(z, (xpos + k) % 4, core)) for k in range(1, 4)]
    cross_f, cross_a = net.slot(), net.slot()
    net.start(part, mine, partner, cross_f)
    f_out[xc] = f3[...]
    with jax.named_scope("all_a"):
        six.wait_recv()
    a_out[xc, 0:8] = a3[...]
    arrive = [net.start(a_out.at[xc], a_out.at[xc], at_grid(z, (xpos + k) % 4, core)) for k in range(1, 4)]
    net.start(a_out.at[xc], a_out.at[xc], partner, cross_a)
    with jax.named_scope("forward_x"):
        for k in range(1, 4):
            there = ((xpos + 4 - k) % 4) * 2 + core
            arrive_f[k - 1].wait_recv()
            ref = f_out.at[there, pl.ds(0, 7)]
            net.start(ref, ref, partner, cross_f)
        for k in range(1, 4):
            there = ((xpos + 4 - k) % 4) * 2 + core
            arrive[k - 1].wait_recv()
            net.start(a_out.at[there], a_out.at[there], partner, cross_a)
    cross = [net.group(cross_f, f_out.at[pl.ds(0, 4), pl.ds(0, 7)], partner), net.group(cross_a, a_out.at[pl.ds(0, 4)], partner)]
    net.settle()
    with jax.named_scope("last"):
        back.wait_recv()
        for made in cross:
            made.wait_recv()


def per_device(features, attend_weight, output_weight, bias_table, bias_type, window_shift, grad_out):
    x = features.transpose(1, 2, 0, 3)
    g = grad_out.transpose(1, 2, 0, 3)
    wt = attend_weight.transpose(0, 2, 1)
    table = bias_table.transpose(1, 0, 2)

    def run(first):
        return pl.pallas_call(
            functools.partial(main_kernel, first),
            out_shape=(
                jax.ShapeDtypeStruct((8, 9, 16, 128), BF16),
                jax.ShapeDtypeStruct((8, 8, 3, 8, 128), BF16),
                jax.ShapeDtypeStruct((6, SLOTS, 8, 128), BF16),
                jax.ShapeDtypeStruct((6, 6, 8, 128), BF16),
            ),
            in_specs=[ANY] * 7,
            out_specs=(VMEM,) * 4,
            scratch_shapes=list(NAMES.values()),
            compiler_params=pltpu.CompilerParams(
                vmem_limit_bytes=56 << 20, collective_id=1 if first == 0 else 2, has_side_effects=True
            ),
            name="block_east" if first == 0 else "block_west",
        )

    args = (bias_type.T, window_shift, x, g, table, wt, output_weight)
    sums, folded, own, borrowed = lax.cond(window_shift[0] <= 6, run(0), run(6), *args)
    return finish(window_shift, sums, folded, own, borrowed)


def finish(window_shift, sums, folded, own, borrowed):
    attend_grad, output_grad, bias_grad, feat = pl.pallas_call(
        finish_kernel,
        out_shape=(
            jax.ShapeDtypeStruct((3, WIDTH, MODEL), F32),
            jax.ShapeDtypeStruct((WIDTH, MODEL), F32),
            jax.ShapeDtypeStruct((3, 64, TABLE), F32),
            jax.ShapeDtypeStruct((6, SLOTS, 8, WIDTH), BF16),
        ),
        in_specs=[SMEM, VMEM, VMEM, VMEM, VMEM],
        out_specs=(VMEM,) * 4,
        compiler_params=pltpu.CompilerParams(vmem_limit_bytes=40 << 20),
        name="finish",
    )(window_shift, sums, folded, own, borrowed)
    return (
        feat.transpose(2, 0, 1, 3),
        attend_grad.transpose(0, 2, 1),
        output_grad,
        bias_grad.transpose(1, 0, 2),
    )


def solution(mesh):
    placed = (
        P(None, "lat", "lon", None),
        P(None, None, "head"),
        P("head", None),
        P(None, "head", None),
        P(None, "lat"),
        P(),
        P(None, "lat", "lon", None),
    )
    return jax.shard_map(
        per_device,
        mesh=mesh,
        in_specs=placed,
        out_specs=(
            P(None, "lat", "lon", "head"),
            P(None, None, "head"),
            P("head", None),
            P(None, "head", None),
        ),
        check_vma=False,
    )
```

```python
import functools

import jax
import jax.numpy as jnp
from jax import lax
from jax.experimental import pallas as pl
from jax.experimental.pallas import tpu as pltpu
from jax.sharding import PartitionSpec as P

F32 = jnp.float32
BF16 = jnp.bfloat16
HEADS = 3
WINS = 4
WIDTH = 96
HEAD = 32
SLOTS = 12
GRID = 72
TOKENS = 144
MODEL = 384
SPAN = 23
TABLE = 3312
TABLE_PAD = 3328
GROUP = 138
SCALE = HEAD ** (-0.5)
VMEM = pl.BlockSpec(memory_space=pltpu.VMEM)
SMEM = pl.BlockSpec(memory_space=pltpu.SMEM)
ANY = pl.BlockSpec(memory_space=pl.ANY)


def dot(a, b, da, db):
    return lax.dot_general(a, b, (((da,), (db,)), ((), ())), preferred_element_type=F32)


def three(x):
    hi = x.astype(BF16)
    rest = x - hi.astype(F32)
    mid = rest.astype(BF16)
    return hi, mid, (rest - mid.astype(F32)).astype(BF16)


def fold_map(ci, shift):
    rows = lax.broadcasted_iota(jnp.int32, (288, 256), 0)
    lane = lax.broadcasted_iota(jnp.int32, (1, 256), 1)
    block = lane // SLOTS
    cj = lane - block * SLOTS
    wrap = jnp.where(ci < shift, 12, 0) - jnp.where(cj < shift, 12, 0)
    target = block * SPAN + (11 + ci) - cj + wrap
    target = jnp.where(lane < TOKENS, target, -1)
    return jnp.where(rows == target, 1.0, 0.0).astype(BF16)


def expand_bias(types, shift, table, tabw, spread, maps, bias):
    for h in range(HEADS):
        for w in range(WINS):
            n = h * WINS + w
            tabw[n : n + 1, 0:TABLE] = table[h, pl.ds(types[w], 1), :]
    spread[...] = jnp.zeros_like(spread)
    for zi in range(2):
        for ai in range(6):
            for zj in range(2):
                at = zi * 1656 + zj * 828 + ai * GROUP
                spread[zi * 6 + ai, 0:12, zj * GROUP : (zj + 1) * GROUP] = tabw[0:12, at : at + GROUP]
    parts = three(spread[...].reshape(192, 288))
    for ci in range(SLOTS):
        chosen = fold_map(ci, shift)
        maps[ci] = chosen
        full = dot(parts[0], chosen, 1, 0) + dot(parts[1], chosen, 1, 0) + dot(parts[2], chosen, 1, 0)
        for n in range(12):
            for k in range(2):
                bias[k, pl.ds(n * SLOTS + ci, 12, stride=TOKENS), :] = full[
                    n * 16 : n * 16 + 12, k * 128 : (k + 1) * 128
                ]


def window_rows(scratch, w):
    halves = []
    for z in range(2):
        lanes = [scratch[k, pl.ds(2 * w + z, GRID, stride=8), :] for k in range(3)]
        halves.append(jnp.concatenate(lanes, axis=1))
    return jnp.concatenate(halves, axis=0).astype(BF16)


def place_rows(own, borrowed, shift, scratch, first, slots):
    for c in slots:
        for a in range(6):
            rows = own[a, c].astype(F32)
            if borrowed is not None:
                keep = c >= shift if first == 0 else c < shift
                rows = jnp.where(keep, rows, borrowed[a, c - first].astype(F32))
            for k in range(3):
                scratch[k, (a * SLOTS + c) * 8 : (a * SLOTS + c + 1) * 8, :] = rows[:, k * 128 : (k + 1) * 128]


def only(x, h):
    return jnp.concatenate([x[k * HEAD : (k + 1) * HEAD] if k == h else jnp.zeros((HEAD, x.shape[1]), x.dtype) for k in range(HEADS)], axis=0)


def forward(xs, wts, bias, proj_out, softs, atts):
    tops = {}
    for w in range(WINS):
        xw = window_rows(xs, w)
        proj = dot(wts, xw, 1, 1).astype(BF16)
        proj_out[w] = proj
        q = dot(xw, wts[0:WIDTH], 1, 1).astype(BF16)
        for h in range(HEADS):
            n = h * WINS + w
            rows = slice(n * TOKENS, (n + 1) * TOKENS)
            added = jnp.concatenate([bias[0, rows, :], bias[1, rows, 0:16]], axis=1)
            logits = dot(q, only(proj[96:192], h), 1, 0) * SCALE + added
            softs[n] = logits
            tops[n] = jnp.max(logits, axis=1, keepdims=True)
    for w in range(WINS):
        sums = []
        for h in range(HEADS):
            n = h * WINS + w
            raised = jnp.exp(softs[n] - tops[n])
            softs[n] = raised
            sums.append(1.0 / jnp.sum(raised, axis=1, keepdims=True))
        att = []
        for h in range(HEADS):
            n = h * WINS + w
            soft = softs[n] * sums[h]
            softs[n] = soft
            att.append(dot(proj_out[w, 192 + h * HEAD : 192 + (h + 1) * HEAD, :], soft.astype(BF16), 1, 1))
        atts[w] = jnp.concatenate(att, axis=0).astype(BF16)


def backward(xs, gs, wos, proj_in, softs, gsofts, atts, scores, sums, dprojs):
    rowsums, dats = {}, {}
    for w in range(WINS):
        gw = window_rows(gs, w)
        dats[w] = dot(wos, gw, 1, 1).astype(BF16)
        da = dot(gw, wos, 1, 1).astype(BF16)
        vt = proj_in[w, 192:288, :]
        for h in range(HEADS):
            n = h * WINS + w
            gsoft = dot(da, only(vt, h), 1, 0)
            gsofts[n] = gsoft
            rowsums[n] = jnp.sum(softs[n] * gsoft, axis=1, keepdims=True)
        low = dot(atts[w], gw, 1, 0)
        if w == 0:
            sums[288:384, :] = low
        else:
            sums[288:384, :] += low
    for w in range(WINS):
        dq, dk, dv = [], [], []
        for h in range(HEADS):
            n = h * WINS + w
            rows = slice(n * TOKENS, (n + 1) * TOKENS)
            own = slice(h * HEAD, (h + 1) * HEAD)
            soft = softs[n]
            gsc = soft * (gsofts[n] - rowsums[n])
            scores[0, rows, :] = gsc[:, 0:128]
            scores[1, rows, 0:16] = gsc[:, 128:144]
            gh = gsc.astype(BF16)
            dv.append(dot(dats[w][own], soft.astype(BF16), 1, 0))
            dq.append(dot(proj_in[w, 96 + h * HEAD : 96 + (h + 1) * HEAD, :], gh, 1, 1) * SCALE)
            dk.append(dot(proj_in[w, own, :], gh, 1, 0) * SCALE)
        dproj = jnp.concatenate(dq + dk + dv, axis=0).astype(BF16)
        dprojs[w] = dproj
        top = dot(dproj, window_rows(xs, w), 1, 0)
        if w == 0:
            sums[0:288, :] = top
        else:
            sums[0:288, :] += top


def fold_scores(types, scores, maps, fold, folded, folded_out):
    total = None
    for ci in range(SLOTS):
        part = jnp.concatenate(
            [scores[0, pl.ds(ci, TOKENS, stride=SLOTS), :], scores[1, pl.ds(ci, TOKENS, stride=SLOTS), :][:, 0:16]], axis=1
        )
        term = dot(part.astype(BF16), maps[ci][:, 0:TOKENS], 1, 1)
        total = term if total is None else total + term
    for k in range(3):
        wide = min(128, 288 - k * 128)
        fold[k, :, 0:wide] = total[:, k * 128 : k * 128 + wide]
    folded[...] = jnp.zeros_like(folded)
    for zi in range(2):
        for ai in range(6):
            got = [fold[k, pl.ds(zi * 6 + ai, 12, stride=12), :] for k in range(3)]
            line = jnp.concatenate(got, axis=1)
            for zj in range(2):
                at = zi * 1656 + zj * 828 + ai * GROUP
                folded[0:12, at : at + GROUP] = line[:, zj * GROUP : (zj + 1) * GROUP]
    row = lax.broadcasted_iota(jnp.int32, (16, 128), 0)
    lane = lax.broadcasted_iota(jnp.int32, (16, 128), 1)
    marks = jnp.zeros((16, 128), jnp.int32)
    for w in range(WINS):
        marks = jnp.where(row == w, types[w], marks)
    folded[:, 3200:TABLE_PAD] = jnp.where(lane >= 112, marks.astype(F32), folded[:, 3200:TABLE_PAD])
    for i in range(16):
        left, right = (folded[:, i * 256 + k * 128 : i * 256 + (k + 1) * 128] for k in range(2))
        folded_out[i, 0] = left[0:8].astype(BF16)
        folded_out[i, 1] = right[0:8].astype(BF16)
        folded_out[i, 2] = jnp.concatenate([left[8:12], right[8:12]], axis=0).astype(BF16)


def pieces_out(wflip, dprojs, piece):
    for w in range(WINS):
        back = dot(wflip[...], dprojs[w], 1, 0).astype(BF16)
        for r in range(4):
            piece[r, :, w * TOKENS : (w + 1) * TOKENS] = back[r * WIDTH : (r + 1) * WIDTH]
    for r in range(4):
        piece[r, :, 576:640] = jnp.zeros((WIDTH, 64), BF16)


def finish_kernel(shift_ref, sums, folded, own, far, attend_out, output_out, bias_out, feat_out):
    first, last = [], []
    for q in range(4):
        high, low = [], []
        for z in range(7):
            for xh in range(2):
                part = folded[xh * 4 + q, z].astype(F32)
                high += [part[0], part[1]]
                low += [part[2, 0:4], part[2, 4:8]]
        first.append(jnp.concatenate(high[0:26], axis=1))
        last.append(jnp.concatenate(low[0:26], axis=1))
    marks = jnp.concatenate([first[q][0:4, TABLE : TABLE + 1] for q in range(4)], axis=0) * 0.0625
    lane = lax.broadcasted_iota(jnp.int32, (16, 128), 1).astype(F32)
    pick = jnp.where(lane == marks, 1.0, 0.0).T[0:64].astype(BF16)
    for h in range(HEADS):
        rows = [first[q][h * WINS : (h + 1) * WINS] if h < 2 else last[q] for q in range(4)]
        bias_out[h] = dot(pick, jnp.concatenate(rows, axis=0).astype(BF16), 1, 0)[:, 0:TABLE]
    for i in range(8):
        for r in range(3):
            for k in range(3):
                part = sums[i, r * 3 + k].astype(F32)
                at, lanes = (i % 2) * 48 + r * 16, slice(k * 128, (k + 1) * 128)
                if i < 6:
                    attend_out[i // 2, at : at + 16, lanes] = part
                else:
                    output_out[at : at + 16, lanes] = part
    shift = shift_ref[0]
    for c in range(SLOTS):
        mine = jnp.where(shift <= 6, c - shift, shift - 1 - c) >= 0
        for a in range(6):
            feat_out[a, c] = jnp.where(mine, own[a, c].astype(F32), far[a, c % 6].astype(F32)).astype(BF16)[:, 0:WIDTH]


def place_features(feat, lines, out):
    for w in range(WINS):
        both = jnp.concatenate([feat[:, w * TOKENS : (w + 1) * TOKENS], jnp.zeros((32, TOKENS), F32)], axis=0).T
        for z in range(2):
            lines[pl.ds(2 * w + z, GRID, stride=8), :] = both[z * GRID : (z + 1) * GRID]
    for a in range(6):
        for c in range(SLOTS):
            at = (a * SLOTS + c) * 8
            out[a, c] = lines[at : at + 8, :].astype(BF16)


class Links:
    def __init__(self, send, recv):
        self.send, self.recv, self.used, self.sent = send, recv, 0, []

    def slot(self):
        self.used += 1
        return self.used - 1

    def copy(self, k, src, dst, to):
        return pltpu.make_async_remote_copy(
            src_ref=src,
            dst_ref=dst,
            send_sem=self.send.at[k],
            recv_sem=self.recv.at[k],
            device_id=to,
            device_id_type=pl.DeviceIdType.MESH,
        )

    def start(self, src, dst, to, k=None):
        made = self.copy(self.slot() if k is None else k, src, dst, to)
        made.start()
        if k is None:
            self.sent.append(made)
        return made

    def group(self, k, whole, to):
        made = self.copy(k, whole, whole, to)
        self.sent.append(made)
        return made

    def many(self, whole, moves):
        k = self.slot()
        for src, dst, to in moves:
            self.start(src, dst, to, k)
        return self.group(k, whole, moves[-1][2])

    def settle(self):
        for made in self.sent:
            made.wait_send()
        self.sent = []


def place():
    lon, lat, head = lax.axis_index("lon"), lax.axis_index("lat"), lax.axis_index("head")
    z, high = lon // 2, lon % 2
    low, core = lat // 2, lat % 2
    return lon, lat, head, z, high, high * 2 + low, core


def at_grid(z, x, core):
    return {"lon": z * 2 + x // 2, "lat": (x % 2) * 2 + core}


def greet(peers):
    barrier = pltpu.get_barrier_semaphore()
    for peer in peers:
        pl.semaphore_signal(barrier, inc=1, device_id=peer, device_id_type=pl.DeviceIdType.MESH)
    return len(peers)


def reduce_peers():
    lon, lat, head, z, high, x, core = place()
    xc = x * 2 + core
    peers = [{"lon": (lon + k) % 16} for k in range(1, 16)]
    peers += [at_grid(z, ((xc + k) % 8) // 2, (xc + k) % 2) for k in range(1, 8)]
    peers += [{"head": (head + k) % 4} for k in range(1, 4)]
    return peers


NAMES = dict(
    xv=pltpu.VMEM((6, SLOTS, 8, MODEL), BF16),
    gv=pltpu.VMEM((6, SLOTS, 8, MODEL), BF16),
    xe=pltpu.VMEM((6, 6, 8, MODEL), BF16),
    ge=pltpu.VMEM((6, 6, 8, MODEL), BF16),
    tabv=pltpu.VMEM((3, 64, TABLE), F32),
    wtv=pltpu.VMEM((3, WIDTH, MODEL), BF16),
    wov=pltpu.VMEM((WIDTH, MODEL), BF16),
    tabw=pltpu.VMEM((16, TABLE_PAD), F32),
    spread=pltpu.VMEM((12, 16, 288), F32),
    maps=pltpu.VMEM((12, 288, 256), BF16),
    bias=pltpu.VMEM((2, 1728, 128), F32),
    xs=pltpu.VMEM((3, 576, 128), F32),
    gs=pltpu.VMEM((3, 576, 128), F32),
    wflip=pltpu.VMEM((MODEL, 288), BF16),
    projs=pltpu.VMEM((WINS, 288, TOKENS), BF16),
    gsofts=pltpu.VMEM((12, TOKENS, TOKENS), F32),
    softs=pltpu.VMEM((12, TOKENS, TOKENS), F32),
    atts=pltpu.VMEM((WINS, WIDTH, TOKENS), BF16),
    scores=pltpu.VMEM((2, 1728, 128), F32),
    dprojs=pltpu.VMEM((WINS, 288, TOKENS), BF16),
    fold=pltpu.VMEM((3, TOKENS, 128), F32),
    sums=pltpu.VMEM((MODEL, MODEL), F32),
    folded=pltpu.VMEM((16, 4096), F32),
    a0=pltpu.VMEM((4, 48, MODEL), BF16),
    ad=pltpu.VMEM((4, 48, MODEL), BF16),
    ax=pltpu.VMEM((4, 48, MODEL), BF16),
    f0=pltpu.VMEM((16, 3, 8, 128), BF16),
    p0=pltpu.VMEM((4, WIDTH, 640), BF16),
    a1=pltpu.VMEM((3, 48, MODEL), BF16),
    f1=pltpu.VMEM((15, 3, 8, 128), BF16),
    p1=pltpu.VMEM((3, WIDTH, 640), BF16),
    a2s=pltpu.VMEM((8, 2, 16, 128), BF16),
    a2=pltpu.VMEM((7, 2, 16, 128), BF16),
    a3=pltpu.VMEM((8, 16, 128), BF16),
    lines=pltpu.VMEM((576, 128), F32),
    f3=pltpu.VMEM((8, 3, 8, 128), BF16),
    send=pltpu.SemaphoreType.DMA((21,)),
    recv=pltpu.SemaphoreType.DMA((21,)),
    load=pltpu.SemaphoreType.DMA((7,)),
    types=pltpu.SMEM((1, 4), jnp.int32),
    shift=pltpu.SMEM((1,), jnp.int32),
)


def main_kernel(first, types_ref, shift_ref, x, g, table, wt, wo, a_out, f_out, own_out, west_out, *scratch):
    v = dict(zip(NAMES, scratch, strict=True))
    lon, lat, head, z, high, xpos, core = place()
    xc = xpos * 2 + core
    step = 1 if first == 0 else 15
    net = Links(v["send"], v["recv"])
    met = greet(reduce_peers())
    loads = []
    given = ((g, "gv"), (x, "xv"), (types_ref, "types"), (shift_ref, "shift"), (table, "tabv"), (wt, "wtv"), (wo, "wov"))
    for src, dst in given:
        made = pltpu.make_async_copy(src, v[dst], v["load"].at[len(loads)])
        made.start()
        loads.append(made)
    with jax.named_scope("enter"):
        for made in loads[0:2]:
            made.wait()
        pl.semaphore_wait(pltpu.get_barrier_semaphore(), met)

    giver = {"lon": (lon + 16 - step) % 16}
    rows, cols = pl.ds((head // 2) * 3, 3), (head % 2) * 3
    quarter = v["ge"].at[rows, pl.ds(cols, 3)]
    halo = [net.start(v["gv"].at[rows, pl.ds(first + cols, 3)], quarter, giver)]
    skip = 0 if first == 0 else 1
    near, spot = pl.ds(first + skip, 6 - skip), pl.ds(skip, 6 - skip)
    halo.append(net.start(v["xv"].at[:, near], v["xe"].at[:, spot], giver))
    with jax.named_scope("bias"):
        for made in loads[2:5]:
            made.wait()
        types = [v["types"][0, w] for w in range(WINS)]
        shift = v["shift"][0]
        expand_bias(types, shift, v["tabv"], v["tabw"], v["spread"], v["maps"], v["bias"])
    mixed = [c for c in range(first, first + 6)]
    still = [c for c in range(SLOTS) if c not in mixed]
    place_rows(v["xv"], None, shift, v["xs"], first, still + mixed[:skip])
    place_rows(v["gv"], None, shift, v["gs"], first, still)
    with jax.named_scope("still"):
        loads[5].wait()
        loads[6].wait()
        wts = v["wtv"][...].reshape(3 * WIDTH, MODEL)
        wos = v["wov"][...]
        v["wflip"][...] = wts.astype(F32).T.astype(BF16)

    with jax.named_scope("halo_q"):
        halo[0].wait_recv()
    handed = [net.start(quarter, quarter, {"head": (head + j) % 4}) for j in range(1, 4)]
    with jax.named_scope("halo_x"):
        halo[1].wait_recv()
    with jax.named_scope("forward"):
        place_rows(v["xv"], v["xe"], shift, v["xs"], first, mixed[skip:])
        forward(v["xs"], wts, v["bias"], v["projs"], v["softs"], v["atts"])
    with jax.named_scope("halo_g"):
        for made in handed:
            made.wait_recv()
    with jax.named_scope("backward"):
        place_rows(v["gv"], v["ge"], shift, v["gs"], first, mixed)
        backward(v["xs"], v["gs"], wos, v["projs"], v["softs"], v["gsofts"], v["atts"], v["scores"], v["sums"], v["dprojs"])

    def zs(k):
        return {"lon": ((z + k) % 8) * 2 + high}

    a0, f0, p0 = v["a0"], v["f0"], v["p0"]
    a1, f1, p1 = v["a1"], v["f1"], v["p1"]
    ad, ax, a2s, a2, a3, f3 = (v[n] for n in ("ad", "ax", "a2s", "a2", "a3", "f3"))
    partner = at_grid(z, xpos, 1 - core)

    def chunk(i, side):
        return v["sums"][pl.ds(pl.multiple_of((2 * i + side) * 48, 16), 48), :]

    for i in range(4):
        a0[i] = chunk(i, 1 - core).astype(BF16)
    twin = net.start(a0, ad, partner)
    with jax.named_scope("fold"):
        fold_scores(types, v["scores"], v["maps"], v["fold"], v["folded"], f0)
    with jax.named_scope("sum_d"):
        twin.wait_recv()
        for i in range(4):
            ax[i] = (chunk(i, core) + ad[i].astype(F32)).astype(BF16)
    one = net.many(a1, [(ax.at[(xpos + k) % 4], a1.at[k - 1], at_grid(z, (xpos + k) % 4, core)) for k in range(1, 4)])
    two = net.many(f1, [(f0.at[(lon + k) % 16], f1.at[k - 1], {"lon": (lon + k) % 16}) for k in range(1, 16)])
    with jax.named_scope("pieces"):
        pieces_out(v["wflip"], v["dprojs"], p0)
    pieces = net.many(p1, [(p0.at[(head + k) % 4], p1.at[k - 1], {"head": (head + k) % 4}) for k in range(1, 4)])

    with jax.named_scope("sum_a"):
        total = chunk(xpos, core) + ad[xpos].astype(F32)
        one.wait_recv()
        for k in range(3):
            total = total + a1[k].astype(F32)
        tiles = [total[r * 16 : (r + 1) * 16, k * 128 : (k + 1) * 128].astype(BF16) for r in range(3) for k in range(3)]
        for k in range(8):
            a2s[k, 0] = tiles[k]
            a2s[k, 1] = tiles[8]
    three_ = net.many(a2, [(a2s.at[(z + k) % 8], a2.at[k - 1], zs(k)) for k in range(1, 8)])

    with jax.named_scope("sum_f"):
        lines = f0[lon].astype(F32)
        two.wait_recv()
        for k in range(15):
            lines = lines + f1[k].astype(F32)
        f3[z] = lines.astype(BF16)
    part = f3.at[pl.ds(0, 7)]
    five = net.many(part, [(f3.at[z], f3.at[z], zs(k)) for k in range(1, 8)])

    with jax.named_scope("sum_z"):
        block = a2s[z].astype(F32)
        three_.wait_recv()
        for k in range(7):
            block = block + a2[k].astype(F32)
        a3[z] = block[0].astype(BF16)
    six = net.many(a3.at[pl.ds(0, 7)], [(a3.at[z], a3.at[z], zs(k)) for k in range(1, 8)])
    a_out[xc, 8] = block[1].astype(BF16)

    with jax.named_scope("sum_p"):
        feat = p0[head].astype(F32)
        pieces.wait_recv()
        for k in range(3):
            feat = feat + p1[k].astype(F32)
        place_features(feat, v["lines"], own_out)
    back = net.start(own_out.at[:, near], west_out.at[:, spot], {"lon": (lon + step) % 16})

    with jax.named_scope("all_f"):
        five.wait_recv()
    mine = f_out.at[xc, pl.ds(0, 7)]
    arrive_f = [net.start(part, mine, at_grid(z, (xpos + k) % 4, core)) for k in range(1, 4)]
    cross_f, cross_a = net.slot(), net.slot()
    net.start(part, mine, partner, cross_f)
    f_out[xc] = f3[...]
    with jax.named_scope("all_a"):
        six.wait_recv()
    a_out[xc, 0:8] = a3[...]
    arrive = [net.start(a_out.at[xc], a_out.at[xc], at_grid(z, (xpos + k) % 4, core)) for k in range(1, 4)]
    net.start(a_out.at[xc], a_out.at[xc], partner, cross_a)
    with jax.named_scope("forward_x"):
        for k in range(1, 4):
            there = ((xpos + 4 - k) % 4) * 2 + core
            arrive_f[k - 1].wait_recv()
            ref = f_out.at[there, pl.ds(0, 7)]
            net.start(ref, ref, partner, cross_f)
        for k in range(1, 4):
            there = ((xpos + 4 - k) % 4) * 2 + core
            arrive[k - 1].wait_recv()
            net.start(a_out.at[there], a_out.at[there], partner, cross_a)
    cross = [net.group(cross_f, f_out.at[pl.ds(0, 4), pl.ds(0, 7)], partner), net.group(cross_a, a_out.at[pl.ds(0, 4)], partner)]
    net.settle()
    with jax.named_scope("last"):
        back.wait_recv()
        for made in cross:
            made.wait_recv()


def per_device(features, attend_weight, output_weight, bias_table, bias_type, window_shift, grad_out):
    x = features.transpose(1, 2, 0, 3)
    g = grad_out.transpose(1, 2, 0, 3)
    wt = attend_weight.transpose(0, 2, 1)
    table = bias_table.transpose(1, 0, 2)

    def run(first):
        return pl.pallas_call(
            functools.partial(main_kernel, first),
            out_shape=(
                jax.ShapeDtypeStruct((8, 9, 16, 128), BF16),
                jax.ShapeDtypeStruct((8, 8, 3, 8, 128), BF16),
                jax.ShapeDtypeStruct((6, SLOTS, 8, 128), BF16),
                jax.ShapeDtypeStruct((6, 6, 8, 128), BF16),
            ),
            in_specs=[ANY] * 7,
            out_specs=(VMEM,) * 4,
            scratch_shapes=list(NAMES.values()),
            compiler_params=pltpu.CompilerParams(
                vmem_limit_bytes=56 << 20, collective_id=1 if first == 0 else 2, has_side_effects=True
            ),
            name="block_east" if first == 0 else "block_west",
        )

    args = (bias_type.T, window_shift, x, g, table, wt, output_weight)
    sums, folded, own, borrowed = lax.cond(window_shift[0] <= 6, run(0), run(6), *args)
    return finish(window_shift, sums, folded, own, borrowed)


def finish(window_shift, sums, folded, own, borrowed):
    attend_grad, output_grad, bias_grad, feat = pl.pallas_call(
        finish_kernel,
        out_shape=(
            jax.ShapeDtypeStruct((3, WIDTH, MODEL), F32),
            jax.ShapeDtypeStruct((WIDTH, MODEL), F32),
            jax.ShapeDtypeStruct((3, 64, TABLE), F32),
            jax.ShapeDtypeStruct((6, SLOTS, 8, WIDTH), BF16),
        ),
        in_specs=[SMEM, VMEM, VMEM, VMEM, VMEM],
        out_specs=(VMEM,) * 4,
        compiler_params=pltpu.CompilerParams(vmem_limit_bytes=40 << 20),
        name="finish",
    )(window_shift, sums, folded, own, borrowed)
    return (
        feat.transpose(2, 0, 1, 3),
        attend_grad.transpose(0, 2, 1),
        output_grad,
        bias_grad.transpose(1, 0, 2),
    )


def solution(mesh):
    placed = (
        P(None, "lat", "lon", None),
        P(None, None, "head"),
        P("head", None),
        P(None, "head", None),
        P(None, "lat"),
        P(),
        P(None, "lat", "lon", None),
    )
    return jax.shard_map(
        per_device,
        mesh=mesh,
        in_specs=placed,
        out_specs=(
            P(None, "lat", "lon", "head"),
            P(None, None, "head"),
            P("head", None),
            P(None, "head", None),
        ),
        check_vma=False,
    )
```
